8 devices in a mesh: dp: 1 (over z), tp: 8 (over x, y, core).
Axes of the slice: x: 2, y: 2, z: 1, core: 2. Of those that a mesh axis runs over, the one named last changes fastest.
Arguments:
- x: bfloat16 [4096, 2048], P(('dp', 'tp'))
- dy: bfloat16 [4096, 2048], P(('dp', 'tp'))
- gain: bfloat16 [2048], replicated
- wq: bfloat16 [2048, 2048], P(None, 'tp')
- wk: bfloat16 [2048, 2048], P(None, 'tp')
- wv: bfloat16 [2048, 2048], P(None, 'tp')
- wo: bfloat16 [2048, 2048], P('tp')
Outputs:
- output 1: bfloat16 [4096, 2048], P(('dp', 'tp'))
- output 2: float32 [1, 2048], P('dp')
- output 3: bfloat16 [2048, 2048], P('dp', 'tp')
- output 4: bfloat16 [2048, 2048], P('dp', 'tp')
- output 5: bfloat16 [2048, 2048], P('dp', 'tp')
- output 6: bfloat16 [2048, 2048], P(('dp', 'tp'))
All inputs are finite; a program needn't handle non-finite values.
Results may differ from the reference program's by a relative error of at most 0.018.
Values are sent between devices in bfloat16 or wider.
A program may use at most 2 GiB of HBM per device.

```python
import jax
import jax.numpy as jnp
from jax import lax

ROWS = 4096
D = 2048
HEADS = 16
KV_HEADS = 16
HEAD = 128
THETA = 10000


def setup_inputs(seed: int = 0, part: int = 0) -> dict:
    kx, ky, kn, kq, kk, kv, ko = jax.random.split(jax.random.key(seed), 7)

    def weights(key, rows, columns):
        return jax.random.normal(key, (rows, columns), jnp.float32) * rows**-0.5

    drawn = {
        "x": jax.random.normal(jax.random.fold_in(kx, part), (ROWS, D), jnp.float32),
        "dy": jax.random.normal(jax.random.fold_in(ky, part), (ROWS, D), jnp.float32) * ROWS**-0.5,
        "gain": 1 + 0.1 * jax.random.normal(kn, (D,), jnp.float32),
        "wq": 2 * weights(kq, D, HEADS * HEAD),
        "wk": 2 * weights(kk, D, KV_HEADS * HEAD),
        "wv": 4 * weights(kv, D, KV_HEADS * HEAD),
        "wo": weights(ko, HEADS * HEAD, D),
    }
    return {k: v.astype(jnp.bfloat16) for k, v in drawn.items()}


def normed(x, gain):
    wide = x.astype(jnp.float32)
    scale = lax.rsqrt(jnp.mean(wide * wide, -1, keepdims=True) + 1e-6)
    return (wide * scale * gain.astype(jnp.float32)).astype(jnp.bfloat16)


def turned(t, place, theta):
    half = t.shape[-1] // 2
    angle = place.astype(jnp.float32)[:, None] * theta ** (-jnp.arange(half, dtype=jnp.float32) / half)
    cos, sin = jnp.cos(angle)[:, None], jnp.sin(angle)[:, None]
    a, b = t[..., :half].astype(jnp.float32), t[..., half:].astype(jnp.float32)
    return jnp.concatenate([a * cos - b * sin, b * cos + a * sin], -1).astype(jnp.bfloat16)


def matmul(a, w):
    return jnp.dot(a, w, preferred_element_type=jnp.float32).astype(jnp.bfloat16)


def einsum(form, a, b):
    return jnp.einsum(form, a.astype(jnp.float32), b.astype(jnp.float32))


def attention(q, k, v):
    scores = einsum("tgsd,ugd->gstu", q, k) * q.shape[-1] ** -0.5
    token = jnp.arange(q.shape[0])
    scores = jnp.where(token[:, None] >= token, scores, -jnp.inf)
    weights = jax.nn.softmax(scores, -1).astype(jnp.bfloat16)
    return einsum("gstu,ugd->tgsd", weights, v).astype(jnp.bfloat16)


def forward(x, gain, wq, wk, wv, wo):
    rows = x.shape[0]
    a, place = normed(x, gain), jnp.arange(rows)
    k = turned(matmul(a, wk).reshape(rows, -1, HEAD), place, THETA)
    q = turned(matmul(a, wq).reshape(rows, -1, HEAD), place, THETA).reshape(rows, k.shape[1], -1, HEAD)
    v = matmul(a, wv).reshape(rows, -1, HEAD)
    seen = attention(q, k, v).reshape(rows, -1)
    return (x.astype(jnp.float32) + jnp.dot(seen, wo, preferred_element_type=jnp.float32)).astype(jnp.bfloat16)


def reference(x, dy, gain, wq, wk, wv, wo):
    _, back = jax.vjp(forward, x, gain.astype(jnp.float32), wq, wk, wv, wo)
    by_x, by_gain, *by_weights = back(dy)
    return (by_x, by_gain[None], *by_weights)
```

```python
import functools

import jax
import jax.numpy as jnp
import numpy as np
from jax import lax
from jax.experimental import pallas as pl
from jax.experimental.pallas import tpu as pltpu
from jax.sharding import PartitionSpec as P

HEAD = 128
THETA = 10000
LOG2E = 1.4426950408889634
HIDDEN = -2e30
NEG = -1e30
ROWS, D, MINE = 4096, 2048, 256
PIECE = 256
KEYS = 512
SCALE = HEAD**-0.5
E = SCALE * LOG2E
BF, F32 = jnp.bfloat16, jnp.float32


def tables():
    half = HEAD // 2
    turn = float(THETA) ** (-np.arange(half) / half)
    both = lambda t: np.concatenate([t, t], 1).astype(np.float32)
    near = np.arange(PIECE)[:, None] * turn
    far = np.arange(0, ROWS, PIECE)[:, None] * turn
    return tuple(jnp.asarray(both(f(t))) for t in (near, far) for f in (np.cos, np.sin))


def dot(a, b, ca=1, cb=0):
    return lax.dot_general(a, b, (((ca,), (cb,)), ((), ())), preferred_element_type=F32)


def angles(block, near_cos, near_sin, far_cos, far_sin):
    fc, fs = far_cos[pl.ds(block, 1), :], far_sin[pl.ds(block, 1), :]
    nc, ns = near_cos[...], near_sin[...]
    sign = jnp.where(lax.broadcasted_iota(jnp.int32, (1, HEAD), 1) < HEAD // 2, -1.0, 1.0)
    return nc * fc - ns * fs, (ns * fc + nc * fs) * sign


def turn(t, cos, sin):
    return t * cos + pltpu.roll(t, HEAD // 2, 1) * sin


def params(n=1, vmem=60):
    return pltpu.CompilerParams(dimension_semantics=("arbitrary",) * n, vmem_limit_bytes=vmem * 2**20)


def whole(shape):
    return pl.BlockSpec(shape, lambda *_: (0,) * len(shape), pipeline_mode=pl.Buffered(1))


ANY = pl.BlockSpec(memory_space=pl.ANY)


def _norm(x_ref, gain_ref, lo_ref, hi_ref):
    wide = x_ref[...].astype(F32)
    scale = lax.rsqrt(jnp.mean(wide * wide, -1, keepdims=True) + 1e-6)
    out = (wide * scale * gain_ref[...].astype(F32)).astype(BF)
    lo_ref[...] = out[:PIECE]
    hi_ref[...] = out[PIECE:]


def norm(x, gain):
    return pl.pallas_call(
        _norm,
        out_shape=[jax.ShapeDtypeStruct((PIECE, D), BF)] * 2,
        compiler_params=pltpu.CompilerParams(vmem_limit_bytes=32 * 2**20),
        cost_estimate=pl.CostEstimate(flops=2 * 2**20, bytes_accessed=4 * 2**20, transcendentals=512),
        name="norm",
    )(x, gain[None])


def _project(n, blocks, *refs):
    pieces, (wq, wk, wv, nc, ns, fc, fs, _, out) = refs[:n], refs[n:]
    for i in range(n):

        @pl.when(pl.program_id(0) == i)
        def _():
            a = pieces[i][...]
            cos, sin = angles(blocks[i], nc, ns, fc, fs)
            for at, w in ((0, wq), (MINE, wk)):
                t = dot(a, w[...]).astype(BF).astype(F32)
                for h in range(0, MINE, HEAD):
                    out[:, at + h : at + h + HEAD] = turn(t[:, h : h + HEAD], cos, sin).astype(BF)
            out[:, 2 * MINE :] = dot(a, wv[...]).astype(BF)


def project(buf, pieces, blocks, wq, wk, wv, tabs):
    n = len(pieces)
    fresh = buf is None
    if fresh:
        buf = jnp.zeros((8, 128), BF)
    piece = whole((PIECE, D))
    return pl.pallas_call(
        functools.partial(_project, n),
        grid_spec=pltpu.PrefetchScalarGridSpec(
            num_scalar_prefetch=1,
            grid=(n,),
            in_specs=[piece] * n + [whole((D, MINE))] * 3 + [whole(t.shape) for t in tabs] + [ANY],
            out_specs=pl.BlockSpec((PIECE, 3 * MINE), lambda i, blocks: (blocks[i], 0)),
        ),
        out_shape=jax.ShapeDtypeStruct((ROWS, 3 * MINE), BF),
        input_output_aliases={} if fresh else {1 + n + 7: 0},
        compiler_params=params(),
        cost_estimate=pl.CostEstimate(flops=2 * n * PIECE * D * 3 * MINE, bytes_accessed=n * PIECE * D * 2 + 3 * 2**20, transcendentals=0),
        name="project",
    )(blocks, *pieces, wq, wk, wv, *tabs, buf)


QROWS = 1024
STRIPS = QROWS // KEYS


def causal(s, hidden):
    ok = lax.broadcasted_iota(jnp.int32, s.shape, 1) >= lax.broadcasted_iota(jnp.int32, s.shape, 0)
    return jnp.where(ok, s, hidden)


def _attend(qkv, o_ref, lse_ref, vt, top_s, mix_s):
    iq = pl.program_id(0)

    @pl.when(iq == 0)
    def _():
        for h in range(2):
            for at in range(0, ROWS, KEYS):
                vt[h, :HEAD, at : at + KEYS] = qkv[at : at + KEYS, 2 * MINE + h * HEAD : 2 * MINE + (h + 1) * HEAD].T
            vt[h, HEAD:, :] = jnp.ones((16, ROWS), BF)

    top_s[...] = jnp.full(top_s.shape, NEG, F32)
    mix_s[...] = jnp.zeros(mix_s.shape, F32)

    def block(j, strips):
        at = pl.multiple_of(j * KEYS, KEYS)
        pieces = [(h, s, m) for s, m in strips for h in range(2)]
        scores = []
        for h, s, _ in pieces:
            k = qkv[pl.ds(at, KEYS), MINE + h * HEAD : MINE + (h + 1) * HEAD]
            q = qkv[pl.ds(pl.multiple_of(iq * QROWS + s * KEYS, KEYS), KEYS), h * HEAD : (h + 1) * HEAD]
            scores.append(dot(k, q, 1, 1))
        weights, keeps = [], []
        for (h, s, m), sc in zip(pieces, scores):
            if m:
                sc = causal(sc, HIDDEN)
            n = 2 * s + h
            old = top_s[n : n + 1, :]
            top = jnp.maximum(old, sc.max(axis=0, keepdims=True))
            top_s[n : n + 1, :] = top
            weights.append(jnp.exp2((sc - top) * E).astype(BF))
            keeps.append(jnp.exp2((old - top) * E))
        for (h, s, m), p, keep in zip(pieces, weights, keeps):
            n = 2 * s + h
            mix_s[n] = mix_s[n] * keep + dot(vt[h, :, pl.ds(at, KEYS)], p)

    lax.fori_loop(0, iq * STRIPS, lambda j, _: block(j, [(s, False) for s in range(STRIPS)]), None)
    for s in range(STRIPS):
        block(iq * STRIPS + s, [(s, True)] + [(t, False) for t in range(s + 1, STRIPS)])
    for s in range(STRIPS):
        for h in range(2):
            n = 2 * s + h
            total = mix_s[n, HEAD : HEAD + 1, :]
            o_ref[s * KEYS : (s + 1) * KEYS, h * HEAD : (h + 1) * HEAD] = (mix_s[n, :HEAD, :] * (1 / total)).T.astype(BF)
            lse_ref[h : h + 1, s * KEYS : (s + 1) * KEYS] = top_s[n : n + 1, :] * E + jnp.log2(total)


def attend(qkv):
    n = 2 * STRIPS
    return pl.pallas_call(
        _attend,
        grid=(ROWS // QROWS,),
        in_specs=[whole((ROWS, 3 * MINE))],
        out_specs=[pl.BlockSpec((QROWS, MINE), lambda i: (i, 0)), pl.BlockSpec((2, QROWS), lambda i: (0, i))],
        out_shape=[jax.ShapeDtypeStruct((ROWS, MINE), BF), jax.ShapeDtypeStruct((2, ROWS), F32)],
        scratch_shapes=[pltpu.VMEM((2, HEAD + 16, ROWS), BF), pltpu.VMEM((n, KEYS), F32), pltpu.VMEM((n, HEAD + 16, KEYS), F32)],
        compiler_params=params(),
        cost_estimate=pl.CostEstimate(flops=2 * ROWS * ROWS * 2 * HEAD * 2, bytes_accessed=8 * 2**20, transcendentals=ROWS * ROWS),
        name="attend",
    )(qkv)


def _lift(n, blocks, *refs):
    pieces, (wo, _, out) = refs[:n], refs[n:]
    for i in range(n):

        @pl.when(pl.program_id(0) == i)
        def _():
            out[...] = dot(pieces[i][...], wo[...], 1, 1).astype(BF)


def lift(buf, pieces, blocks, wo):
    n = len(pieces)
    fresh = buf is None
    if fresh:
        buf = jnp.zeros((8, 128), BF)
    return pl.pallas_call(
        functools.partial(_lift, n),
        grid_spec=pltpu.PrefetchScalarGridSpec(
            num_scalar_prefetch=1,
            grid=(n,),
            in_specs=[whole((PIECE, D))] * n + [whole((MINE, D)), ANY],
            out_specs=pl.BlockSpec((PIECE, MINE), lambda i, blocks: (blocks[i], 0)),
        ),
        out_shape=jax.ShapeDtypeStruct((ROWS, MINE), BF),
        input_output_aliases={} if fresh else {1 + n + 1: 0},
        compiler_params=params(),
        cost_estimate=pl.CostEstimate(flops=2 * n * PIECE * D * MINE, bytes_accessed=n * PIECE * D * 2 + 2**20, transcendentals=0),
        name="lift",
    )(blocks, *pieces, wo, buf)


def _back(n, first, last, chips, qkv, do_ref, o_ref, lse_ref, nc, ns, fc, fs, *refs):
    if first:
        (dqm_in, dqt_in, acc_in), refs = (None,) * 3, refs
    else:
        (dqm_in, dqt_in, acc_in), refs = refs[:3], refs[3:]
    if last:
        dqm, dqt, dkvm, dkvt, acc, kt, dq_s, delta_s = refs
    else:
        dqm, dqt, acc, kt, dq_s, delta_s = refs
    step = pl.program_id(0)
    chip, core = chips[step], chips[n]

    @pl.when(step == 0)
    def _():
        acc[...] = jnp.zeros(acc.shape, F32) if first else acc_in[...]
        for h in range(2):
            for at in range(0, ROWS, KEYS):
                kt[h, :, at : at + KEYS] = qkv[at : at + KEYS, MINE + h * HEAD : MINE + (h + 1) * HEAD].T

    dq_s[...] = jnp.zeros(dq_s.shape, F32)
    for h in range(2):
        lanes = slice(h * HEAD, (h + 1) * HEAD)
        for s in range(STRIPS):
            at = s * KEYS
            both = do_ref[at : at + KEYS, lanes].astype(F32) * o_ref[at : at + KEYS, lanes].astype(F32)
            delta_s[h : h + 1, at : at + KEYS] = both.T.sum(axis=0, keepdims=True)

    def block(j, strip, width, masked):
        at = pl.multiple_of(j * KEYS, KEYS)
        here = pl.ds(at, KEYS)
        left = strip * KEYS
        rows = pl.ds(pl.multiple_of(chip * QROWS + left, KEYS), width)
        cols = slice(left, left + width)
        qs, dos, scores, dps = [], [], [], []
        for h in range(2):
            lanes = slice(h * HEAD, (h + 1) * HEAD)
            q, do = qkv[rows, lanes], do_ref[cols, lanes]
            scores.append(dot(qkv[here, MINE + h * HEAD : MINE + (h + 1) * HEAD], q, 1, 1))
            dps.append(dot(qkv[here, 2 * MINE + h * HEAD : 2 * MINE + (h + 1) * HEAD], do, 1, 1))
            qs.append(q)
            dos.append(do)
        for h in range(2):
            p = jnp.exp2(scores[h] * E - lse_ref[h : h + 1, cols])
            if masked:
                p = causal(p, 0.0)
            ds = (p * (dps[h] - delta_s[h : h + 1, cols])).astype(BF)
            acc[here, MINE + h * HEAD : MINE + (h + 1) * HEAD] += dot(p.astype(BF), dos[h])
            acc[here, h * HEAD : (h + 1) * HEAD] += dot(ds, qs[h])
            dq_s[h, :, cols] += dot(kt[h, :, here], ds)

    lax.fori_loop(0, chip * STRIPS, lambda j, _: block(j, 0, QROWS, False), None)
    for s in range(STRIPS):
        block(chip * STRIPS + s, s, QROWS - s * KEYS, True)

    per = KEYS // PIECE
    for s in range(STRIPS):
        for i in range(per):
            cos, sin = angles(chip * (QROWS // PIECE) + s * per + i, nc, ns, fc, fs)
            at = s * KEYS + i * PIECE
            got = [turn((dq_s[h, :, at : at + PIECE] * SCALE).T, cos, -sin).astype(BF) for h in range(2)]
            got = jnp.concatenate(got, 1)

            @pl.when(core == s)
            def _():
                dqm[i * PIECE : (i + 1) * PIECE, :] = got

            @pl.when(core != s)
            def _():
                dqt[i * PIECE : (i + 1) * PIECE, :] = got

    if last:

        @pl.when(step == n - 1)
        def _():
            def finish(b, _):
                cos, sin = angles(b, nc, ns, fc, fs)
                here = pl.ds(pl.multiple_of(b * PIECE, PIECE), PIECE)
                got = [turn(acc[here, h * HEAD : (h + 1) * HEAD] * SCALE, cos, -sin).astype(BF) for h in range(2)]
                got = jnp.concatenate(got + [acc[here, MINE:].astype(BF)], 1)
                part = lax.rem(lax.div(b, per), 2)
                to = pl.ds(pl.multiple_of((lax.div(b, 2 * per) * per + lax.rem(b, per)) * PIECE, PIECE), PIECE)

                @pl.when(core == part)
                def _():
                    dkvm[to, :] = got

                @pl.when(core != part)
                def _():
                    dkvt[to, :] = got

            lax.fori_loop(0, ROWS // PIECE, finish, None)


def back(chips, n, qkv, d_out, o, lse, tabs, state, last):
    first = state is None
    queries = pl.BlockSpec((QROWS, MINE), lambda i, chips: (chips[i], 0))
    half = pl.BlockSpec((KEYS, MINE), lambda i, chips: (chips[i], 0))
    out_specs, out_shape = [half, half], [jax.ShapeDtypeStruct((ROWS // 2, MINE), BF)] * 2
    acc = jax.ShapeDtypeStruct((ROWS, 2 * MINE), F32)
    scratch = [pltpu.VMEM((2, HEAD, ROWS), BF), pltpu.VMEM((2, HEAD, QROWS), F32), pltpu.VMEM((2, QROWS), F32)]
    if last:
        out_specs += [whole((ROWS // 2, 2 * MINE))] * 2
        out_shape += [jax.ShapeDtypeStruct((ROWS // 2, 2 * MINE), BF)] * 2
        scratch = [pltpu.VMEM(acc.shape, F32)] + scratch
    else:
        out_specs += [whole(acc.shape)]
        out_shape += [acc]
    given, more = [], []
    if not first:
        given, more = list(state), [ANY, ANY, whole(acc.shape)]
    return pl.pallas_call(
        functools.partial(_back, n, first, last),
        grid_spec=pltpu.PrefetchScalarGridSpec(
            num_scalar_prefetch=1,
            grid=(n,),
            in_specs=[whole((ROWS, 3 * MINE)), queries, queries, pl.BlockSpec((2, QROWS), lambda i, chips: (0, chips[i]))]
            + [whole(t.shape) for t in tabs]
            + more,
            out_specs=out_specs,
            scratch_shapes=scratch,
        ),
        out_shape=out_shape,
        input_output_aliases={} if first else {9: 0, 10: 1},
        compiler_params=params(vmem=62),
        cost_estimate=pl.CostEstimate(flops=n * 2 * ROWS * ROWS * HEAD * 5 // 2, bytes_accessed=20 * 2**20, transcendentals=n * ROWS * ROWS // 4),
        name="back",
    )(chips, qkv, d_out, o, lse, *tabs, *given)


WIDE = 512


def _terms(n, blocks, *refs):
    rows, refs = refs[: 4 * n], refs[4 * n :]
    ws, refs = refs[:6], refs[6:]
    adds, outs = refs[:-n], refs[-n:]
    for i in range(n):
        qm, kvm, qr, kvr = rows[4 * i : 4 * i + 4]
        total = None
        for q, kv, (wq, wk, wv) in ((qm, kvm, ws[:3]), (qr, kvr, ws[3:])):
            t = dot(q[...], wq[...], 1, 1) + dot(kv[:, :MINE], wk[...], 1, 1) + dot(kv[:, MINE:], wv[...], 1, 1)
            total = t if total is None else total + t
        if adds:
            total = total + adds[i][...].astype(F32)
        outs[i][...] = total.astype(outs[i].dtype)


def terms(blocks, n, grads, weights, adds=()):
    specs = []
    for i in range(n):
        at = lambda j, blocks, i=i: (blocks[i], 0)
        specs += [pl.BlockSpec((PIECE, MINE), at), pl.BlockSpec((PIECE, 2 * MINE), at)] * 2
    out = pl.BlockSpec((PIECE, WIDE), lambda j, blocks: (0, j))
    return pl.pallas_call(
        functools.partial(_terms, n),
        grid_spec=pltpu.PrefetchScalarGridSpec(
            num_scalar_prefetch=1,
            grid=(D // WIDE,),
            in_specs=specs + [pl.BlockSpec((WIDE, MINE), lambda j, blocks: (j, 0))] * 6 + [out] * len(adds),
            out_specs=[out] * n,
        ),
        out_shape=[jax.ShapeDtypeStruct((PIECE, D), BF)] * n,
        compiler_params=params(),
        cost_estimate=pl.CostEstimate(flops=2 * n * PIECE * D * 6 * MINE, bytes_accessed=8 * 2**20, transcendentals=0),
        name="terms",
    )(blocks, *(list(grads) * n), *weights, *adds)


def _end(blocks, qm, kvm, qr, kvr, wq, wk, wv, uq, uk, uv, g0, g1, x_ref, dy_ref, gain_ref, dx_ref, dgain_ref):
    i = pl.program_id(0)
    da = dot(qm[...], wq[...], 1, 1) + dot(kvm[:, :MINE], wk[...], 1, 1) + dot(kvm[:, MINE:], wv[...], 1, 1)
    da = da + dot(qr[...], uq[...], 1, 1) + dot(kvr[:, :MINE], uk[...], 1, 1) + dot(kvr[:, MINE:], uv[...], 1, 1)
    da = da + g0[0].astype(F32) + g1[0].astype(F32)
    wide = x_ref[...].astype(F32)
    scale = lax.rsqrt(jnp.mean(wide * wide, -1, keepdims=True) + 1e-6)
    hat = wide * scale
    got = da * gain_ref[...].astype(F32)
    inner = jnp.mean(got * hat, -1, keepdims=True)
    dx_ref[...] = (dy_ref[...].astype(F32) + (got - hat * inner) * scale).astype(BF)

    @pl.when(i == 0)
    def _():
        dgain_ref[...] = jnp.zeros(dgain_ref.shape, F32)

    dgain_ref[...] += (da * hat).sum(axis=0, keepdims=True)


def end(blocks, grads, weights, got, x, dy, gain):
    part = 128
    per = PIECE // part
    at = lambda j, blocks: (blocks[0] * 2 * per + j, 0)
    row = pl.BlockSpec((part, D), lambda j, blocks: (j, 0))
    return pl.pallas_call(
        _end,
        grid_spec=pltpu.PrefetchScalarGridSpec(
            num_scalar_prefetch=1,
            grid=(2 * per,),
            in_specs=[pl.BlockSpec((part, MINE), at), pl.BlockSpec((part, 2 * MINE), at)] * 2
            + [whole((D, MINE))] * 6
            + [pl.BlockSpec((1, part, D), lambda j, blocks: (lax.div(j, per), lax.rem(j, per), 0))] * 2
            + [row, row, whole((1, D))],
            out_specs=[row, whole((1, D))],
        ),
        out_shape=[jax.ShapeDtypeStruct((2 * PIECE, D), BF), jax.ShapeDtypeStruct((1, D), F32)],
        compiler_params=params(),
        cost_estimate=pl.CostEstimate(flops=4 * PIECE * D * 6 * MINE, bytes_accessed=16 * 2**20, transcendentals=512),
        name="end",
    )(blocks, *grads, *weights, *got, x, dy, gain[None])


def _weights(rows, *refs):
    n = len(rows)
    pieces, refs = refs[:n], refs[n:]
    blocks, (dqm, dkvm, dqt, dkvt, gq, gk, gv, acc) = None, refs
    return pieces, blocks


def _by_qkv(n, same, blocks, *refs):
    pieces, (dqm, dkvm, dqt, dkvt, gq, gk, gv) = refs[:n], refs[n:]
    total = None
    for at in range(0, n, 4):
        a = jnp.concatenate([pieces[i][...] for i in range(at, at + 4)], 0)
        take = lambda m, t: jnp.concatenate(
            [(m if same[i] else t)[pl.ds(pl.multiple_of(blocks[i] * PIECE, PIECE), PIECE), :] for i in range(at, at + 4)], 0)
        g = jnp.concatenate([take(dqm, dqt), take(dkvm, dkvt)], 1)
        t = dot(a, g, 0, 0)
        total = t if total is None else total + t
    gq[...] = total[:, :MINE].astype(BF)
    gk[...] = total[:, MINE : 2 * MINE].astype(BF)
    gv[...] = total[:, 2 * MINE :].astype(BF)


def by_qkv(pieces, same, blocks, dqm, dkvm, dqt, dkvt):
    n = len(pieces)
    tile = 512
    out = pl.BlockSpec((tile, MINE), lambda j, blocks: (j, 0))
    return pl.pallas_call(
        functools.partial(_by_qkv, n, same),
        grid_spec=pltpu.PrefetchScalarGridSpec(
            num_scalar_prefetch=1,
            grid=(D // tile,),
            in_specs=[pl.BlockSpec((PIECE, tile), lambda j, blocks: (0, j))] * n
            + [whole((ROWS // 2, MINE)), whole((ROWS // 2, 2 * MINE))] * 2,
            out_specs=[out] * 3,
        ),
        out_shape=[jax.ShapeDtypeStruct((D, MINE), BF)] * 3,
        compiler_params=params(),
        cost_estimate=pl.CostEstimate(flops=2 * ROWS * D * 3 * MINE, bytes_accessed=26 * 2**20, transcendentals=0),
        name="by_qkv",
    )(blocks, *pieces, dqm, dkvm, dqt, dkvt)


def _by_wo(n, blocks, *refs):
    pieces, (o, g) = refs[:n], refs[n:]
    total = None
    for at in range(0, n, 4):
        dy = jnp.concatenate([pieces[i][...] for i in range(at, at + 4)], 0)
        seen = jnp.concatenate([o[pl.ds(pl.multiple_of(blocks[i] * PIECE, PIECE), PIECE), :] for i in range(at, at + 4)], 0)
        t = dot(seen, dy, 0, 0)
        total = t if total is None else total + t
    g[...] = total.astype(BF)


def by_wo(pieces, blocks, o):
    n = len(pieces)
    tile = 512
    return pl.pallas_call(
        functools.partial(_by_wo, n),
        grid_spec=pltpu.PrefetchScalarGridSpec(
            num_scalar_prefetch=1,
            grid=(D // tile,),
            in_specs=[pl.BlockSpec((PIECE, tile), lambda j, blocks: (0, j))] * n + [whole((ROWS, MINE))],
            out_specs=pl.BlockSpec((MINE, tile), lambda j, blocks: (0, j)),
        ),
        out_shape=jax.ShapeDtypeStruct((MINE, D), BF),
        compiler_params=params(),
        cost_estimate=pl.CostEstimate(flops=2 * ROWS * D * MINE, bytes_accessed=19 * 2**20, transcendentals=0),
        name="by_wo",
    )(blocks, *pieces, o)


CORE, Y, X = 1, 2, 4


def swap(t, flip):
    return lax.ppermute(t, "tp", [(i, i ^ flip) for i in range(8)])


def gather(lo, hi):
    x0, y1 = swap(lo, X), swap(hi, Y)
    x1, y0 = swap(hi, X), swap(lo, Y)
    c0, c1 = swap(lo, CORE), swap(hi, CORE)
    d0, d1 = swap(x0, Y), swap(y1, X)
    near = [(lo, (0, 0)), (hi, (0, 1)), (c0, (1, 0)), (c1, (1, 1))]
    mid = [(x0, (4, 0)), (x1, (4, 1)), (y0, (2, 0)), (y1, (2, 1))]
    mid += [(swap(t, CORE), (f ^ 1, h)) for t, (f, h) in mid]
    far = [(d0, (6, 0)), (d1, (6, 1))]
    far += [(swap(t, CORE), (f ^ 1, h)) for t, (f, h) in far]
    return near, mid, far


def solution(mesh):
    def step(x, dy, gain, wq, wk, wv, wo):
        tabs = tables()
        me = lax.axis_index("tp")
        core, chip = me & 1, me >> 1
        number = lambda group: jnp.stack([(me ^ f) * 2 + h for _, (f, h) in group]).astype(jnp.int32)
        place = lambda flip, h: ((me ^ flip) >> 1) * 2 + h

        lo, hi = norm(x, gain)
        near, mid, far = gather(lo, hi)
        near_y, mid_y, far_y = gather(dy[:PIECE], dy[PIECE:])
        theirs = [swap(w, CORE) for w in (wq, wk, wv)]

        qkv = project(None, [t for t, _ in near], number(near), wq, wk, wv, tabs)
        qkv = project(qkv, [t for t, _ in mid], number(mid), wq, wk, wv, tabs)
        qkv = project(qkv, [t for t, _ in far], number(far), wq, wk, wv, tabs)
        o, lse = attend(qkv)

        d_out = lift(None, [t for t, _ in near_y + mid_y], number(near_y + mid_y), wo)
        state = back(jnp.stack([chip, chip ^ 1, chip ^ 2, core]), 3, qkv, d_out, o, lse, tabs, None, False)
        d_out = lift(d_out, [t for t, _ in far_y], number(far_y), wo)
        dqm, dqt, dkvm, dkvt = back(jnp.stack([chip ^ 3, core]), 1, qkv, d_out, o, lse, tabs, state, True)

        grads = (dqm, dkvm, swap(dqt, CORE), swap(dkvt, CORE))
        weights = (wq, wk, wv, *theirs)
        d_lo, d_hi = terms(jnp.stack([place(6, 0), place(6, 1)]), 2, grads, weights)
        from_y, from_x = swap(d_lo, Y), swap(d_hi, X)
        x_hi, y_lo = terms(jnp.stack([place(4, 1), place(2, 0)]), 2, grads, weights)
        got_x_hi, got_y_lo = swap(x_hi, X), swap(y_lo, Y)
        x_lo, y_hi = terms(jnp.stack([place(4, 0), place(2, 1)]), 2, grads, weights, (from_y, from_x))
        got_x_lo, got_y_hi = swap(x_lo, X), swap(y_hi, Y)

        everything = near + mid + far
        same = [f & 1 == 0 for _, (f, _) in everything]
        places = jnp.stack([place(f, h) for _, (f, h) in everything])
        by_wq, by_wk, by_wv = by_qkv([t for t, _ in everything], same, places, dqm, dkvm, dqt, dkvt)
        everything = near_y + mid_y + far_y
        g_wo = by_wo([t for t, _ in everything], number(everything), o)

        got = [jnp.stack([got_x_lo, got_x_hi]), jnp.stack([got_y_lo, got_y_hi])]
        by_x, by_gain = end(jnp.stack([chip]), grads, weights, got, x, dy, gain)
        for flip in (CORE, Y, X):
            by_gain = by_gain + swap(by_gain, flip)
        return by_x, by_gain, by_wq, by_wk, by_wv, g_wo

    tokens, columns = P(("dp", "tp"), None), P(None, "tp")
    return jax.shard_map(
        step,
        mesh=mesh,
        in_specs=(tokens, tokens, P(None), columns, columns, columns, P("tp", None)),
        out_specs=(tokens, P("dp", None), P("dp", "tp"), P("dp", "tp"), P("dp", "tp"), P(("dp", "tp"), None)),
        check_vma=False,
    )
```

```python
import jax
import jax.numpy as jnp
import numpy as np
from jax import lax
from jax.experimental import pallas as pl
from jax.experimental.pallas import tpu as pltpu
from jax.sharding import PartitionSpec as P

HEAD = 128
THETA = 10000
LOG2E = 1.4426950408889634
NEG, HIDDEN = -1e30, -2e30
ROWS, D, MINE = 4096, 2048, 256
PIECE = 256
KEYS = 512
CHIP = 1024
SOME = 64
WIDE = 512
SCALE = HEAD**-0.5
E = SCALE * LOG2E
BF, F32 = jnp.bfloat16, jnp.float32
TWO = range(2)
MESH = pl.DeviceIdType.MESH


def tables():
    half = HEAD // 2
    freq = float(THETA) ** (-np.arange(half) / half)
    both = lambda t: np.concatenate([t, t], 1).astype(np.float32)
    near = np.arange(PIECE)[:, None] * freq
    far = np.arange(0, ROWS, PIECE)[:, None] * freq
    return tuple(jnp.asarray(both(f(t))) for t in (near, far) for f in (np.cos, np.sin))


def dot(a, b, ca=1, cb=0):
    return lax.dot_general(a, b, (((ca,), (cb,)), ((), ())), preferred_element_type=F32)


def span(start, size):
    return pl.ds(pl.multiple_of(start, size), size)


def lanes(h, base=0):
    return slice(base + h * HEAD, base + (h + 1) * HEAD)


def turn(t, cos, sin):
    return t * cos + pltpu.roll(t, HEAD // 2, 1) * sin


def causal(s, hidden):
    ok = lax.broadcasted_iota(jnp.int32, s.shape, 1) >= lax.broadcasted_iota(jnp.int32, s.shape, 0)
    return jnp.where(ok, s, hidden)


def flipped(at, f):
    return lax.rem(at + f, 2)


class Place:
    def __init__(self, x, y, core):
        self.x, self.y, self.core = x, y, core

    def beside(self, fx, fy, fc):
        return Place(flipped(self.x, fx), flipped(self.y, fy), flipped(self.core, fc))

    def device(self):
        return 2 * self.chip() + self.core

    def chip(self):
        return 2 * self.x + self.y

    def id(self):
        return {"tp": self.device()}

    def seen(self, r):
        return self.beside(lax.rem(r, 2), lax.div(r, 2), 0).chip()

    def piece(self, group, i):
        odd, core = i % 2, i // 2
        if group == 0:
            return self.rows((0, 0, core), odd)
        if group == 3:
            return self.rows((1, 1, core), odd)
        return self.rows((1 - odd, odd, core), odd if group == 1 else 1 - odd)

    def rows(self, to, half):
        return span((2 * self.beside(*to).device() + half) * PIECE, PIECE)


OWN, XN, YN, CN, ACROSS = (0, 0, 0), (1, 0, 0), (0, 1, 0), (0, 0, 1), (1, 1, 0)
SENDS = [(0, 1, 0, XN), (1, 1, 1, YN), (0, 0, 2, CN), (1, 0, 3, CN), (1, 2, 0, XN), (0, 2, 1, YN)]
FORWARDS = {1: [(0, 3, 0, YN), (1, 3, 1, XN), (0, 1, 2, CN), (1, 1, 3, CN)], 2: [(0, 2, 2, CN), (1, 2, 3, CN)], 3: [(0, 3, 2, CN), (1, 3, 3, CN)]}


class Gather:
    def __init__(self, place, own, buf, sends, recvs, local, stage, loads):
        self.place, self.own, self.buf, self.sends, self.recvs, self.local = place, own, buf, sends, recvs, local
        self.stage, self.loads = stage, loads

    def copy(self, src, group, i, to):
        there = self.place.beside(*to)
        at = self.buf.at[there.piece(group, i), :]
        slot = 4 * group + i
        return pltpu.make_async_remote_copy(src_ref=at if src is None else src, dst_ref=at, send_sem=self.sends.at[slot],
                                            recv_sem=self.recvs.at[slot], device_id=there.id(), device_id_type=MESH)

    def kept(self):
        return [pltpu.make_async_copy(self.own.at[h], self.buf.at[self.place.rows(OWN, h), :], self.local.at[h]) for h in TWO]

    def begin(self):
        for h, group, i, to in SENDS:
            self.copy(self.own.at[h], group, i, to).start()
        for c in self.kept():
            c.start()

    def arrived(self, group, i):
        at = self.buf.at[self.place.piece(group, i), :]
        slot = 4 * group + i
        pltpu.make_async_remote_copy(src_ref=at, dst_ref=at, send_sem=self.sends.at[slot], recv_sem=self.recvs.at[slot],
                                     device_id=self.place.beside(*XN).id(), device_id_type=MESH).wait_recv()

    def forward(self, group):
        for i in TWO:
            self.arrived(group, i)
        for i, g, n, to in FORWARDS[group]:
            self.copy(self.buf.at[self.place.piece(group, i), :], g, n, to).start()

    def sent(self):
        for h, group, i, to in SENDS:
            self.copy(self.own.at[h], group, i, to).wait_send()
        for at, todo in FORWARDS.items():
            for i, g, n, to in todo:
                self.copy(self.buf.at[self.place.piece(at, i), :], g, n, to).wait_send()

    def work(self, group, do):
        def load(i):
            slot = lax.rem(i, 2)
            return pltpu.make_async_copy(self.buf.at[self.place.piece(group, i), :], self.stage.at[slot], self.loads.at[slot])

        if group == 0:
            for c in self.kept():
                c.wait()
        load(jnp.int32(0)).start()

        def body(i, _):
            @pl.when(i < 3)
            def _():
                @pl.when(i >= 1)
                def _():
                    self.arrived(group, i + 1)

                load(i + 1).start()

            load(i).wait()
            do(lax.rem(i, 2), self.place.piece(group, i).start // PIECE)

        lax.fori_loop(0, 4, body, None)


def _step(x_ref, dy_ref, gain_ref, wq, wk, wv, wo, nc, ns, fc, fs,
          ga, gy, landing, dx_out, gq_out, gk_out, gv_out, gwo_out, gain_out,
          own, stage, qkv, do_s, vt, kt, top_s, lse_s, delta_s, acc, dq_s, grad, theirs, uq, uk, uv, dgain,
          send_a, send_y, recv_a, recv_y, local, loads, send_w, recv_w, send_g, recv_g, send_r, recv_r, send_n, recv_n, outs):
    me = lax.axis_index("tp")
    place = Place(lax.div(me, 4), lax.rem(lax.div(me, 2), 2), lax.rem(me, 2))
    others = [place.beside(n // 4, n // 2 % 2, n % 2) for n in range(1, 8)]
    barrier = pltpu.get_barrier_semaphore()
    for there in others:
        pl.semaphore_signal(barrier, inc=1, device_id=there.id(), device_id_type=MESH)
    pl.semaphore_wait(barrier, len(others))

    a_all = Gather(place, own.at[0], ga, send_a, recv_a, local.at[0], stage, loads)
    y_all = Gather(place, own.at[1], gy, send_y, recv_y, local.at[1], stage, loads)

    def push(src, dst, to, sends, recvs, slot):
        return pltpu.make_async_remote_copy(src_ref=src, dst_ref=dst, send_sem=sends.at[slot], recv_sem=recvs.at[slot],
                                            device_id=place.beside(*to).id(), device_id_type=MESH)

    def angles(block):
        far_c, far_s = fc[pl.ds(block, 1), :], fs[pl.ds(block, 1), :]
        near_c, near_s = nc[...], ns[...]
        sign = jnp.where(lax.broadcasted_iota(jnp.int32, (1, HEAD), 1) < HEAD // 2, -1.0, 1.0)
        return near_c * far_c - near_s * far_s, (near_s * far_c + near_c * far_s) * sign

    def project(slot, block):
        a = stage[slot]
        cos, sin = angles(block)
        rows = span(block * PIECE, PIECE)
        for at, w in ((0, wq), (MINE, wk)):
            t = dot(a, w[...]).astype(BF).astype(F32)
            for h in TWO:
                got = turn(t[:, lanes(h)], cos, sin).astype(BF)
                qkv[rows, lanes(h, at)] = got
                if at:
                    kt[h, :, rows] = got.T
        v = dot(a, wv[...]).astype(BF)
        qkv[rows, 2 * MINE :] = v
        for h in TWO:
            vt[h, :HEAD, rows] = v[:, lanes(h)].T

    def lift(slot, block):
        rows = span(block * PIECE, PIECE)
        got = dot(stage[slot], wo[...], 1, 1).astype(BF)
        do_s[rows, :] = got
        for h in TWO:
            both = got[:, lanes(h)].astype(F32).T * vt[h, :HEAD, rows].astype(F32)
            delta_s[h : h + 1, rows] = both.sum(axis=0, keepdims=True)

    def attend(chip, at, strips):
        keys = span(at, KEYS)
        pieces = [(h, s, m) for s, m in strips for h in TWO]
        scores = [dot(qkv[keys, lanes(h, MINE)], qkv[span(chip * CHIP + s * KEYS, KEYS), lanes(h)], 1, 1) for h, s, _ in pieces]
        weights, keeps = [], []
        for (h, s, masked), score in zip(pieces, scores):
            if masked:
                score = causal(score, HIDDEN)
            n = 2 * s + h
            old = top_s[chip, n : n + 1, :]
            top = jnp.maximum(old, score.max(axis=0, keepdims=True))
            top_s[chip, n : n + 1, :] = top
            weights.append(jnp.exp2((score - top) * E).astype(BF))
            keeps.append(jnp.exp2((old - top) * E))
        for (h, s, _), p, keep in zip(pieces, weights, keeps):
            here = pl.ds(pl.multiple_of((4 * chip + 2 * s + h) * MINE, MINE), HEAD + 16)
            acc[here, :] = acc[here, :] * keep + dot(vt[h, :, keys], p)

    def attend_pair(q, k):
        lax.fori_loop(0, 2, lambda n, _: attend(q, k * CHIP + n * KEYS, [(0, False), (1, False)]), None)

    def attend_self(q):
        attend(q, q * CHIP, [(0, True), (1, False)])
        attend(q, q * CHIP + KEYS, [(1, True)])

    def attended(chip, _):
        for s in TWO:
            for h in TWO:
                n = 2 * s + h
                base = pl.multiple_of((4 * chip + n) * MINE, MINE)
                total = acc[pl.ds(base + HEAD, 8), :][:1]
                rows = span(chip * CHIP + s * KEYS, KEYS)
                vt[h, :HEAD, rows] = (acc[pl.ds(base, HEAD), :] * (1 / total)).astype(BF)
                lse_s[h : h + 1, rows] = top_s[chip, n : n + 1, :] * E + jnp.log2(total)

    def back(chip, at, strip, masked):
        here = span(at, KEYS)
        rows = span(chip * CHIP + strip * KEYS, KEYS)
        qs = [qkv[rows, lanes(h)] for h in TWO]
        dos = [do_s[rows, lanes(h)] for h in TWO]
        scores = [dot(qkv[here, lanes(h, MINE)], qs[h], 1, 1) for h in TWO]
        dps = [dot(qkv[here, lanes(h, 2 * MINE)], dos[h], 1, 1) for h in TWO]
        for h in TWO:
            p = jnp.exp2(scores[h] * E - lse_s[h : h + 1, rows])
            if masked:
                p = causal(p, 0.0)
            ds = (p * (dps[h] - delta_s[h : h + 1, rows])).astype(BF)
            acc[here, lanes(h, MINE)] += dot(p.astype(BF), dos[h])
            acc[here, lanes(h)] += dot(ds, qs[h])
            dq_s[h, :, rows] += dot(kt[h, :, here], ds)

    def back_pair(q, k):
        lax.fori_loop(0, 4, lambda t, _: back(q, k * CHIP + lax.div(t, 2) * KEYS, lax.rem(t, 2), False), None)

    def back_self(q):
        lax.fori_loop(0, 2, lambda n, _: back(q, q * CHIP + n * KEYS, n, True), None)
        back(q, q * CHIP, 1, False)

    def pairs(do, count, first, second):
        def body(t, _):
            a, b = place.seen(first(t)), place.seen(second(t))
            do(jnp.maximum(a, b), jnp.minimum(a, b))

        lax.fori_loop(0, count, body, None)

    def near(pair):
        pairs(pair, 3, lambda t: lax.div(t, 2), lambda t: t - lax.div(t, 2) + 1)

    def far(pair):
        pairs(pair, 3, lambda t: t, lambda t: jnp.int32(3))

    def alone(one, first, last):
        lax.fori_loop(first, last, lambda r, _: one(place.seen(r)), None)

    def hats(at):
        wide = x_ref[pl.ds(at, SOME), :].astype(F32)
        scale = lax.rsqrt(jnp.mean(wide * wide, -1, keepdims=True) + 1e-6)
        return wide * scale, scale

    def normed(n, _):
        for h in TWO:
            here = span(n * SOME, SOME)
            own[0, h, here, :] = (hats(h * PIECE + n * SOME)[0] * gain_ref[...].astype(F32)).astype(BF)

    lax.fori_loop(0, PIECE // SOME, normed, None)
    a_all.begin()
    fetch = [pltpu.make_async_copy(dy_ref.at[pl.ds(h * PIECE, PIECE)], own.at[1, h], local.at[1, h]) for h in TWO]
    for c in fetch:
        c.start()
    swaps = [push(w, u, CN, send_w, recv_w, n) for n, (w, u) in enumerate(((wq, uq), (wk, uk), (wv, uv)))]
    for c in swaps:
        c.start()
    top_s[...] = jnp.full(top_s.shape, NEG, F32)
    acc[...] = jnp.zeros(acc.shape, F32)
    for h in TWO:
        vt[h, HEAD:, :] = jnp.ones((16, ROWS), BF)
    for c in fetch:
        c.wait()

    a_all.work(0, project)
    a_all.forward(1)
    y_all.begin()
    a_all.work(1, project)
    a_all.forward(2)
    a_all.work(2, project)
    near(attend_pair)
    alone(attend_self, 0, 3)
    a_all.forward(3)
    a_all.work(3, project)
    far(attend_pair)
    alone(attend_self, 3, 4)
    lax.fori_loop(0, 4, attended, None)
    acc[...] = jnp.zeros(acc.shape, F32)
    dq_s[...] = jnp.zeros(dq_s.shape, F32)

    y_all.work(0, lift)
    y_all.forward(1)
    alone(back_self, 0, 1)
    y_all.work(1, lift)
    y_all.forward(2)
    y_all.work(2, lift)
    near(back_pair)
    alone(back_self, 1, 3)
    y_all.forward(3)
    y_all.work(3, lift)
    far(back_pair)
    alone(back_self, 3, 4)
    a_all.sent()
    y_all.sent()

    def finish(block):
        cos, sin = angles(block)
        rows = span(block * PIECE, PIECE)
        for h in TWO:
            grad[rows, lanes(h)] = turn((dq_s[h, :, rows] * SCALE).T, cos, -sin).astype(BF)
            grad[rows, lanes(h, MINE)] = turn(acc[rows, lanes(h)] * SCALE, cos, -sin).astype(BF)
        grad[rows, 2 * MINE :] = acc[rows, MINE:].astype(BF)

    def trade(r, core):
        chip = place.seen(r)
        return push(grad.at[span(chip * CHIP + core * KEYS, KEYS), :], theirs.at[chip], CN, send_g, recv_g, r)

    def finish_chip(r, core):
        for n in TWO:
            finish(place.seen(r) * (CHIP // PIECE) + core * (KEYS // PIECE) + n)

    def outward(n, _):
        finish_chip(3 - n, 1 - place.core)
        trade(3 - n, 1 - place.core).start()

    lax.fori_loop(0, 4, outward, None)
    lax.fori_loop(0, 4, lambda n, _: finish_chip(3 - n, place.core), None)
    for c in swaps:
        c.wait()

    def product(to, start, size, cols):
        there = place.beside(*to)
        mine = grad[pl.ds(pl.multiple_of(there.device() * KEYS + start, PIECE), size), :]
        other = theirs[there.chip(), pl.ds(start, size), :]
        total = None
        for g, ws in ((mine, (wq, wk, wv)), (other, (uq, uk, uv))):
            for n, w in enumerate(ws):
                t = dot(g[:, n * MINE : (n + 1) * MINE], w[cols, :], 1, 1)
                total = t if total is None else total + t
        return total

    def columns(do):
        lax.fori_loop(0, D // WIDE, lambda j, _: do(span(j * WIDE, WIDE)), None)

    def scatter(slot, src, to):
        return push(src, landing.at[slot], to, send_r, recv_r, slot)

    def landed(slot, dst):
        scatter(slot, landing.at[slot], XN).wait_recv()
        c = pltpu.make_async_copy(landing.at[slot], dst, loads.at[0])
        c.start()
        c.wait()

    def both(cols):
        t = product(ACROSS, 0, KEYS, cols).astype(BF)
        own[0, 0, :, cols] = t[:PIECE]
        own[0, 1, :, cols] = t[PIECE:]

    def direct(cols):
        own[1, 0, :, cols] = product(XN, PIECE, PIECE, cols).astype(BF)
        own[1, 1, :, cols] = product(YN, 0, PIECE, cols).astype(BF)

    def joined(cols):
        stage[0, :, cols] = (product(XN, 0, PIECE, cols) + own[0, 0, :, cols].astype(F32)).astype(BF)
        stage[1, :, cols] = (product(YN, PIECE, PIECE, cols) + own[0, 1, :, cols].astype(F32)).astype(BF)

    routes = [(own.at[0, 0], YN), (own.at[0, 1], XN), (own.at[1, 0], XN), (own.at[1, 1], YN), (stage.at[0], XN), (stage.at[1], YN)]
    moves = [scatter(n, src, to) for n, (src, to) in enumerate(routes)]

    trade(3, 1 - place.core).wait_recv()
    columns(both)
    for c in moves[:2]:
        c.start()
    for r in range(3):
        trade(r, 1 - place.core).wait_recv()
    columns(direct)
    for c in moves[2:4]:
        c.start()

    def tile(buf, j, slot):
        return pltpu.make_async_copy(buf.at[:, span(j * MINE, MINE)], qkv.at[:, pl.ds(slot * MINE, MINE)], loads.at[slot])

    def stream(buf, do):
        tile(buf, 0, 0).start()

        def body(n, _):
            for slot in TWO:
                j = 2 * n + slot

                @pl.when(j + 1 < D // MINE)
                def _():
                    tile(buf, j + 1, 1 - slot).start()

                tile(buf, j, slot).wait()
                do(j, qkv.at[:, slot * MINE : (slot + 1) * MINE])

        lax.fori_loop(0, D // MINE // 2, body, None)

    def by_wo(j, dy):
        for h in TWO:
            qkv[pl.ds(pl.multiple_of(D + j * MINE + h * HEAD, HEAD), HEAD), 2 * MINE :] = dot(vt[h, :HEAD, :], dy[...]).astype(BF)

    def by_qkv(j, a):
        t = sum(dot(a[n : n + CHIP, :], grad[n : n + CHIP, :], 0, 0) for n in range(0, ROWS, CHIP)).astype(BF)
        rows = span(j * MINE, MINE)
        do_s[rows, :] = t[:, :MINE]
        do_s[span(D + j * MINE, MINE), :] = t[:, MINE : 2 * MINE]
        qkv[rows, 2 * MINE :] = t[:, 2 * MINE :]

    stream(gy, by_wo)
    for n in TWO:
        moves[n].wait_send()
        landed(n, own.at[0, n])
    columns(joined)
    for c in moves[4:]:
        c.start()
    stream(ga, by_qkv)
    rest = 2 * MINE
    writes = [(do_s.at[:D], gq_out), (do_s.at[D:], gk_out), (qkv.at[:D, rest:], gv_out)]
    writes += [(qkv.at[D + j * MINE : D + (j + 1) * MINE, rest:], gwo_out.at[:, j * MINE : (j + 1) * MINE]) for j in range(D // MINE)]
    writes = [pltpu.make_async_copy(src, dst, outs.at[n]) for n, (src, dst) in enumerate(writes)]
    for c in writes:
        c.start()

    def mine(j, _):
        acc[span(j * WIDE, WIDE), :] = product(OWN, 0, KEYS, span(j * WIDE, WIDE))

    lax.fori_loop(0, D // WIDE, mine, None)
    for n in TWO:
        landed(2 + n, own.at[0, n])
    for c in moves[2:]:
        c.wait_send()
    again = [pltpu.make_async_copy(dy_ref.at[pl.ds(h * PIECE, PIECE)], own.at[1, h], local.at[1, h]) for h in TWO]
    for c in again:
        c.start()
    for n in TWO:
        landed(4 + n, stage.at[n])
    for c in again:
        c.wait()

    gain = gain_ref[...].astype(F32)
    dgain[0] = jnp.zeros(dgain.shape[1:], F32)
    for half in TWO:
        direct_in, joined_in = own.at[0, 1 - half], stage.at[half]

        def ended(n, _):
            here = span(n * SOME, SOME)
            at = half * PIECE + n * SOME
            da = jnp.concatenate([acc[pl.ds(j * WIDE + at, SOME), :] for j in range(D // WIDE)], 1)
            da = da + direct_in[here, :].astype(F32) + joined_in[here, :].astype(F32)
            hat, scale = hats(at)
            got = da * gain
            inner = jnp.mean(got * hat, -1, keepdims=True)
            stage[half, here, :] = (own[1, half, here, :].astype(F32) + (got - hat * inner) * scale).astype(BF)
            dgain[0] += (da * hat).sum(axis=0, keepdims=True)

        lax.fori_loop(0, PIECE // SOME, ended, None)
    tell = [push(dgain.at[0], dgain.at[n], (n // 4, n // 2 % 2, n % 2), send_n, recv_n, n) for n in range(1, 8)]
    for c in tell:
        c.start()
    results = [pltpu.make_async_copy(stage.at[h], dx_out.at[pl.ds(h * PIECE, PIECE)], local.at[0, h]) for h in TWO]
    for c in results:
        c.start()
    for c in tell + results:
        c.wait()
    total = [dgain[n] for n in range(8)]
    while len(total) > 1:
        total = [total[n] + total[n + 1] for n in range(0, len(total), 2)]
    gain_out[...] = total[0]
    for r in range(4):
        trade(r, 1 - place.core).wait_send()
    for c in writes:
        c.wait()


def solution(mesh):
    hbm, vmem = pl.BlockSpec(memory_space=pltpu.HBM), pl.BlockSpec(memory_space=pltpu.VMEM)
    shape = jax.ShapeDtypeStruct
    dma = lambda *n: pltpu.SemaphoreType.DMA(n)

    def step(x, dy, gain, wq, wk, wv, wo):
        rows, tall = shape((ROWS, D), BF), shape((D, MINE), BF)
        outs = pl.pallas_call(
            _step,
            in_specs=[vmem, hbm] + [vmem] * 9,
            out_specs=[hbm] * 8 + [vmem],
            out_shape=[rows, rows, shape((6, PIECE, D), BF), shape((KEYS, D), BF), tall, tall, tall, shape((MINE, D), BF), shape((1, D), F32)],
            scratch_shapes=[
                pltpu.VMEM((2, 2, PIECE, D), BF),
                pltpu.VMEM((2, PIECE, D), BF),
                pltpu.VMEM((ROWS, 3 * MINE), BF),
                pltpu.VMEM((ROWS, MINE), BF),
                pltpu.VMEM((2, HEAD + 16, ROWS), BF),
                pltpu.VMEM((2, HEAD, ROWS), BF),
                pltpu.VMEM((4, 4, KEYS), F32),
                pltpu.VMEM((2, ROWS), F32),
                pltpu.VMEM((2, ROWS), F32),
                pltpu.VMEM((ROWS, 2 * MINE), F32),
                pltpu.VMEM((2, HEAD, ROWS), F32),
                pltpu.VMEM((ROWS, 3 * MINE), BF),
                pltpu.VMEM((4, KEYS, 3 * MINE), BF),
                *[pltpu.VMEM((D, MINE), BF)] * 3,
                pltpu.VMEM((8, 1, D), F32),
                *[dma(16)] * 4, dma(2, 2), dma(2), dma(3), dma(3), dma(4), dma(4), dma(6), dma(6), dma(8), dma(8), dma(11),
            ],
            compiler_params=pltpu.CompilerParams(collective_id=0, has_side_effects=True, vmem_limit_bytes=67043328),
            cost_estimate=pl.CostEstimate(flops=80 * 10**9, bytes_accessed=2**27, transcendentals=2 * ROWS * ROWS),
            name="step",
        )(x, dy, gain[None], wq, wk, wv, wo, *tables())
        return outs[3], outs[8], *outs[4:8]

    tokens, columns = P(("dp", "tp"), None), P(None, "tp")
    return jax.shard_map(
        step,
        mesh=mesh,
        in_specs=(tokens, tokens, P(None), columns, columns, columns, P("tp", None)),
        out_specs=(tokens, P("dp", None), P("dp", "tp"), P("dp", "tp"), P("dp", "tp"), P(("dp", "tp"), None)),
        check_vma=False,
    )
```

```python
import jax
import jax.numpy as jnp
import numpy as np
from jax import lax
from jax.experimental import pallas as pl
from jax.experimental.pallas import tpu as pltpu
from jax.sharding import PartitionSpec as P

HEAD = 128
THETA = 10000
LOG2E = 1.4426950408889634
NEG, HIDDEN = -1e30, -2e30
ROWS, D, MINE = 4096, 2048, 256
PIECE = 256
KEYS = 512
CHIP = 1024
SOME = 32
WIDE = 512
SCALE = HEAD**-0.5
E = SCALE * LOG2E
BF, F32 = jnp.bfloat16, jnp.float32
TWO = range(2)
MESH = pl.DeviceIdType.MESH


def tables():
    half = HEAD // 2
    freq = float(THETA) ** (-np.arange(half) / half)
    both = lambda t: np.concatenate([t, t], 1).astype(np.float32)
    near = np.arange(PIECE)[:, None] * freq
    far = np.arange(0, ROWS, PIECE)[:, None] * freq
    return tuple(jnp.asarray(both(f(t))) for t in (near, far) for f in (np.cos, np.sin))


def dot(a, b, ca=1, cb=0):
    return lax.dot_general(a, b, (((ca,), (cb,)), ((), ())), preferred_element_type=F32)


def span(start, size):
    return pl.ds(pl.multiple_of(start, size), size)


def lanes(h, base=0):
    return slice(base + h * HEAD, base + (h + 1) * HEAD)


def turn(t, cos, sin):
    return t * cos + pltpu.roll(t, HEAD // 2, 1) * sin


def causal(s, hidden):
    ok = lax.broadcasted_iota(jnp.int32, s.shape, 1) >= lax.broadcasted_iota(jnp.int32, s.shape, 0)
    return jnp.where(ok, s, hidden)


def flipped(at, f):
    return lax.rem(at + f, 2)


class Place:
    def __init__(self, x, y, core):
        self.x, self.y, self.core = x, y, core

    def beside(self, fx, fy, fc):
        return Place(flipped(self.x, fx), flipped(self.y, fy), flipped(self.core, fc))

    def device(self):
        return 2 * self.chip() + self.core

    def chip(self):
        return 2 * self.x + self.y

    def id(self):
        return {"tp": self.device()}

    def seen(self, r):
        return self.beside(lax.rem(r, 2), lax.div(r, 2), 0).chip()

    def piece(self, group, i):
        odd, core = i % 2, i // 2
        if group == 0:
            return self.rows((0, 0, core), odd)
        if group == 3:
            return self.rows((1, 1, core), odd)
        return self.rows((1 - odd, odd, core), odd if group == 1 else 1 - odd)

    def rows(self, to, half):
        return span((2 * self.beside(*to).device() + half) * PIECE, PIECE)


OWN, XN, YN, CN, ACROSS = (0, 0, 0), (1, 0, 0), (0, 1, 0), (0, 0, 1), (1, 1, 0)
FAR_SENDS = [(0, 1, 0, XN), (1, 1, 1, YN), (1, 2, 0, XN), (0, 2, 1, YN)]
NEAR_SENDS = [(0, 0, 2, CN), (1, 0, 3, CN)]
SENDS = FAR_SENDS + NEAR_SENDS
FORWARDS = {1: [(0, 3, 0, YN), (1, 3, 1, XN), (0, 1, 2, CN), (1, 1, 3, CN)], 2: [(0, 2, 2, CN), (1, 2, 3, CN)], 3: [(0, 3, 2, CN), (1, 3, 3, CN)]}


class Gather:
    def __init__(self, place, own, buf, sends, recvs, local, stage, loads):
        self.place, self.own, self.buf, self.sends, self.recvs, self.local = place, own, buf, sends, recvs, local
        self.stage, self.loads = stage, loads

    def copy(self, src, group, i, to):
        there = self.place.beside(*to)
        at = self.buf.at[there.piece(group, i), :]
        slot = 4 * group + i
        return pltpu.make_async_remote_copy(src_ref=at if src is None else src, dst_ref=at, send_sem=self.sends.at[slot],
                                            recv_sem=self.recvs.at[slot], device_id=there.id(), device_id_type=MESH)

    def kept(self):
        return [pltpu.make_async_copy(self.own.at[h], self.buf.at[self.place.rows(OWN, h), :], self.local.at[h]) for h in TWO]

    def keep(self):
        for c in self.kept():
            c.start()

    def begin(self, sends):
        for h, group, i, to in sends:
            self.copy(self.own.at[h], group, i, to).start()

    def arrived(self, group, i):
        at = self.buf.at[self.place.piece(group, i), :]
        slot = 4 * group + i
        pltpu.make_async_remote_copy(src_ref=at, dst_ref=at, send_sem=self.sends.at[slot], recv_sem=self.recvs.at[slot],
                                     device_id=self.place.beside(*XN).id(), device_id_type=MESH).wait_recv()

    def forward(self, group):
        for i in TWO:
            self.arrived(group, i)
        for i, g, n, to in FORWARDS[group]:
            self.copy(self.buf.at[self.place.piece(group, i), :], g, n, to).start()

    def sent(self):
        for h, group, i, to in SENDS:
            self.copy(self.own.at[h], group, i, to).wait_send()
        for at, todo in FORWARDS.items():
            for i, g, n, to in todo:
                self.copy(self.buf.at[self.place.piece(at, i), :], g, n, to).wait_send()

    def work(self, group, do):
        def load(i):
            slot = lax.rem(i, 2)
            return pltpu.make_async_copy(self.buf.at[self.place.piece(group, i), :], self.stage.at[slot], self.loads.at[slot])

        if group == 0:
            for c in self.kept():
                c.wait()
        load(jnp.int32(0)).start()

        def body(i, _):
            @pl.when(i < 3)
            def _():
                @pl.when(i >= 1)
                def _():
                    self.arrived(group, i + 1)

                load(i + 1).start()

            load(i).wait()
            do(lax.rem(i, 2), self.place.piece(group, i).start // PIECE)

        lax.fori_loop(0, 4, body, None)


def _step(x_ref, dy_ref, gain_ref, wq_in, wk_in, wv_in, wo_in, nc, ns, fc, fs,
          ga, gy, landing, dx_out, gq_out, gk_out, gv_out, gwo_out, gain_out,
          own, stage, qkv, do_s, vt, kt, top_s, lse_s, delta_s, acc, dq_s, grad, theirs, wq, wk, wv, wo, uq, uk, uv, dgain, told,
          send_a, send_y, recv_a, recv_y, local, loads, send_w, recv_w, send_g, recv_g, send_r, recv_r, send_n, recv_n, outs, given, last):
    me = lax.axis_index("tp")
    place = Place(lax.div(me, 4), lax.rem(lax.div(me, 2), 2), lax.rem(me, 2))
    others = [place.beside(n // 4, n // 2 % 2, n % 2) for n in range(1, 8)]
    barrier = pltpu.get_barrier_semaphore()
    for there in others:
        pl.semaphore_signal(barrier, inc=1, device_id=there.id(), device_id_type=MESH)
    fills = [(wo_in, stage.at[0]), (wq_in, wq), (wk_in, wk), (wv_in, wv)]
    fills = [pltpu.make_async_copy(src, dst, given.at[n]) for n, (src, dst) in enumerate(fills)]
    for c in fills:
        c.start()

    a_all = Gather(place, own.at[0], ga, send_a, recv_a, local.at[0], stage, loads)
    y_all = Gather(place, own.at[1], gy, send_y, recv_y, local.at[1], stage, loads)

    def push(src, dst, to, sends, recvs, slot):
        return pltpu.make_async_remote_copy(src_ref=src, dst_ref=dst, send_sem=sends.at[slot], recv_sem=recvs.at[slot],
                                            device_id=place.beside(*to).id(), device_id_type=MESH)

    def angles(block):
        far_c, far_s = fc[pl.ds(block, 1), :], fs[pl.ds(block, 1), :]
        near_c, near_s = nc[...], ns[...]
        sign = jnp.where(lax.broadcasted_iota(jnp.int32, (1, HEAD), 1) < HEAD // 2, -1.0, 1.0)
        return near_c * far_c - near_s * far_s, (near_s * far_c + near_c * far_s) * sign

    def project(slot, block):
        a = stage[slot]
        cos, sin = angles(block)
        rows = span(block * PIECE, PIECE)
        for at, w in ((0, wq), (MINE, wk)):
            t = dot(a, w[...]).astype(BF).astype(F32)
            for h in TWO:
                got = turn(t[:, lanes(h)], cos, sin).astype(BF)
                qkv[rows, lanes(h, at)] = got
                if at:
                    kt[h, :, rows] = got.T
        v = dot(a, wv[...]).astype(BF)
        qkv[rows, 2 * MINE :] = v
        for h in TWO:
            vt[h, :HEAD, rows] = v[:, lanes(h)].T

    def lift(slot, block):
        rows = span(block * PIECE, PIECE)
        do_s[rows, :] = dot(stage[slot], wo[...]).astype(BF)

    def prepare(chip):
        for s in TWO:
            rows = span(chip * CHIP + s * KEYS, KEYS)
            for h in TWO:
                both = do_s[rows, lanes(h)].astype(F32).T * vt[h, :HEAD, rows].astype(F32)
                delta_s[h : h + 1, rows] = both.sum(axis=0, keepdims=True)

    def attend(chip, at, strips):
        keys = span(at, KEYS)
        pieces = [(h, s, m) for s, m in strips for h in TWO]
        scores = [dot(qkv[keys, lanes(h, MINE)], qkv[span(chip * CHIP + s * KEYS, KEYS), lanes(h)], 1, 1) for h, s, _ in pieces]
        weights, keeps = [], []
        for (h, s, masked), score in zip(pieces, scores):
            if masked:
                score = causal(score, HIDDEN)
            n = 2 * s + h
            old = top_s[chip, n : n + 1, :]
            top = jnp.maximum(old, score.max(axis=0, keepdims=True))
            top_s[chip, n : n + 1, :] = top
            weights.append(jnp.exp2((score - top) * E).astype(BF))
            keeps.append(jnp.exp2((old - top) * E))
        for (h, s, _), p, keep in zip(pieces, weights, keeps):
            here = pl.ds(pl.multiple_of((4 * chip + 2 * s + h) * MINE, MINE), HEAD + 16)
            acc[here, :] = acc[here, :] * keep + dot(vt[h, :, keys], p)

    def attend_pair(q, k):
        lax.fori_loop(0, 2, lambda n, _: attend(q, k * CHIP + n * KEYS, [(0, False), (1, False)]), None)

    def attend_self(q):
        attend(q, q * CHIP, [(0, True), (1, False)])
        attend(q, q * CHIP + KEYS, [(1, True)])

    def attended(chip, _):
        for s in TWO:
            for h in TWO:
                n = 2 * s + h
                base = pl.multiple_of((4 * chip + n) * MINE, MINE)
                total = acc[pl.ds(base + HEAD, 8), :][:1]
                rows = span(chip * CHIP + s * KEYS, KEYS)
                vt[h, :HEAD, rows] = (acc[pl.ds(base, HEAD), :] * (1 / total)).astype(BF)
                lse_s[h : h + 1, rows] = top_s[chip, n : n + 1, :] * E + jnp.log2(total)

    def back(chip, at, strip, masked):
        here = span(at, KEYS)
        rows = span(chip * CHIP + strip * KEYS, KEYS)
        qs = [qkv[rows, lanes(h)] for h in TWO]
        dos = [do_s[rows, lanes(h)] for h in TWO]
        scores = [dot(qkv[here, lanes(h, MINE)], qs[h], 1, 1) for h in TWO]
        dps = [dot(qkv[here, lanes(h, 2 * MINE)], dos[h], 1, 1) for h in TWO]
        for h in TWO:
            p = jnp.exp2(scores[h] * E - lse_s[h : h + 1, rows])
            if masked:
                p = causal(p, 0.0)
            ds = (p * (dps[h] - delta_s[h : h + 1, rows])).astype(BF)
            acc[here, lanes(h, MINE)] += dot(p.astype(BF), dos[h])
            acc[here, lanes(h)] += dot(ds, qs[h])
            dq_s[h, :, rows] += dot(kt[h, :, here], ds)

    def back_pair(q, k):
        lax.fori_loop(0, 4, lambda t, _: back(q, k * CHIP + lax.div(t, 2) * KEYS, lax.rem(t, 2), False), None)

    def back_self(q):
        lax.fori_loop(0, 2, lambda n, _: back(q, q * CHIP + n * KEYS, n, True), None)
        back(q, q * CHIP, 1, False)

    def pairs(do, count, first, second):
        def body(t, _):
            a, b = place.seen(first(t)), place.seen(second(t))
            do(jnp.maximum(a, b), jnp.minimum(a, b))

        lax.fori_loop(0, count, body, None)

    def near(pair):
        pairs(pair, 3, lambda t: lax.div(t, 2), lambda t: t - lax.div(t, 2) + 1)

    def far(pair, first, last):
        pairs(pair, last - first, lambda t: t + first, lambda t: jnp.int32(3))

    def alone(one, first, last):
        lax.fori_loop(first, last, lambda r, _: one(place.seen(r)), None)

    def hats(at):
        wide = x_ref[pl.ds(at, SOME), :].astype(F32)
        scale = lax.rsqrt(jnp.mean(wide * wide, -1, keepdims=True) + 1e-6)
        return wide * scale, scale

    def gain_row():
        return gain_ref[...].astype(F32).reshape(1, D)

    def normed(n, _):
        for h in TWO:
            here = span(n * SOME, SOME)
            own[0, h, here, :] = (hats(h * PIECE + n * SOME)[0] * gain_row()).astype(BF)

    lax.fori_loop(0, PIECE // SOME, normed, None)
    pl.semaphore_wait(barrier, len(others))
    a_all.begin(SENDS)
    a_all.keep()
    fetch = [pltpu.make_async_copy(dy_ref.at[pl.ds(h * PIECE, PIECE)], own.at[1, h], local.at[1, h]) for h in TWO]
    for c in fetch:
        c.start()
    swaps = [push(w, u, CN, send_w, recv_w, n) for n, (w, u) in enumerate(((wq_in, uq), (wk_in, uk), (wv_in, uv)))]
    for c in swaps:
        c.start()
    top_s[...] = jnp.full(top_s.shape, NEG, F32)
    acc[...] = jnp.zeros(acc.shape, F32)
    for h in TWO:
        vt[h, HEAD:, :] = jnp.ones((16, ROWS), BF)
    for c in fills:
        c.wait()
    wo[...] = stage[0].T
    for c in fetch:
        c.wait()
    y_all.begin(NEAR_SENDS)
    y_all.keep()

    a_all.work(0, project)
    alone(attend_self, 0, 1)
    y_all.work(0, lift)
    a_all.forward(1)
    y_all.begin(FAR_SENDS)
    a_all.work(1, project)
    a_all.forward(2)
    a_all.work(2, project)
    near(attend_pair)
    alone(attend_self, 1, 3)
    a_all.forward(3)
    a_all.work(3, project)
    far(attend_pair, 0, 3)
    alone(attend_self, 3, 4)
    lax.fori_loop(0, 4, attended, None)
    acc[...] = jnp.zeros(acc.shape, F32)
    dq_s[...] = jnp.zeros(dq_s.shape, F32)

    alone(prepare, 0, 1)
    alone(back_self, 0, 1)
    y_all.forward(1)
    y_all.work(1, lift)
    y_all.forward(2)
    y_all.work(2, lift)
    alone(prepare, 1, 3)
    near(back_pair)
    y_all.forward(3)
    alone(back_self, 1, 3)
    y_all.work(3, lift)
    alone(prepare, 3, 4)
    far(back_pair, 1, 3)
    a_all.sent()
    y_all.sent()

    def finish(block):
        cos, sin = angles(block)
        rows = span(block * PIECE, PIECE)
        for h in TWO:
            grad[rows, lanes(h)] = turn((dq_s[h, :, rows] * SCALE).T, cos, -sin).astype(BF)
            grad[rows, lanes(h, MINE)] = turn(acc[rows, lanes(h)] * SCALE, cos, -sin).astype(BF)
        grad[rows, 2 * MINE :] = acc[rows, MINE:].astype(BF)

    def block(r, core, half):
        return (place.seen(r) * 2 + core) * 2 + half

    def trade(r, half):
        there = theirs.at[place.seen(r), span(half * PIECE, PIECE), :]
        return push(grad.at[span(block(r, 1 - place.core, half) * PIECE, PIECE), :], there, CN, send_g, recv_g, 2 * r + half)

    def settle(r, half):
        finish(block(r, 1 - place.core, half))
        trade(r, half).start()
        finish(block(r, place.core, half))

    def product(to, start, size, cols):
        there = place.beside(*to)
        mine = grad[pl.ds(pl.multiple_of(there.device() * KEYS + start, PIECE), size), :]
        other = theirs[there.chip(), pl.ds(start, size), :]
        total = None
        for g, ws in ((mine, (wq, wk, wv)), (other, (uq, uk, uv))):
            for n, w in enumerate(ws):
                t = dot(g[:, n * MINE : (n + 1) * MINE], w[cols, :], 1, 1)
                total = t if total is None else total + t
        return total

    routes = [(own.at[0, 0], YN), (own.at[0, 1], XN), (own.at[1, 0], XN), (own.at[1, 1], YN), (stage.at[0], XN), (stage.at[1], YN)]

    def move(slot, j):
        src, to = routes[slot]
        cols = span(j * WIDE, WIDE)
        return push(src.at[:, cols], landing.at[slot, :, cols], to, send_r, recv_r, slot * (D // WIDE) + j)

    def take(slot, j, dst, sem):
        cols = span(j * WIDE, WIDE)
        move(slot, j).wait_recv()
        c = pltpu.make_async_copy(landing.at[slot, :, cols], dst.at[:, cols], sem)
        c.start()
        return c

    def columns(do):
        lax.fori_loop(0, D // WIDE, lambda j, _: do(j, span(j * WIDE, WIDE)), None)

    def both(j, cols):
        t = product(ACROSS, 0, KEYS, cols).astype(BF)
        for n in TWO:
            own[0, n, :, cols] = t[n * PIECE : (n + 1) * PIECE]
        for n in TWO:
            move(n, j).start()

    def direct(j, cols):
        own[1, 0, :, cols] = product(XN, PIECE, PIECE, cols).astype(BF)
        move(2, j).start()
        own[1, 1, :, cols] = product(YN, 0, PIECE, cols).astype(BF)
        move(3, j).start()

    def joined(j):
        cols = span(j * WIDE, WIDE)
        for n in TWO:
            move(n, j).wait_send()
        for c in [take(n, j, own.at[0, n], last.at[n]) for n in TWO]:
            c.wait()
        stage[0, :, cols] = (product(XN, 0, PIECE, cols) + own[0, 0, :, cols].astype(F32)).astype(BF)
        move(4, j).start()
        stage[1, :, cols] = (product(YN, PIECE, PIECE, cols) + own[0, 1, :, cols].astype(F32)).astype(BF)
        move(5, j).start()

    settle(1, 1)
    settle(2, 0)
    for c in swaps:
        c.wait()
    trade(1, 1).wait_recv()
    trade(2, 0).wait_recv()
    columns(direct)
    far(back_pair, 0, 1)
    alone(back_self, 3, 4)
    rest = [(3, 0), (3, 1), (1, 0), (2, 1), (0, 0), (0, 1)]
    for r, half in rest:
        settle(r, half)
    for r, half in rest:
        trade(r, half).wait_recv()
    columns(both)

    tiles = [(ga, qkv.at[:, :MINE]), (ga, qkv.at[:, MINE : 2 * MINE]), (gy, qkv.at[:, 2 * MINE :]), (gy, do_s)]
    results = [gq_out, gk_out, gv_out, gwo_out]

    def tile(j, slot):
        made = []
        for n in TWO:
            buf, dst = tiles[2 * n + slot]
            made.append(pltpu.make_async_copy(buf.at[:, span(j * MINE, MINE)], dst, loads.at[2 * n + slot]))
        return made

    def out(j, slot, n):
        to = results[n].at[:, :, span(j * MINE, MINE)] if n == 3 else results[n].at[pl.ds(2 * j, 2)]
        return pltpu.make_async_copy(kt.at[:, :, pl.ds((4 * slot + n) * MINE, MINE)], to, outs.at[4 * slot + n])

    for c in tile(0, 0):
        c.start()

    def stream(n, _):
        for slot in TWO:
            j = 2 * n + slot

            @pl.when(j + 1 < D // MINE)
            def _():
                for c in tile(j + 1, 1 - slot):
                    c.start()

            for c in tile(j, slot):
                c.wait()

            @pl.when(n > 0)
            def _():
                for i in range(4):
                    out(j - 2, slot, i).wait()

            a, dy = tiles[slot][1], tiles[2 + slot][1]
            t = sum(dot(a[k : k + CHIP, :], grad[k : k + CHIP, :], 0, 0) for k in range(0, ROWS, CHIP)).astype(BF)
            for h in TWO:
                for i in range(3):
                    kt[h, :, (4 * slot + i) * MINE : (4 * slot + i + 1) * MINE] = t[lanes(h), i * MINE : (i + 1) * MINE]
                kt[h, :, (4 * slot + 3) * MINE : (4 * slot + 4) * MINE] = dot(vt[h, :HEAD, :], dy[...]).astype(BF)
            for i in range(4):
                out(j, slot, i).start()
        joined(n)

    lax.fori_loop(0, D // WIDE, stream, None)

    def mine(j, cols):
        acc[cols, :] = product(OWN, 0, KEYS, cols)

    columns(mine)
    again = [pltpu.make_async_copy(dy_ref.at[pl.ds(h * PIECE, PIECE)], own.at[1, h], local.at[1, h]) for h in TWO]
    taken = []
    for j in range(D // WIDE):
        for n in TWO:
            move(2 + n, j).wait_send()
            taken.append(take(2 + n, j, own.at[0, n], last.at[2 + 4 * n + j]))
    for c in again:
        c.start()
    for j in range(D // WIDE):
        for n in TWO:
            move(4 + n, j).wait_send()
            taken.append(take(4 + n, j, stage.at[n], last.at[10 + 4 * n + j]))
    for c in taken + again:
        c.wait()

    gain = gain_row()
    dgain[...] = jnp.zeros(dgain.shape, F32)
    for half in TWO:
        direct_in, joined_in = own.at[0, 1 - half], stage.at[half]

        def ended(n, _):
            here = span(n * SOME, SOME)
            at = half * PIECE + n * SOME
            da = jnp.concatenate([acc[pl.ds(j * WIDE + at, SOME), :] for j in range(D // WIDE)], 1)
            da = da + direct_in[here, :].astype(F32) + joined_in[here, :].astype(F32)
            hat, scale = hats(at)
            got = da * gain
            inner = jnp.mean(got * hat, -1, keepdims=True)
            stage[half, here, :] = (own[1, half, here, :].astype(F32) + (got - hat * inner) * scale).astype(BF)
            dgain[...] += (da * hat).reshape(SOME // 8, 8, D).sum(axis=0)

        lax.fori_loop(0, PIECE // SOME, ended, None)
        pltpu.make_async_copy(stage.at[half], dx_out.at[pl.ds(half * PIECE, PIECE)], local.at[0, half]).start()
    told[0] = dgain[...].sum(axis=0, keepdims=True)
    tell = [push(told.at[0], told.at[n], (n // 4, n // 2 % 2, n % 2), send_n, recv_n, n) for n in range(1, 8)]
    for c in tell:
        c.start()
    for slot in TWO:
        for i in range(4):
            out(D // MINE - 2 + slot, slot, i).wait()
    for r in range(4):
        for half in TWO:
            trade(r, half).wait_send()
    for half in TWO:
        pltpu.make_async_copy(stage.at[half], dx_out.at[pl.ds(half * PIECE, PIECE)], local.at[0, half]).wait()
    for c in tell:
        c.wait()
    total = [told[n] for n in range(8)]
    while len(total) > 1:
        total = [total[n] + total[n + 1] for n in range(0, len(total), 2)]
    gain_out[...] = total[0]


def _hand(n, *refs):
    srcs, dsts, bufs, sems = refs[:n], refs[n : 2 * n], refs[2 * n : 3 * n], refs[3 * n]
    loads = [pltpu.make_async_copy(src, buf, sems.at[0, i]) for i, (src, buf) in enumerate(zip(srcs, bufs))]
    stores = [pltpu.make_async_copy(buf, dst, sems.at[1, i]) for i, (buf, dst) in enumerate(zip(bufs, dsts))]
    for c in loads:
        c.start()
    for load, store in zip(loads, stores):
        load.wait()
        store.start()
    for c in stores:
        c.wait()


def hand(arrays):
    hbm = pl.BlockSpec(memory_space=pltpu.HBM)
    n = len(arrays)
    return pl.pallas_call(
        lambda *refs: _hand(n, *refs),
        in_specs=[hbm] * n,
        out_specs=[hbm] * n,
        out_shape=[jax.ShapeDtypeStruct(t.shape, t.dtype) for t in arrays],
        scratch_shapes=[pltpu.VMEM(t.shape, t.dtype) for t in arrays] + [pltpu.SemaphoreType.DMA((2, n))],
        name="hand",
    )(*arrays)


def solution(mesh):
    hbm, vmem = pl.BlockSpec(memory_space=pltpu.HBM), pl.BlockSpec(memory_space=pltpu.VMEM)
    shape = jax.ShapeDtypeStruct
    dma = lambda *n: pltpu.SemaphoreType.DMA(n)

    def step(x, dy, gain, wq, wk, wv, wo):
        rows, tall = shape((ROWS, D), BF), shape((D // HEAD, HEAD, MINE), BF)
        outs = pl.pallas_call(
            _step,
            in_specs=[vmem, hbm, vmem] + [hbm] * 4 + [vmem] * 4,
            out_specs=[hbm] * 8 + [vmem],
            out_shape=[rows, rows, shape((6, PIECE, D), BF), shape((KEYS, D), BF), tall, tall, tall, shape((2, HEAD, D), BF), shape((1, D), F32)],
            scratch_shapes=[
                pltpu.VMEM((2, 2, PIECE, D), BF),
                pltpu.VMEM((2, PIECE, D), BF),
                pltpu.VMEM((ROWS, 3 * MINE), BF),
                pltpu.VMEM((ROWS, MINE), BF),
                pltpu.VMEM((2, HEAD + 16, ROWS), BF),
                pltpu.VMEM((2, HEAD, ROWS), BF),
                pltpu.VMEM((4, 4, KEYS), F32),
                pltpu.VMEM((2, ROWS), F32),
                pltpu.VMEM((2, ROWS), F32),
                pltpu.VMEM((ROWS, 2 * MINE), F32),
                pltpu.VMEM((2, HEAD, ROWS), F32),
                pltpu.VMEM((ROWS, 3 * MINE), BF),
                pltpu.VMEM((4, KEYS, 3 * MINE), BF),
                *[pltpu.VMEM((D, MINE), BF)] * 7,
                pltpu.VMEM((8, D), F32),
                pltpu.VMEM((8, 1, D), F32),
                *[dma(16)] * 4, dma(2, 2), *[dma(4)] * 3, *[dma(8)] * 2, *[dma(24)] * 2, *[dma(8)] * 3, dma(4), dma(18),
            ],
            compiler_params=pltpu.CompilerParams(collective_id=0, has_side_effects=True, vmem_limit_bytes=67043328),
            cost_estimate=pl.CostEstimate(flops=80 * 10**9, bytes_accessed=2**27, transcendentals=2 * ROWS * ROWS),
            name="step",
        )(x, dy, gain, wq, wk, wv, wo, *tables())
        dx, gq, gk, gv, gwo, dgain = hand(outs[3:])
        return dx, dgain, *[t.reshape(D, MINE) for t in (gq, gk, gv)], gwo.reshape(MINE, D)

    tokens, columns = P(("dp", "tp"), None), P(None, "tp")
    return jax.shard_map(
        step,
        mesh=mesh,
        in_specs=(tokens, tokens, P(None), columns, columns, columns, P("tp", None)),
        out_specs=(tokens, P("dp", None), P("dp", "tp"), P("dp", "tp"), P("dp", "tp"), P(("dp", "tp"), None)),
        check_vma=False,
    )
```

```python
import jax
import jax.numpy as jnp
import numpy as np
from jax import lax
from jax.experimental import pallas as pl
from jax.experimental.pallas import tpu as pltpu
from jax.sharding import PartitionSpec as P

HEAD = 128
THETA = 10000
LOG2E = 1.4426950408889634
NEG, HIDDEN = -1e30, -2e30
ROWS, D, MINE = 4096, 2048, 256
PIECE = 256
KEYS = 512
CHIP = 1024
SOME = 32
WIDE = 512
SCALE = HEAD**-0.5
E = SCALE * LOG2E
BF, F32 = jnp.bfloat16, jnp.float32
TWO = range(2)
MESH = pl.DeviceIdType.MESH


def tables():
    half = HEAD // 2
    freq = float(THETA) ** (-np.arange(half) / half)
    both = lambda t: np.concatenate([t, t], 1).astype(np.float32)
    near = np.arange(PIECE)[:, None] * freq
    far = np.arange(0, ROWS, PIECE)[:, None] * freq
    return tuple(jnp.asarray(both(f(t))) for t in (near, far) for f in (np.cos, np.sin))


def dot(a, b, ca=1, cb=0):
    return lax.dot_general(a, b, (((ca,), (cb,)), ((), ())), preferred_element_type=F32)


def span(start, size):
    return pl.ds(pl.multiple_of(start, size), size)


def lanes(h, base=0):
    return slice(base + h * HEAD, base + (h + 1) * HEAD)


def turn(t, cos, sin):
    return t * cos + pltpu.roll(t, HEAD // 2, 1) * sin


def causal(s, hidden):
    ok = lax.broadcasted_iota(jnp.int32, s.shape, 1) >= lax.broadcasted_iota(jnp.int32, s.shape, 0)
    return jnp.where(ok, s, hidden)


def flipped(at, f):
    return lax.rem(at + f, 2)


class Place:
    def __init__(self, x, y, core):
        self.x, self.y, self.core = x, y, core

    def beside(self, fx, fy, fc):
        return Place(flipped(self.x, fx), flipped(self.y, fy), flipped(self.core, fc))

    def device(self):
        return 2 * self.chip() + self.core

    def chip(self):
        return 2 * self.x + self.y

    def id(self):
        return {"tp": self.device()}

    def seen(self, r):
        return self.beside(lax.rem(r, 2), lax.div(r, 2), 0).chip()

    def piece(self, group, i):
        odd, core = i % 2, i // 2
        beyond = (group + 1) // 2
        far, one = beyond // 2, beyond % 2
        swapped = group // 2 - group // 3
        return self.rows((far + one * (1 - odd), far + one * odd, core), odd + swapped * (1 - 2 * odd))

    def rows(self, to, half):
        return span((2 * self.beside(*to).device() + half) * PIECE, PIECE)


OWN, XN, YN, CN, ACROSS = (0, 0, 0), (1, 0, 0), (0, 1, 0), (0, 0, 1), (1, 1, 0)
FAR_SENDS = [(0, 1, 0, XN), (1, 1, 1, YN), (1, 2, 0, XN), (0, 2, 1, YN)]
NEAR_SENDS = [(0, 0, 2, CN), (1, 0, 3, CN)]
SENDS = FAR_SENDS + NEAR_SENDS
FORWARDS = {1: [(0, 3, 0, YN), (1, 3, 1, XN), (0, 1, 2, CN), (1, 1, 3, CN)], 2: [(0, 2, 2, CN), (1, 2, 3, CN)], 3: [(0, 3, 2, CN), (1, 3, 3, CN)]}


class Gather:
    def __init__(self, place, own, buf, sends, recvs, local, stage, loads):
        self.place, self.own, self.buf, self.sends, self.recvs, self.local = place, own, buf, sends, recvs, local
        self.stage, self.loads = stage, loads

    def copy(self, src, group, i, to):
        there = self.place.beside(*to)
        at = self.buf.at[there.piece(group, i), :]
        slot = 4 * group + i
        return pltpu.make_async_remote_copy(src_ref=at if src is None else src, dst_ref=at, send_sem=self.sends.at[slot],
                                            recv_sem=self.recvs.at[slot], device_id=there.id(), device_id_type=MESH)

    def kept(self):
        return [pltpu.make_async_copy(self.own.at[h], self.buf.at[self.place.rows(OWN, h), :], self.local.at[h]) for h in TWO]

    def keep(self):
        for c in self.kept():
            c.start()

    def begin(self, sends):
        for h, group, i, to in sends:
            self.copy(self.own.at[h], group, i, to).start()

    def ready(self):
        for c in self.kept():
            c.wait()

    def arrived(self, group, i):
        at = self.buf.at[self.place.piece(group, i), :]
        slot = 4 * group + i
        pltpu.make_async_remote_copy(src_ref=at, dst_ref=at, send_sem=self.sends.at[slot], recv_sem=self.recvs.at[slot],
                                     device_id=self.place.beside(*XN).id(), device_id_type=MESH).wait_recv()

    def forward(self, group):
        for i in TWO:
            self.arrived(group, i)
        for i, g, n, to in FORWARDS[group]:
            self.copy(self.buf.at[self.place.piece(group, i), :], g, n, to).start()

    def sent(self):
        for h, group, i, to in SENDS:
            self.copy(self.own.at[h], group, i, to).wait_send()
        for at, todo in FORWARDS.items():
            for i, g, n, to in todo:
                self.copy(self.buf.at[self.place.piece(at, i), :], g, n, to).wait_send()

    def work(self, group, do):
        def load(i):
            slot = lax.rem(i, 2)
            return pltpu.make_async_copy(self.buf.at[self.place.piece(group, i), :], self.stage.at[slot], self.loads.at[slot])

        load(jnp.int32(0)).start()

        def body(i, _):
            @pl.when(i < 3)
            def _():
                @pl.when(i >= 1)
                def _():
                    self.arrived(group, i + 1)

                load(i + 1).start()

            load(i).wait()
            do(lax.rem(i, 2), self.place.piece(group, i).start // PIECE)

        lax.fori_loop(0, 4, body, None)


def _step(x_ref, dy_ref, gain_ref, wq_in, wk_in, wv_in, wo_in, nc, ns, fc, fs,
          ga, gy, landing, dx_out, gq_out, gk_out, gv_out, gwo_out, gain_out,
          own, stage, qkv, do_s, vt, kt, top_s, lse_s, delta_s, acc, dq_s, grad, theirs, wq, wk, wv, wo, uq, uk, uv, dgain, told,
          send_a, send_y, recv_a, recv_y, local, loads, send_w, recv_w, send_g, recv_g, send_r, recv_r, send_n, recv_n, outs, given, last):
    me = lax.axis_index("tp")
    place = Place(lax.div(me, 4), lax.rem(lax.div(me, 2), 2), lax.rem(me, 2))
    others = [place.beside(n // 4, n // 2 % 2, n % 2) for n in range(1, 8)]
    barrier = pltpu.get_barrier_semaphore()
    for there in others:
        pl.semaphore_signal(barrier, inc=1, device_id=there.id(), device_id_type=MESH)
    fills = [(wo_in, stage.at[0]), (wq_in, wq), (wk_in, wk), (wv_in, wv)]
    fills = [pltpu.make_async_copy(src, dst, given.at[n]) for n, (src, dst) in enumerate(fills)]
    for c in fills:
        c.start()

    a_all = Gather(place, own.at[0], ga, send_a, recv_a, local.at[0], stage, loads)
    y_all = Gather(place, own.at[1], gy, send_y, recv_y, local.at[1], stage, loads)

    def push(src, dst, to, sends, recvs, slot):
        return pltpu.make_async_remote_copy(src_ref=src, dst_ref=dst, send_sem=sends.at[slot], recv_sem=recvs.at[slot],
                                            device_id=place.beside(*to).id(), device_id_type=MESH)

    def angles(block):
        far_c, far_s = fc[pl.ds(block, 1), :], fs[pl.ds(block, 1), :]
        near_c, near_s = nc[...], ns[...]
        sign = jnp.where(lax.broadcasted_iota(jnp.int32, (1, HEAD), 1) < HEAD // 2, -1.0, 1.0)
        return near_c * far_c - near_s * far_s, (near_s * far_c + near_c * far_s) * sign

    def project(slot, block):
        a = stage[slot]
        cos, sin = angles(block)
        rows = span(block * PIECE, PIECE)
        for at, w in ((0, wq), (MINE, wk)):
            t = dot(a, w[...]).astype(BF).astype(F32)
            for h in TWO:
                got = turn(t[:, lanes(h)], cos, sin).astype(BF)
                qkv[rows, lanes(h, at)] = got
                if at:
                    kt[h, :, rows] = got.T
        v = dot(a, wv[...]).astype(BF)
        qkv[rows, 2 * MINE :] = v
        for h in TWO:
            vt[h, :HEAD, rows] = v[:, lanes(h)].T

    def lift(slot, block):
        rows = span(block * PIECE, PIECE)
        do_s[rows, :] = dot(stage[slot], wo[...]).astype(BF)

    def prepare(chip):
        for s in TWO:
            rows = span(chip * CHIP + s * KEYS, KEYS)
            for h in TWO:
                both = do_s[rows, lanes(h)].astype(F32).T * vt[h, :HEAD, rows].astype(F32)
                delta_s[h : h + 1, rows] = both.sum(axis=0, keepdims=True)

    def attend(chip, at, strips):
        keys = span(at, KEYS)
        pieces = [(h, s, m) for s, m in strips for h in TWO]
        scores = [dot(qkv[keys, lanes(h, MINE)], qkv[span(chip * CHIP + s * KEYS, KEYS), lanes(h)], 1, 1) for h, s, _ in pieces]
        weights, keeps = [], []
        for (h, s, masked), score in zip(pieces, scores):
            if masked:
                score = causal(score, HIDDEN)
            n = 2 * s + h
            old = top_s[chip, n : n + 1, :]
            top = jnp.maximum(old, score.max(axis=0, keepdims=True))
            top_s[chip, n : n + 1, :] = top
            weights.append(jnp.exp2((score - top) * E).astype(BF))
            keeps.append(jnp.exp2((old - top) * E))
        for (h, s, _), p, keep in zip(pieces, weights, keeps):
            here = pl.ds(pl.multiple_of((4 * chip + 2 * s + h) * MINE, MINE), HEAD + 16)
            acc[here, :] = acc[here, :] * keep + dot(vt[h, :, keys], p)

    def attend_pair(q, k):
        lax.fori_loop(0, 2, lambda n, _: attend(q, k * CHIP + n * KEYS, [(0, False), (1, False)]), None)

    def attend_self(q):
        attend(q, q * CHIP, [(0, True), (1, False)])
        attend(q, q * CHIP + KEYS, [(1, True)])

    def attended(chip, _):
        for s in TWO:
            for h in TWO:
                n = 2 * s + h
                base = pl.multiple_of((4 * chip + n) * MINE, MINE)
                total = acc[pl.ds(base + HEAD, 8), :][:1]
                rows = span(chip * CHIP + s * KEYS, KEYS)
                vt[h, :HEAD, rows] = (acc[pl.ds(base, HEAD), :] * (1 / total)).astype(BF)
                lse_s[h : h + 1, rows] = top_s[chip, n : n + 1, :] * E + jnp.log2(total)

    def back(chip, at, strip, masked):
        here = span(at, KEYS)
        rows = span(chip * CHIP + strip * KEYS, KEYS)
        qs = [qkv[rows, lanes(h)] for h in TWO]
        dos = [do_s[rows, lanes(h)] for h in TWO]
        scores = [dot(qkv[here, lanes(h, MINE)], qs[h], 1, 1) for h in TWO]
        dps = [dot(qkv[here, lanes(h, 2 * MINE)], dos[h], 1, 1) for h in TWO]
        for h in TWO:
            p = jnp.exp2(scores[h] * E - lse_s[h : h + 1, rows])
            if masked:
                p = causal(p, 0.0)
            ds = (p * (dps[h] - delta_s[h : h + 1, rows])).astype(BF)
            acc[here, lanes(h, MINE)] += dot(p.astype(BF), dos[h])
            acc[here, lanes(h)] += dot(ds, qs[h])
            dq_s[h, :, rows] += dot(kt[h, :, here], ds)

    def back_pair(q, k):
        lax.fori_loop(0, 4, lambda t, _: back(q, k * CHIP + lax.div(t, 2) * KEYS, lax.rem(t, 2), False), None)

    def back_self(q):
        lax.fori_loop(0, 2, lambda n, _: back(q, q * CHIP + n * KEYS, n, True), None)
        back(q, q * CHIP, 1, False)

    def pairs(do, first, last):
        def body(p, _):
            end = p // 5
            a, b = place.seen(p // 2 - 2 * end), place.seen(p - p // 2 + 1 - end)
            do(jnp.maximum(a, b), jnp.minimum(a, b))

        lax.fori_loop(first, last, body, None)

    def alone(one, first, last):
        lax.fori_loop(first, last, lambda r, _: one(place.seen(r)), None)

    def hats(at):
        wide = x_ref[pl.ds(at, SOME), :].astype(F32)
        scale = lax.rsqrt(jnp.mean(wide * wide, -1, keepdims=True) + 1e-6)
        return wide * scale, scale

    def gain_row():
        return gain_ref[...].astype(F32).reshape(1, D)

    def normed(n, _):
        for h in TWO:
            here = span(n * SOME, SOME)
            own[0, h, here, :] = (hats(h * PIECE + n * SOME)[0] * gain_row()).astype(BF)

    lax.fori_loop(0, PIECE // SOME, normed, None)
    pl.semaphore_wait(barrier, len(others))
    a_all.begin(SENDS)
    a_all.keep()
    fetch = [pltpu.make_async_copy(dy_ref.at[pl.ds(h * PIECE, PIECE)], own.at[1, h], local.at[1, h]) for h in TWO]
    for c in fetch:
        c.start()
    swaps = [push(w, u, CN, send_w, recv_w, n) for n, (w, u) in enumerate(((wq_in, uq), (wk_in, uk), (wv_in, uv)))]
    for c in swaps:
        c.start()
    top_s[...] = jnp.full(top_s.shape, NEG, F32)
    acc[...] = jnp.zeros(acc.shape, F32)
    for h in TWO:
        vt[h, HEAD:, :] = jnp.ones((16, ROWS), BF)
    for c in fills:
        c.wait()
    wo[...] = stage[0].T
    for c in fetch:
        c.wait()
    y_all.begin(NEAR_SENDS)
    y_all.keep()

    def forward_pass(g, _):
        for n in (1, 2, 3):

            @pl.when(g == n)
            def _():
                a_all.forward(n)
                if n == 1:
                    y_all.begin(FAR_SENDS)

        a_all.work(g, project)

        @pl.when(g == 0)
        def _():
            y_all.ready()
            y_all.work(0, lift)

        near, far = g // 2 * 3, g // 3 * 3
        pairs(attend_pair, far, near + far)
        alone(attend_self, far, near + far // 3)

    a_all.ready()
    lax.fori_loop(0, 4, forward_pass, None)
    lax.fori_loop(0, 4, attended, None)
    acc[...] = jnp.zeros(acc.shape, F32)
    dq_s[...] = jnp.zeros(dq_s.shape, F32)
    alone(prepare, 0, 1)

    def finish(block):
        cos, sin = angles(block)
        rows = span(block * PIECE, PIECE)
        for h in TWO:
            grad[rows, lanes(h)] = turn((dq_s[h, :, rows] * SCALE).T, cos, -sin).astype(BF)
            grad[rows, lanes(h, MINE)] = turn(acc[rows, lanes(h)] * SCALE, cos, -sin).astype(BF)
        grad[rows, 2 * MINE :] = acc[rows, MINE:].astype(BF)

    def block(r, core, half):
        return (place.seen(r) * 2 + core) * 2 + half

    def trade(r, half):
        there = theirs.at[place.seen(r), span(half * PIECE, PIECE), :]
        return push(grad.at[span(block(r, 1 - place.core, half) * PIECE, PIECE), :], there, CN, send_g, recv_g, 2 * r + half)

    def settle(r, half):
        finish(block(r, 1 - place.core, half))
        trade(r, half).start()
        finish(block(r, place.core, half))

    def product(to, start, size, cols):
        there = place.beside(*to)
        mine = grad[pl.ds(pl.multiple_of(there.device() * KEYS + start, PIECE), size), :]
        other = theirs[there.chip(), pl.ds(start, size), :]
        total = None
        for g, ws in ((mine, (wq, wk, wv)), (other, (uq, uk, uv))):
            for n, w in enumerate(ws):
                t = dot(g[:, n * MINE : (n + 1) * MINE], w[cols, :], 1, 1)
                total = t if total is None else total + t
        return total

    routes = [(own.at[0, 0], YN), (own.at[0, 1], XN), (own.at[1, 0], XN), (own.at[1, 1], YN), (stage.at[0], XN), (stage.at[1], YN)]

    def move(slot, j):
        src, to = routes[slot]
        cols = span(j * WIDE, WIDE)
        return push(src.at[:, cols], landing.at[slot, :, cols], to, send_r, recv_r, slot * (D // WIDE) + j)

    def take(slot, j, dst, sem):
        cols = span(j * WIDE, WIDE)
        move(slot, j).wait_recv()
        c = pltpu.make_async_copy(landing.at[slot, :, cols], dst.at[:, cols], sem)
        c.start()
        return c

    def columns(do):
        lax.fori_loop(0, D // WIDE, lambda j, _: do(j, span(j * WIDE, WIDE)), None)

    def both(j, cols):
        t = product(ACROSS, 0, KEYS, cols).astype(BF)
        for n in TWO:
            own[0, n, :, cols] = t[n * PIECE : (n + 1) * PIECE]
        for n in TWO:
            move(n, j).start()

    def direct(j, cols):
        own[1, 0, :, cols] = product(XN, PIECE, PIECE, cols).astype(BF)
        move(2, j).start()
        own[1, 1, :, cols] = product(YN, 0, PIECE, cols).astype(BF)
        move(3, j).start()

    def joined(j):
        cols = span(j * WIDE, WIDE)
        for n in TWO:
            move(n, j).wait_send()
        for c in [take(n, j, own.at[0, n], last.at[n]) for n in TWO]:
            c.wait()
        stage[0, :, cols] = (product(XN, 0, PIECE, cols) + own[0, 0, :, cols].astype(F32)).astype(BF)
        move(4, j).start()
        stage[1, :, cols] = (product(YN, PIECE, PIECE, cols) + own[0, 1, :, cols].astype(F32)).astype(BF)
        move(5, j).start()

    def backward_pass(stage_number, _):
        @pl.when(stage_number == 1)
        def _():
            for g in (1, 2):
                y_all.forward(g)
                y_all.work(g, lift)
            alone(prepare, 1, 3)

        @pl.when(stage_number == 2)
        def _():
            y_all.forward(3)

        @pl.when(stage_number == 3)
        def _():
            y_all.work(3, lift)
            alone(prepare, 3, 4)

        @pl.when(stage_number == 4)
        def _():
            a_all.sent()
            y_all.sent()
            lax.fori_loop(0, 2, lambda t, _: settle(1 + t, 1 - t), None)
            for c in swaps:
                c.wait()
            for t in TWO:
                trade(1 + t, 1 - t).wait_recv()
            columns(direct)

        n = stage_number
        odd, end = n % 2, n // 4
        first = (n + 1) // 2 * 3 - 3 * odd - end
        pairs(back_pair, first, first + odd * (3 - n // 3) + end)
        once = (1 - odd) * (1 + n // 2 - n // 4)
        start = n // 2 + end - (n // 2) // 2 * (1 - end)
        alone(back_self, start, start + (1 - odd) * (1 + (n // 2) % 2))

    lax.fori_loop(0, 5, backward_pass, None)

    def remaining(t):
        late = t // 4
        return (1 - late) * (3 - 3 * (t // 2)) + late * (1 + t % 2), t % 2

    lax.fori_loop(0, 6, lambda t, _: settle(*remaining(t)), None)
    lax.fori_loop(0, 6, lambda t, _: trade(*remaining(t)).wait_recv(), None)
    columns(both)

    tiles = [(ga, qkv.at[:, :MINE]), (ga, qkv.at[:, MINE : 2 * MINE]), (gy, qkv.at[:, 2 * MINE :]), (gy, do_s)]
    results = [gq_out, gk_out, gv_out, gwo_out]

    def tile(j, slot):
        made = []
        for n in TWO:
            buf, dst = tiles[2 * n + slot]
            made.append(pltpu.make_async_copy(buf.at[:, span(j * MINE, MINE)], dst, loads.at[2 * n + slot]))
        return made

    def out(j, slot, n):
        to = results[n].at[:, :, span(j * MINE, MINE)] if n == 3 else results[n].at[pl.ds(2 * j, 2)]
        return pltpu.make_async_copy(kt.at[:, :, pl.ds((4 * slot + n) * MINE, MINE)], to, outs.at[4 * slot + n])

    for c in tile(0, 0):
        c.start()

    def stream(n, _):
        for slot in TWO:
            j = 2 * n + slot

            @pl.when(j + 1 < D // MINE)
            def _():
                for c in tile(j + 1, 1 - slot):
                    c.start()

            for c in tile(j, slot):
                c.wait()

            @pl.when(n > 0)
            def _():
                for i in range(4):
                    out(j - 2, slot, i).wait()

            a, dy = tiles[slot][1], tiles[2 + slot][1]
            t = sum(dot(a[k : k + CHIP, :], grad[k : k + CHIP, :], 0, 0) for k in range(0, ROWS, CHIP)).astype(BF)
            for h in TWO:
                for i in range(3):
                    kt[h, :, (4 * slot + i) * MINE : (4 * slot + i + 1) * MINE] = t[lanes(h), i * MINE : (i + 1) * MINE]
                kt[h, :, (4 * slot + 3) * MINE : (4 * slot + 4) * MINE] = dot(vt[h, :HEAD, :], dy[...]).astype(BF)
            for i in range(4):
                out(j, slot, i).start()
        joined(n)

    lax.fori_loop(0, D // WIDE, stream, None)

    def mine(j, cols):
        acc[cols, :] = product(OWN, 0, KEYS, cols)

    columns(mine)
    again = [pltpu.make_async_copy(dy_ref.at[pl.ds(h * PIECE, PIECE)], own.at[1, h], local.at[1, h]) for h in TWO]
    taken = []
    for j in range(D // WIDE):
        for n in TWO:
            move(2 + n, j).wait_send()
            taken.append(take(2 + n, j, own.at[0, n], last.at[2 + 4 * n + j]))
    for c in again:
        c.start()
    for j in range(D // WIDE):
        for n in TWO:
            move(4 + n, j).wait_send()
            taken.append(take(4 + n, j, stage.at[n], last.at[10 + 4 * n + j]))
    for c in taken + again:
        c.wait()

    gain = gain_row()
    dgain[...] = jnp.zeros(dgain.shape, F32)
    for half in TWO:
        direct_in, joined_in = own.at[0, 1 - half], stage.at[half]

        def ended(n, _):
            here = span(n * SOME, SOME)
            at = half * PIECE + n * SOME
            da = jnp.concatenate([acc[pl.ds(j * WIDE + at, SOME), :] for j in range(D // WIDE)], 1)
            da = da + direct_in[here, :].astype(F32) + joined_in[here, :].astype(F32)
            hat, scale = hats(at)
            got = da * gain
            inner = jnp.mean(got * hat, -1, keepdims=True)
            stage[half, here, :] = (own[1, half, here, :].astype(F32) + (got - hat * inner) * scale).astype(BF)
            dgain[...] += (da * hat).reshape(SOME // 8, 8, D).sum(axis=0)

        lax.fori_loop(0, PIECE // SOME, ended, None)
        pltpu.make_async_copy(stage.at[half], dx_out.at[pl.ds(half * PIECE, PIECE)], local.at[0, half]).start()
    told[0] = dgain[...].sum(axis=0, keepdims=True)
    tell = [push(told.at[0], told.at[n], (n // 4, n // 2 % 2, n % 2), send_n, recv_n, n) for n in range(1, 8)]
    for c in tell:
        c.start()
    for slot in TWO:
        for i in range(4):
            out(D // MINE - 2 + slot, slot, i).wait()
    for r in range(4):
        for half in TWO:
            trade(r, half).wait_send()
    for half in TWO:
        pltpu.make_async_copy(stage.at[half], dx_out.at[pl.ds(half * PIECE, PIECE)], local.at[0, half]).wait()
    for c in tell:
        c.wait()
    total = [told[n] for n in range(8)]
    while len(total) > 1:
        total = [total[n] + total[n + 1] for n in range(0, len(total), 2)]
    gain_out[...] = total[0]


def _hand(n, *refs):
    srcs, dsts, bufs, sems = refs[:n], refs[n : 2 * n], refs[2 * n : 3 * n], refs[3 * n]
    loads = [pltpu.make_async_copy(src, buf, sems.at[0, i]) for i, (src, buf) in enumerate(zip(srcs, bufs))]
    stores = [pltpu.make_async_copy(buf, dst, sems.at[1, i]) for i, (buf, dst) in enumerate(zip(bufs, dsts))]
    for c in loads:
        c.start()
    for load, store in zip(loads, stores):
        load.wait()
        store.start()
    for c in stores:
        c.wait()


def hand(arrays):
    hbm = pl.BlockSpec(memory_space=pltpu.HBM)
    n = len(arrays)
    return pl.pallas_call(
        lambda *refs: _hand(n, *refs),
        in_specs=[hbm] * n,
        out_specs=[hbm] * n,
        out_shape=[jax.ShapeDtypeStruct(t.shape, t.dtype) for t in arrays],
        scratch_shapes=[pltpu.VMEM(t.shape, t.dtype) for t in arrays] + [pltpu.SemaphoreType.DMA((2, n))],
        name="hand",
    )(*arrays)


def solution(mesh):
    hbm, vmem = pl.BlockSpec(memory_space=pltpu.HBM), pl.BlockSpec(memory_space=pltpu.VMEM)
    shape = jax.ShapeDtypeStruct
    dma = lambda *n: pltpu.SemaphoreType.DMA(n)

    def step(x, dy, gain, wq, wk, wv, wo):
        rows, tall = shape((ROWS, D), BF), shape((D // HEAD, HEAD, MINE), BF)
        outs = pl.pallas_call(
            _step,
            in_specs=[vmem, hbm, vmem] + [hbm] * 4 + [vmem] * 4,
            out_specs=[hbm] * 8 + [vmem],
            out_shape=[rows, rows, shape((6, PIECE, D), BF), shape((KEYS, D), BF), tall, tall, tall, shape((2, HEAD, D), BF), shape((1, D), F32)],
            scratch_shapes=[
                pltpu.VMEM((2, 2, PIECE, D), BF),
                pltpu.VMEM((2, PIECE, D), BF),
                pltpu.VMEM((ROWS, 3 * MINE), BF),
                pltpu.VMEM((ROWS, MINE), BF),
                pltpu.VMEM((2, HEAD + 16, ROWS), BF),
                pltpu.VMEM((2, HEAD, ROWS), BF),
                pltpu.VMEM((4, 4, KEYS), F32),
                pltpu.VMEM((2, ROWS), F32),
                pltpu.VMEM((2, ROWS), F32),
                pltpu.VMEM((ROWS, 2 * MINE), F32),
                pltpu.VMEM((2, HEAD, ROWS), F32),
                pltpu.VMEM((ROWS, 3 * MINE), BF),
                pltpu.VMEM((4, KEYS, 3 * MINE), BF),
                *[pltpu.VMEM((D, MINE), BF)] * 7,
                pltpu.VMEM((8, D), F32),
                pltpu.VMEM((8, 1, D), F32),
                *[dma(16)] * 4, dma(2, 2), *[dma(4)] * 3, *[dma(8)] * 2, *[dma(24)] * 2, *[dma(8)] * 3, dma(4), dma(18),
            ],
            compiler_params=pltpu.CompilerParams(collective_id=0, has_side_effects=True, vmem_limit_bytes=67043328),
            cost_estimate=pl.CostEstimate(flops=80 * 10**9, bytes_accessed=2**27, transcendentals=2 * ROWS * ROWS),
            name="step",
        )(x, dy, gain, wq, wk, wv, wo, *tables())
        dx, gq, gk, gv, gwo, dgain = hand(outs[3:])
        return dx, dgain, *[t.reshape(D, MINE) for t in (gq, gk, gv)], gwo.reshape(MINE, D)

    tokens, columns = P(("dp", "tp"), None), P(None, "tp")
    return jax.shard_map(
        step,
        mesh=mesh,
        in_specs=(tokens, tokens, P(None), columns, columns, columns, P("tp", None)),
        out_specs=(tokens, P("dp", None), P("dp", "tp"), P("dp", "tp"), P("dp", "tp"), P(("dp", "tp"), None)),
        check_vma=False,
    )
```

```python
import jax
import jax.numpy as jnp
import numpy as np
from jax import lax
from jax.experimental import pallas as pl
from jax.experimental.pallas import tpu as pltpu
from jax.sharding import PartitionSpec as P

HEAD = 128
THETA = 10000
LOG2E = 1.4426950408889634
NEG, HIDDEN = -1e30, -2e30
ROWS, D, MINE = 4096, 2048, 256
PIECE = 256
KEYS = 512
CHIP = 1024
SOME = 32
WIDE = 512
SCALE = HEAD**-0.5
E = SCALE * LOG2E
BF, F32 = jnp.bfloat16, jnp.float32
TWO = range(2)
MESH = pl.DeviceIdType.MESH


def tables():
    half = HEAD // 2
    freq = float(THETA) ** (-np.arange(half) / half)
    both = lambda t: np.concatenate([t, t], 1).astype(np.float32)
    near = np.arange(PIECE)[:, None] * freq
    far = np.arange(0, ROWS, PIECE)[:, None] * freq
    return tuple(jnp.asarray(both(f(t))) for t in (near, far) for f in (np.cos, np.sin))


def dot(a, b, ca=1, cb=0):
    return lax.dot_general(a, b, (((ca,), (cb,)), ((), ())), preferred_element_type=F32)


def span(start, size):
    return pl.ds(pl.multiple_of(start, size), size)


def lanes(h, base=0):
    return slice(base + h * HEAD, base + (h + 1) * HEAD)


def turn(t, cos, sin):
    return t * cos + pltpu.roll(t, HEAD // 2, 1) * sin


def causal(s, hidden):
    ok = lax.broadcasted_iota(jnp.int32, s.shape, 1) >= lax.broadcasted_iota(jnp.int32, s.shape, 0)
    return jnp.where(ok, s, hidden)


def loop(last, body, first=0):
    lax.fori_loop(first, last, body, None)


def flipped(at, f):
    return lax.rem(at + f, 2)


class Place:
    def __init__(self, x, y, core):
        self.x, self.y, self.core = x, y, core

    def beside(self, fx, fy, fc):
        return Place(flipped(self.x, fx), flipped(self.y, fy), flipped(self.core, fc))

    def device(self):
        return 2 * self.chip() + self.core

    def chip(self):
        return 2 * self.x + self.y

    def id(self):
        return {"tp": self.device()}

    def seen(self, r):
        return self.beside(lax.rem(r, 2), lax.div(r, 2), 0).chip()

    def piece(self, group, i):
        odd, core = i % 2, i // 2
        beyond = (group + 1) // 2
        far, one = beyond // 2, beyond % 2
        swapped = group // 2 - group // 3
        return self.rows((far + one * (1 - odd), far + one * odd, core), odd + swapped * (1 - 2 * odd))

    def rows(self, to, half):
        return span((2 * self.beside(*to).device() + half) * PIECE, PIECE)


OWN, XN, YN, CN, ACROSS = (0, 0, 0), (1, 0, 0), (0, 1, 0), (0, 0, 1), (1, 1, 0)
FAR_SENDS = [(0, 1, 0, XN), (1, 1, 1, YN), (1, 2, 0, XN), (0, 2, 1, YN)]
NEAR_SENDS = [(0, 0, 2, CN), (1, 0, 3, CN)]
SENDS = FAR_SENDS + NEAR_SENDS
FORWARDS = {1: [(0, 3, 0, YN), (1, 3, 1, XN), (0, 1, 2, CN), (1, 1, 3, CN)], 2: [(0, 2, 2, CN), (1, 2, 3, CN)], 3: [(0, 3, 2, CN), (1, 3, 3, CN)]}


class Gather:
    def __init__(self, place, own, buf, sends, recvs, local, stage, loads):
        self.place, self.own, self.buf, self.sends, self.recvs, self.local = place, own, buf, sends, recvs, local
        self.stage, self.loads = stage, loads

    def copy(self, src, group, i, to):
        there = self.place.beside(*to)
        at = self.buf.at[there.piece(group, i), :]
        slot = 4 * group + i
        return pltpu.make_async_remote_copy(src_ref=at if src is None else src, dst_ref=at, send_sem=self.sends.at[slot],
                                            recv_sem=self.recvs.at[slot], device_id=there.id(), device_id_type=MESH)

    def kept(self):
        return [pltpu.make_async_copy(self.own.at[h], self.buf.at[self.place.rows(OWN, h), :], self.local.at[h]) for h in TWO]

    def keep(self):
        for c in self.kept():
            c.start()

    def begin(self, sends):
        for h, group, i, to in sends:
            self.copy(self.own.at[h], group, i, to).start()

    def ready(self):
        for c in self.kept():
            c.wait()

    def arrived(self, group, i):
        at = self.buf.at[self.place.piece(group, i), :]
        slot = 4 * group + i
        pltpu.make_async_remote_copy(src_ref=at, dst_ref=at, send_sem=self.sends.at[slot], recv_sem=self.recvs.at[slot],
                                     device_id=self.place.beside(*XN).id(), device_id_type=MESH).wait_recv()

    def forward(self, group):
        for i in TWO:
            self.arrived(group, i)
        for i, g, n, to in FORWARDS[group]:
            self.copy(self.buf.at[self.place.piece(group, i), :], g, n, to).start()

    def sent(self):
        for h, group, i, to in SENDS:
            self.copy(self.own.at[h], group, i, to).wait_send()
        for at, todo in FORWARDS.items():
            for i, g, n, to in todo:
                self.copy(self.buf.at[self.place.piece(at, i), :], g, n, to).wait_send()

    def work(self, group, do):
        def load(i):
            slot = lax.rem(i, 2)
            return pltpu.make_async_copy(self.buf.at[self.place.piece(group, i), :], self.stage.at[slot], self.loads.at[slot])

        load(jnp.int32(0)).start()

        def body(i, _):
            @pl.when(i < 3)
            def _():
                @pl.when(i >= 1)
                def _():
                    self.arrived(group, i + 1)

                load(i + 1).start()

            load(i).wait()
            do(lax.rem(i, 2), self.place.piece(group, i).start // PIECE)

        loop(4, body)


def _step(x_ref, dy_ref, gain_ref, wq_in, wk_in, wv_in, wo_in, nc, ns, fc, fs,
          ga, gy, landing, dx_out, gq_out, gk_out, gv_out, gwo_out, gain_out,
          own, stage, qkv, do_s, vt, kt, top_s, lse_s, delta_s, acc, dq_s, grad, theirs, wq, wk, wv, wo, uq, uk, uv, dgain, told,
          send_a, send_y, recv_a, recv_y, local, loads, send_w, recv_w, send_g, recv_g, send_r, recv_r, send_n, recv_n, outs, given, last):
    me = lax.axis_index("tp")
    place = Place(lax.div(me, 4), lax.rem(lax.div(me, 2), 2), lax.rem(me, 2))
    others = [place.beside(n // 4, n // 2 % 2, n % 2) for n in range(1, 8)]
    barrier = pltpu.get_barrier_semaphore()
    for there in others:
        pl.semaphore_signal(barrier, inc=1, device_id=there.id(), device_id_type=MESH)
    fills = [(wo_in, stage.at[0]), (wq_in, wq), (wk_in, wk), (wv_in, wv)]
    fills = [pltpu.make_async_copy(src, dst, given.at[n]) for n, (src, dst) in enumerate(fills)]
    for c in fills:
        c.start()

    a_all = Gather(place, own.at[0], ga, send_a, recv_a, local.at[0], stage, loads)
    y_all = Gather(place, own.at[1], gy, send_y, recv_y, local.at[1], stage, loads)

    def push(src, dst, to, sends, recvs, slot):
        return pltpu.make_async_remote_copy(src_ref=src, dst_ref=dst, send_sem=sends.at[slot], recv_sem=recvs.at[slot],
                                            device_id=place.beside(*to).id(), device_id_type=MESH)

    def angles(block):
        far_c, far_s = fc[pl.ds(block, 1), :], fs[pl.ds(block, 1), :]
        near_c, near_s = nc[...], ns[...]
        sign = jnp.where(lax.broadcasted_iota(jnp.int32, (1, HEAD), 1) < HEAD // 2, -1.0, 1.0)
        return near_c * far_c - near_s * far_s, (near_s * far_c + near_c * far_s) * sign

    def project(slot, block):
        a = stage[slot]
        cos, sin = angles(block)
        rows = span(block * PIECE, PIECE)
        for at, w in ((0, wq), (MINE, wk)):
            t = dot(a, w[...]).astype(BF).astype(F32)
            for h in TWO:
                got = turn(t[:, lanes(h)], cos, sin).astype(BF)
                qkv[rows, lanes(h, at)] = got
                if at:
                    kt[h, :, rows] = got.T
        v = dot(a, wv[...]).astype(BF)
        qkv[rows, 2 * MINE :] = v
        for h in TWO:
            vt[h, :HEAD, rows] = v[:, lanes(h)].T

    def lift(slot, block):
        rows = span(block * PIECE, PIECE)
        do_s[rows, :] = dot(stage[slot], wo[...]).astype(BF)

    def prepare(block):
        rows = span(block * PIECE, PIECE)
        for h in TWO:
            both = do_s[rows, lanes(h)].astype(F32).T * vt[h, :HEAD, rows].astype(F32)
            delta_s[h : h + 1, rows] = both.sum(axis=0, keepdims=True)

    def lift_all(slot, block):
        lift(slot, block)
        prepare(block)

    def attend(chip, at, strips):
        keys = span(at, KEYS)
        pieces = [(h, s, m) for s, m in strips for h in TWO]
        scores = [dot(qkv[keys, lanes(h, MINE)], qkv[span(chip * CHIP + s * KEYS, KEYS), lanes(h)], 1, 1) for h, s, _ in pieces]
        weights, keeps = [], []
        for (h, s, masked), score in zip(pieces, scores):
            if masked:
                score = causal(score, HIDDEN)
            n = 2 * s + h
            old = top_s[chip, n : n + 1, :]
            top = jnp.maximum(old, score.max(axis=0, keepdims=True))
            top_s[chip, n : n + 1, :] = top
            weights.append(jnp.exp2((score - top) * E).astype(BF))
            keeps.append(jnp.exp2((old - top) * E))
        for (h, s, _), p, keep in zip(pieces, weights, keeps):
            here = pl.ds(pl.multiple_of((4 * chip + 2 * s + h) * MINE, MINE), HEAD + 16)
            acc[here, :] = acc[here, :] * keep + dot(vt[h, :, keys], p)

    def attend_pair(q, k):
        loop(2, lambda n, _: attend(q, k * CHIP + n * KEYS, [(0, False), (1, False)]))

    def attend_self(q):
        attend(q, q * CHIP, [(0, True), (1, False)])
        attend(q, q * CHIP + KEYS, [(1, True)])

    def attended(chip, _):
        for s in TWO:
            for h in TWO:
                n = 2 * s + h
                base = pl.multiple_of((4 * chip + n) * MINE, MINE)
                total = acc[pl.ds(base + HEAD, 8), :][:1]
                rows = span(chip * CHIP + s * KEYS, KEYS)
                vt[h, :HEAD, rows] = (acc[pl.ds(base, HEAD), :] * (1 / total)).astype(BF)
                lse_s[h : h + 1, rows] = top_s[chip, n : n + 1, :] * E + jnp.log2(total)

    def back(chip, at, strip, masked):
        here = span(at, KEYS)
        rows = span(chip * CHIP + strip * KEYS, KEYS)
        qs = [qkv[rows, lanes(h)] for h in TWO]
        dos = [do_s[rows, lanes(h)] for h in TWO]
        scores = [dot(qkv[here, lanes(h, MINE)], qs[h], 1, 1) for h in TWO]
        dps = [dot(qkv[here, lanes(h, 2 * MINE)], dos[h], 1, 1) for h in TWO]
        for h in TWO:
            p = jnp.exp2(scores[h] * E - lse_s[h : h + 1, rows])
            if masked:
                p = causal(p, 0.0)
            ds = (p * (dps[h] - delta_s[h : h + 1, rows])).astype(BF)
            acc[here, lanes(h, MINE)] += dot(p.astype(BF), dos[h])
            acc[here, lanes(h)] += dot(ds, qs[h])
            dq_s[h, :, rows] += dot(kt[h, :, here], ds)

    def back_halves(q, k):
        ats = [code // 2 * CHIP + code % 2 * PIECE for code in (q, k)]
        rows, here = ([span(at + n * KEYS, PIECE) for n in TWO] for at in ats)
        two = lambda ref, at, cols: jnp.concatenate([ref[r, cols] for r in at], 0)
        side = lambda get: jnp.concatenate([get(r) for r in rows], 1)
        qs = [two(qkv, rows, lanes(h)) for h in TWO]
        dos = [two(do_s, rows, lanes(h)) for h in TWO]
        scores = [dot(two(qkv, here, lanes(h, MINE)), qs[h], 1, 1) for h in TWO]
        dps = [dot(two(qkv, here, lanes(h, 2 * MINE)), dos[h], 1, 1) for h in TWO]
        for h in TWO:
            p = jnp.exp2(scores[h] * E - side(lambda r: lse_s[h : h + 1, r]))
            ds = (p * (dps[h] - side(lambda r: delta_s[h : h + 1, r]))).astype(BF)
            for base, t in ((MINE, dot(p.astype(BF), dos[h])), (0, dot(ds, qs[h]))):
                for n in TWO:
                    acc[here[n], lanes(h, base)] += t[n * PIECE : (n + 1) * PIECE]
            t = dot(jnp.concatenate([kt[h, :, r] for r in here], 1), ds)
            for n in TWO:
                dq_s[h, :, rows[n]] += t[:, n * PIECE : (n + 1) * PIECE]

    runs = ["00100110002101211021", "0011011100200120102011201121", "1130113120302031", "10301031213021310030003101300131"]
    digits = [int(c) for c in "".join(runs)]
    ends = [sum(len(r) for r in runs[:n]) // 4 for n in range(len(runs) + 1)]
    bit = lambda field, by: sum((v // by % 2) << n for n, v in enumerate(digits[field::4]))
    masks = [bit(field, by) for field, by in ((0, 2), (0, 1), (1, 1), (2, 2), (2, 1), (3, 1))]

    def between(first, last):
        def body(n, _):
            bits = [lax.rem(lax.shift_right_logical(jnp.int32(m), n), 2) for m in masks]
            a, b = (2 * place.seen(2 * bits[e] + bits[e + 1]) + bits[e + 2] for e in (0, 3))
            back_halves(jnp.maximum(a, b), jnp.minimum(a, b))

        loop(last, body, first)

    def back_self(q):
        loop(2, lambda n, _: back(q, q * CHIP + n * KEYS, n, True))
        back(q, q * CHIP, 1, False)

    def pairs(do, first, last):
        def body(p, _):
            end = p // 5
            a, b = place.seen(p // 2 - 2 * end), place.seen(p - p // 2 + 1 - end)
            do(jnp.maximum(a, b), jnp.minimum(a, b))

        loop(last, body, first)

    def alone(one, first, last):
        loop(last, lambda r, _: one(place.seen(r)), first)

    def hats(at):
        wide = x_ref[pl.ds(at, SOME), :].astype(F32)
        scale = lax.rsqrt(jnp.mean(wide * wide, -1, keepdims=True) + 1e-6)
        return wide * scale, scale

    def gain_row():
        return gain_ref[...].astype(F32).reshape(1, D)

    def normed(n, _):
        for h in TWO:
            here = span(n * SOME, SOME)
            own[0, h, here, :] = (hats(h * PIECE + n * SOME)[0] * gain_row()).astype(BF)

    loop(PIECE // SOME, normed)
    pl.semaphore_wait(barrier, len(others))
    a_all.begin(SENDS)
    a_all.keep()
    fetch = [pltpu.make_async_copy(dy_ref.at[pl.ds(h * PIECE, PIECE)], own.at[1, h], local.at[1, h]) for h in TWO]
    for c in fetch:
        c.start()
    swaps = [push(w, u, CN, send_w, recv_w, n) for n, (w, u) in enumerate(((wq_in, uq), (wk_in, uk), (wv_in, uv)))]
    for c in swaps:
        c.start()
    top_s[...] = jnp.full(top_s.shape, NEG, F32)
    acc[...] = jnp.zeros(acc.shape, F32)
    for h in TWO:
        vt[h, HEAD:, :] = jnp.ones((16, ROWS), BF)
    for c in fills:
        c.wait()
    wo[...] = stage[0].T
    for c in fetch:
        c.wait()
    y_all.begin(NEAR_SENDS)
    y_all.keep()

    def forward_pass(g, _):
        for n in (1, 2, 3):

            @pl.when(g == n)
            def _():
                a_all.forward(n)
                if n == 1:
                    y_all.begin(FAR_SENDS)

        a_all.work(g, project)

        @pl.when(g == 0)
        def _():
            y_all.ready()
            y_all.work(0, lift)

        near, far = g // 2 * 3, g // 3 * 3
        pairs(attend_pair, far, near + far)
        alone(attend_self, far, near + far // 3)

    a_all.ready()
    loop(4, forward_pass)
    loop(4, attended)
    acc[...] = jnp.zeros(acc.shape, F32)
    dq_s[...] = jnp.zeros(dq_s.shape, F32)
    loop(4, lambda n, _: prepare(place.chip() * 4 + n))

    def finish(block):
        cos, sin = angles(block)
        rows = span(block * PIECE, PIECE)
        for h in TWO:
            grad[rows, lanes(h)] = turn((dq_s[h, :, rows] * SCALE).T, cos, -sin).astype(BF)
            grad[rows, lanes(h, MINE)] = turn(acc[rows, lanes(h)] * SCALE, cos, -sin).astype(BF)
        grad[rows, 2 * MINE :] = acc[rows, MINE:].astype(BF)

    def block(r, core, half):
        return (place.seen(r) * 2 + core) * 2 + half

    def trade(r, half):
        there = theirs.at[place.seen(r), span(half * PIECE, PIECE), :]
        return push(grad.at[span(block(r, 1 - place.core, half) * PIECE, PIECE), :], there, CN, send_g, recv_g, 2 * r + half)

    def settle(r, half):
        finish(block(r, 1 - place.core, half))
        trade(r, half).start()
        finish(block(r, place.core, half))

    def product(to, start, size, cols):
        there = place.beside(*to)
        mine = grad[pl.ds(pl.multiple_of(there.device() * KEYS + start, PIECE), size), :]
        other = theirs[there.chip(), pl.ds(start, size), :]
        total = None
        for g, ws in ((mine, (wq, wk, wv)), (other, (uq, uk, uv))):
            for n, w in enumerate(ws):
                t = dot(g[:, n * MINE : (n + 1) * MINE], w[cols, :], 1, 1)
                total = t if total is None else total + t
        return total

    routes = [(own.at[0, 0], YN), (own.at[0, 1], XN), (own.at[1, 0], XN), (own.at[1, 1], YN), (stage.at[0], XN), (stage.at[1], YN)]

    def move(slot, j):
        src, to = routes[slot]
        cols = span(j * WIDE, WIDE)
        return push(src.at[:, cols], landing.at[slot, :, cols], to, send_r, recv_r, slot * (D // WIDE) + j)

    def take(slot, j, dst, sem):
        cols = span(j * WIDE, WIDE)
        move(slot, j).wait_recv()
        c = pltpu.make_async_copy(landing.at[slot, :, cols], dst.at[:, cols], sem)
        c.start()
        return c

    def columns(do):
        loop(D // WIDE, lambda j, _: do(j, span(j * WIDE, WIDE)))

    def both(j, cols):
        t = product(ACROSS, 0, KEYS, cols).astype(BF)
        for n in TWO:
            own[0, n, :, cols] = t[n * PIECE : (n + 1) * PIECE]
        for n in TWO:
            move(n, j).start()

    def direct(j, cols):
        own[1, 0, :, cols] = product(XN, PIECE, PIECE, cols).astype(BF)
        move(2, j).start()
        own[1, 1, :, cols] = product(YN, 0, PIECE, cols).astype(BF)
        move(3, j).start()

    def joined(j):
        cols = span(j * WIDE, WIDE)
        for n in TWO:
            move(n, j).wait_send()
        for c in [take(n, j, own.at[0, n], last.at[n]) for n in TWO]:
            c.wait()
        stage[0, :, cols] = (product(XN, 0, PIECE, cols) + own[0, 0, :, cols].astype(F32)).astype(BF)
        move(4, j).start()
        stage[1, :, cols] = (product(YN, PIECE, PIECE, cols) + own[0, 1, :, cols].astype(F32)).astype(BF)
        move(5, j).start()

    def backward_pass(n, _):
        for g in (1, 2):

            @pl.when(n == g)
            def _():
                y_all.forward(g)
                y_all.work(g, lift_all)

        @pl.when(n == 3)
        def _():
            y_all.forward(3)

        @pl.when(n == 4)
        def _():
            y_all.work(3, lift_all)

        @pl.when(n == 5)
        def _():
            a_all.sent()
            y_all.sent()
            loop(2, lambda t, _: settle(1 + t, 1 - t))
            for c in swaps:
                c.wait()
            for t in TWO:
                trade(1 + t, 1 - t).wait_recv()
            columns(direct)

        first = last = n * 0
        for at, begin, end in zip((1, 2, 4, 5), ends, ends[1:]):
            here = 1 - jnp.minimum(jnp.abs(n - at), 1)
            first, last = first + here * begin, last + here * end
        between(first, last)
        skip = n % 3 * (2 - n % 3)
        start = (n + 1) // 2
        alone(back_self, start, start + 1 - skip)

    loop(6, backward_pass)

    def remaining(t):
        late = t // 4
        return (1 - late) * (3 - 3 * (t // 2)) + late * (1 + t % 2), t % 2

    loop(2, lambda t, _: settle(*remaining(t)))
    for t in TWO:
        trade(3, t).wait_recv()
    columns(both)
    loop(6, lambda t, _: settle(*remaining(t)), 2)
    loop(6, lambda t, _: trade(*remaining(t)).wait_recv(), 2)

    tiles = [(ga, qkv.at[:, :MINE]), (ga, qkv.at[:, MINE : 2 * MINE]), (gy, qkv.at[:, 2 * MINE :]), (gy, do_s)]
    results = [gq_out, gk_out, gv_out, gwo_out]

    def tile(j, slot):
        made = []
        for n in TWO:
            buf, dst = tiles[2 * n + slot]
            made.append(pltpu.make_async_copy(buf.at[:, span(j * MINE, MINE)], dst, loads.at[2 * n + slot]))
        return made

    def out(j, slot, n):
        to = results[n].at[:, :, span(j * MINE, MINE)] if n == 3 else results[n].at[pl.ds(2 * j, 2)]
        return pltpu.make_async_copy(kt.at[:, :, pl.ds((4 * slot + n) * MINE, MINE)], to, outs.at[4 * slot + n])

    for c in tile(0, 0):
        c.start()

    def stream(n, _):
        for slot in TWO:
            j = 2 * n + slot

            @pl.when(j + 1 < D // MINE)
            def _():
                for c in tile(j + 1, 1 - slot):
                    c.start()

            for c in tile(j, slot):
                c.wait()

            @pl.when(n > 0)
            def _():
                for i in range(4):
                    out(j - 2, slot, i).wait()

            a, dy = tiles[slot][1], tiles[2 + slot][1]
            t = sum(dot(a[k : k + CHIP, :], grad[k : k + CHIP, :], 0, 0) for k in range(0, ROWS, CHIP)).astype(BF)
            for h in TWO:
                for i in range(3):
                    kt[h, :, (4 * slot + i) * MINE : (4 * slot + i + 1) * MINE] = t[lanes(h), i * MINE : (i + 1) * MINE]
                kt[h, :, (4 * slot + 3) * MINE : (4 * slot + 4) * MINE] = dot(vt[h, :HEAD, :], dy[...]).astype(BF)
            for i in range(4):
                out(j, slot, i).start()
        joined(n)

    loop(D // WIDE, stream)

    def mine(j, cols):
        acc[cols, :] = product(OWN, 0, KEYS, cols)

    columns(mine)
    again = [pltpu.make_async_copy(dy_ref.at[pl.ds(h * PIECE, PIECE)], own.at[1, h], local.at[1, h]) for h in TWO]
    taken = []
    for j in range(D // WIDE):
        for n in TWO:
            move(2 + n, j).wait_send()
            taken.append(take(2 + n, j, own.at[0, n], last.at[2 + 4 * n + j]))
    for c in again:
        c.start()
    for j in range(D // WIDE):
        for n in TWO:
            move(4 + n, j).wait_send()
            taken.append(take(4 + n, j, stage.at[n], last.at[10 + 4 * n + j]))
    for c in taken + again:
        c.wait()

    gain = gain_row()
    dgain[...] = jnp.zeros(dgain.shape, F32)
    for half in TWO:
        direct_in, joined_in = own.at[0, 1 - half], stage.at[half]

        def ended(n, _):
            here = span(n * SOME, SOME)
            at = half * PIECE + n * SOME
            da = jnp.concatenate([acc[pl.ds(j * WIDE + at, SOME), :] for j in range(D // WIDE)], 1)
            da = da + direct_in[here, :].astype(F32) + joined_in[here, :].astype(F32)
            hat, scale = hats(at)
            got = da * gain
            inner = jnp.mean(got * hat, -1, keepdims=True)
            stage[half, here, :] = (own[1, half, here, :].astype(F32) + (got - hat * inner) * scale).astype(BF)
            dgain[...] += (da * hat).reshape(SOME // 8, 8, D).sum(axis=0)

        loop(PIECE // SOME, ended)
        pltpu.make_async_copy(stage.at[half], dx_out.at[pl.ds(half * PIECE, PIECE)], local.at[0, half]).start()
    told[0] = dgain[...].sum(axis=0, keepdims=True)
    tell = [push(told.at[0], told.at[n], (n // 4, n // 2 % 2, n % 2), send_n, recv_n, n) for n in range(1, 8)]
    for c in tell:
        c.start()
    for slot in TWO:
        for i in range(4):
            out(D // MINE - 2 + slot, slot, i).wait()
    for r in range(4):
        for half in TWO:
            trade(r, half).wait_send()
    for half in TWO:
        pltpu.make_async_copy(stage.at[half], dx_out.at[pl.ds(half * PIECE, PIECE)], local.at[0, half]).wait()
    for c in tell:
        c.wait()
    total = [told[n] for n in range(8)]
    while len(total) > 1:
        total = [total[n] + total[n + 1] for n in range(0, len(total), 2)]
    gain_out[...] = total[0]


def _hand(n, *refs):
    srcs, dsts, bufs, sems = refs[:n], refs[n : 2 * n], refs[2 * n : 3 * n], refs[3 * n]
    loads = [pltpu.make_async_copy(src, buf, sems.at[0, i]) for i, (src, buf) in enumerate(zip(srcs, bufs))]
    stores = [pltpu.make_async_copy(buf, dst, sems.at[1, i]) for i, (buf, dst) in enumerate(zip(bufs, dsts))]
    for c in loads:
        c.start()
    for load, store in zip(loads, stores):
        load.wait()
        store.start()
    for c in stores:
        c.wait()


def hand(arrays):
    hbm = pl.BlockSpec(memory_space=pltpu.HBM)
    n = len(arrays)
    return pl.pallas_call(
        lambda *refs: _hand(n, *refs),
        in_specs=[hbm] * n,
        out_specs=[hbm] * n,
        out_shape=[jax.ShapeDtypeStruct(t.shape, t.dtype) for t in arrays],
        scratch_shapes=[pltpu.VMEM(t.shape, t.dtype) for t in arrays] + [pltpu.SemaphoreType.DMA((2, n))],
        name="hand",
    )(*arrays)


def solution(mesh):
    hbm, vmem = pl.BlockSpec(memory_space=pltpu.HBM), pl.BlockSpec(memory_space=pltpu.VMEM)
    shape = jax.ShapeDtypeStruct
    dma = lambda *n: pltpu.SemaphoreType.DMA(n)

    def step(x, dy, gain, wq, wk, wv, wo):
        rows, tall = shape((ROWS, D), BF), shape((D // HEAD, HEAD, MINE), BF)
        outs = pl.pallas_call(
            _step,
            in_specs=[vmem, hbm, vmem] + [hbm] * 4 + [vmem] * 4,
            out_specs=[hbm] * 8 + [vmem],
            out_shape=[rows, rows, shape((6, PIECE, D), BF), shape((KEYS, D), BF), tall, tall, tall, shape((2, HEAD, D), BF), shape((1, D), F32)],
            scratch_shapes=[
                pltpu.VMEM((2, 2, PIECE, D), BF),
                pltpu.VMEM((2, PIECE, D), BF),
                pltpu.VMEM((ROWS, 3 * MINE), BF),
                pltpu.VMEM((ROWS, MINE), BF),
                pltpu.VMEM((2, HEAD + 16, ROWS), BF),
                pltpu.VMEM((2, HEAD, ROWS), BF),
                pltpu.VMEM((4, 4, KEYS), F32),
                pltpu.VMEM((2, ROWS), F32),
                pltpu.VMEM((2, ROWS), F32),
                pltpu.VMEM((ROWS, 2 * MINE), F32),
                pltpu.VMEM((2, HEAD, ROWS), F32),
                pltpu.VMEM((ROWS, 3 * MINE), BF),
                pltpu.VMEM((4, KEYS, 3 * MINE), BF),
                *[pltpu.VMEM((D, MINE), BF)] * 7,
                pltpu.VMEM((8, D), F32),
                pltpu.VMEM((8, 1, D), F32),
                *[dma(16)] * 4, dma(2, 2), *[dma(4)] * 3, *[dma(8)] * 2, *[dma(24)] * 2, *[dma(8)] * 3, dma(4), dma(18),
            ],
            compiler_params=pltpu.CompilerParams(collective_id=0, has_side_effects=True, vmem_limit_bytes=67043328),
            cost_estimate=pl.CostEstimate(flops=80 * 10**9, bytes_accessed=2**27, transcendentals=2 * ROWS * ROWS),
            name="step",
        )(x, dy, gain, wq, wk, wv, wo, *tables())
        dx, gq, gk, gv, gwo, dgain = hand(outs[3:])
        return dx, dgain, *[t.reshape(D, MINE) for t in (gq, gk, gv)], gwo.reshape(MINE, D)

    tokens, columns = P(("dp", "tp"), None), P(None, "tp")
    return jax.shard_map(
        step,
        mesh=mesh,
        in_specs=(tokens, tokens, P(None), columns, columns, columns, P("tp", None)),
        out_specs=(tokens, P("dp", None), P("dp", "tp"), P("dp", "tp"), P("dp", "tp"), P(("dp", "tp"), None)),
        check_vma=False,
    )
```

```python
import jax
import jax.numpy as jnp
import numpy as np
from jax import lax
from jax.experimental import pallas as pl
from jax.experimental.pallas import tpu as pltpu
from jax.sharding import PartitionSpec as P

HEAD = 128
THETA = 10000
LOG2E = 1.4426950408889634
NEG, HIDDEN = -1e30, -2e30
ROWS, D, MINE = 4096, 2048, 256
PIECE = 256
KEYS = 512
CHIP = 1024
SOME = 32
WIDE = 512
SCALE = HEAD**-0.5
E = SCALE * LOG2E
BF, F32 = jnp.bfloat16, jnp.float32
TWO = range(2)
MESH = pl.DeviceIdType.MESH


def tables():
    half = HEAD // 2
    freq = float(THETA) ** (-np.arange(half) / half)
    both = lambda t: np.concatenate([t, t], 1).astype(np.float32)
    near = np.arange(PIECE)[:, None] * freq
    far = np.arange(0, ROWS, PIECE)[:, None] * freq
    return tuple(jnp.asarray(both(f(t))) for t in (near, far) for f in (np.cos, np.sin))


def dot(a, b, ca=1, cb=0):
    return lax.dot_general(a, b, (((ca,), (cb,)), ((), ())), preferred_element_type=F32)


def span(start, size):
    return pl.ds(pl.multiple_of(start, size), size)


def lanes(h, base=0):
    return slice(base + h * HEAD, base + (h + 1) * HEAD)


def turn(t, cos, sin):
    return t * cos + pltpu.roll(t, HEAD // 2, 1) * sin


def causal(s, hidden):
    ok = lax.broadcasted_iota(jnp.int32, s.shape, 1) >= lax.broadcasted_iota(jnp.int32, s.shape, 0)
    return jnp.where(ok, s, hidden)


def loop(last, body, first=0):
    lax.fori_loop(first, last, body, None)


def flipped(at, f):
    return lax.rem(at + f, 2)


class Place:
    def __init__(self, x, y, core):
        self.x, self.y, self.core = x, y, core

    def beside(self, fx, fy, fc):
        return Place(flipped(self.x, fx), flipped(self.y, fy), flipped(self.core, fc))

    def device(self):
        return 2 * self.chip() + self.core

    def chip(self):
        return 2 * self.x + self.y

    def id(self):
        return {"tp": self.device()}

    def seen(self, r):
        return self.beside(lax.rem(r, 2), lax.div(r, 2), 0).chip()

    def piece(self, group, i):
        odd, core = i % 2, i // 2
        beyond = (group + 1) // 2
        far, one = beyond // 2, beyond % 2
        swapped = group // 2 - group // 3
        return self.rows((far + one * (1 - odd), far + one * odd, core), odd + swapped * (1 - 2 * odd))

    def rows(self, to, half):
        return span((2 * self.beside(*to).device() + half) * PIECE, PIECE)


OWN, XN, YN, CN, ACROSS = (0, 0, 0), (1, 0, 0), (0, 1, 0), (0, 0, 1), (1, 1, 0)
FAR_SENDS = [(0, 1, 0, XN), (1, 1, 1, YN), (1, 2, 0, XN), (0, 2, 1, YN)]
NEAR_SENDS = [(0, 0, 2, CN), (1, 0, 3, CN)]
SENDS = FAR_SENDS + NEAR_SENDS
FORWARDS = {1: [(0, 3, 0, YN), (1, 3, 1, XN), (0, 1, 2, CN), (1, 1, 3, CN)], 2: [(0, 2, 2, CN), (1, 2, 3, CN)], 3: [(0, 3, 2, CN), (1, 3, 3, CN)]}


class Gather:
    def __init__(self, place, pool, base, buf, sends, recvs, local, loads):
        self.place, self.pool, self.buf, self.sends, self.recvs, self.local = place, pool, buf, sends, recvs, local
        self.own, self.loads = [pool.at[base + h] for h in TWO], loads

    def copy(self, src, group, i, to):
        there = self.place.beside(*to)
        at = self.buf.at[there.piece(group, i), :]
        slot = 4 * group + i
        return pltpu.make_async_remote_copy(src_ref=at if src is None else src, dst_ref=at, send_sem=self.sends.at[slot],
                                            recv_sem=self.recvs.at[slot], device_id=there.id(), device_id_type=MESH)

    def kept(self):
        return [pltpu.make_async_copy(self.own[h], self.buf.at[self.place.rows(OWN, h), :], self.local.at[h]) for h in TWO]

    def keep(self):
        for c in self.kept():
            c.start()

    def begin(self, sends):
        for h, group, i, to in sends:
            self.copy(self.own[h], group, i, to).start()

    def ready(self):
        for c in self.kept():
            c.wait()

    def arrived(self, group, i):
        at = self.buf.at[self.place.piece(group, i), :]
        slot = 4 * group + i
        pltpu.make_async_remote_copy(src_ref=at, dst_ref=at, send_sem=self.sends.at[slot], recv_sem=self.recvs.at[slot],
                                     device_id=self.place.beside(*XN).id(), device_id_type=MESH).wait_recv()

    def forward(self, group):
        for i in TWO:
            self.arrived(group, i)
        for i, g, n, to in FORWARDS[group]:
            self.copy(self.buf.at[self.place.piece(group, i), :], g, n, to).start()

    def sent(self):
        for h, group, i, to in SENDS:
            self.copy(self.own[h], group, i, to).wait_send()
        for at, todo in FORWARDS.items():
            for i, g, n, to in todo:
                self.copy(self.buf.at[self.place.piece(at, i), :], g, n, to).wait_send()

    def work(self, group, do):
        def load(i):
            slot = lax.rem(i, 2) + 4
            return slot, pltpu.make_async_copy(self.buf.at[self.place.piece(group, i), :], self.pool.at[slot], self.loads.at[slot - 4])

        load(jnp.int32(0))[1].start()

        def body(i, _):
            @pl.when(i < 3)
            def _():
                @pl.when(i >= 1)
                def _():
                    self.arrived(group, i + 1)

                load(i + 1)[1].start()

            slot, c = load(i)
            c.wait()
            do(slot, self.place.piece(group, i).start // PIECE)

        loop(4, body)

    def deep(self, group, do, at_once):
        def load(i):
            slot = lax.rem(i + 4, 6)
            return slot, pltpu.make_async_copy(self.buf.at[self.place.piece(group, i), :], self.pool.at[slot], self.loads.at[i])

        def others():
            for i in (2, 3):
                self.arrived(group, i)
                load(jnp.int32(i))[1].start()

        for i in TWO:
            load(jnp.int32(i))[1].start()
        if at_once:
            others()

        def body(i, _):
            if not at_once:
                pl.when(i == 2)(others)
            slot, c = load(i)
            c.wait()
            do(slot, self.place.piece(group, i).start // PIECE)

        loop(4, body)


def _step(x_ref, dy_ref, gain_ref, wq_in, wk_in, wv_in, wo_in, nc, ns, fc, fs,
          ga, gy, landing, dx_out, gq_out, gk_out, gv_out, gwo_out, gain_out,
          pool, x_s, scale_s, inner_s, qkv, do_s, vt, kt, top_s, lse_s, delta_s, acc, dq_s, grad, theirs, wq, wk, wv, wo, uq, uk, uv, dgain, told,
          send_a, send_y, recv_a, recv_y, local, loads, send_w, recv_w, send_g, recv_g, send_r, recv_r, send_n, recv_n, outs, given, last):
    me = lax.axis_index("tp")
    place = Place(lax.div(me, 4), lax.rem(lax.div(me, 2), 2), lax.rem(me, 2))
    others = [place.beside(n // 4, n // 2 % 2, n % 2) for n in range(1, 8)]
    barrier = pltpu.get_barrier_semaphore()
    for there in others:
        pl.semaphore_signal(barrier, inc=1, device_id=there.id(), device_id_type=MESH)
    fills = [(x_ref.at[pl.ds(h * PIECE, PIECE)], x_s.at[pl.ds(h * PIECE, PIECE)]) for h in TWO]
    fills += [(wo_in, pool.at[4]), (wq_in, wq), (wk_in, wk), (wv_in, wv)]
    fills = [pltpu.make_async_copy(src, dst, given.at[n]) for n, (src, dst) in enumerate(fills)]
    for c in fills:
        c.start()

    a_all = Gather(place, pool, 0, ga, send_a, recv_a, local.at[0], loads)
    y_all = Gather(place, pool, 2, gy, send_y, recv_y, local.at[1], loads)

    def push(src, dst, to, sends, recvs, slot):
        return pltpu.make_async_remote_copy(src_ref=src, dst_ref=dst, send_sem=sends.at[slot], recv_sem=recvs.at[slot],
                                            device_id=place.beside(*to).id(), device_id_type=MESH)

    def angles(block):
        far_c, far_s = fc[pl.ds(block, 1), :], fs[pl.ds(block, 1), :]
        near_c, near_s = nc[...], ns[...]
        sign = jnp.where(lax.broadcasted_iota(jnp.int32, (1, HEAD), 1) < HEAD // 2, -1.0, 1.0)
        return near_c * far_c - near_s * far_s, (near_s * far_c + near_c * far_s) * sign

    def project(slot, block):
        a = pool[slot]
        cos, sin = angles(block)
        rows = span(block * PIECE, PIECE)
        for at, w in ((0, wq), (MINE, wk)):
            t = dot(a, w[...]).astype(BF).astype(F32)
            for h in TWO:
                got = turn(t[:, lanes(h)], cos, sin).astype(BF)
                qkv[rows, lanes(h, at)] = got
                if at:
                    kt[h, :, rows] = got.T
        v = dot(a, wv[...]).astype(BF)
        qkv[rows, 2 * MINE :] = v
        for h in TWO:
            vt[h, :HEAD, rows] = v[:, lanes(h)].T

    def lift(slot, block):
        rows = span(block * PIECE, PIECE)
        do_s[rows, :] = dot(pool[slot], wo[...]).astype(BF)

    def prepare(block):
        rows = span(block * PIECE, PIECE)
        for h in TWO:
            both = do_s[rows, lanes(h)].astype(F32).T * vt[h, :HEAD, rows].astype(F32)
            delta_s[h : h + 1, rows] = both.sum(axis=0, keepdims=True)

    def lift_all(slot, block):
        lift(slot, block)
        prepare(block)

    def attend(chip, at, strips):
        keys = span(at, KEYS)
        pieces = [(h, s, m) for s, m in strips for h in TWO]
        scores = [dot(qkv[keys, lanes(h, MINE)], qkv[span(chip * CHIP + s * KEYS, KEYS), lanes(h)], 1, 1) for h, s, _ in pieces]
        weights, keeps = [], []
        for (h, s, masked), score in zip(pieces, scores):
            if masked:
                score = causal(score, HIDDEN)
            n = 2 * s + h
            old = top_s[chip, n : n + 1, :]
            top = jnp.maximum(old, score.max(axis=0, keepdims=True))
            top_s[chip, n : n + 1, :] = top
            weights.append(jnp.exp2((score - top) * E).astype(BF))
            keeps.append(jnp.exp2((old - top) * E))
        for (h, s, _), p, keep in zip(pieces, weights, keeps):
            here = pl.ds(pl.multiple_of((4 * chip + 2 * s + h) * MINE, MINE), HEAD + 16)
            acc[here, :] = acc[here, :] * keep + dot(vt[h, :, keys], p)

    def attend_pair(q, k):
        loop(2, lambda n, _: attend(q, k * CHIP + n * KEYS, [(0, False), (1, False)]))

    def attend_self(q):
        attend(q, q * CHIP, [(0, True), (1, False)])
        attend(q, q * CHIP + KEYS, [(1, True)])

    def attended(chip, _):
        for s in TWO:
            for h in TWO:
                n = 2 * s + h
                base = pl.multiple_of((4 * chip + n) * MINE, MINE)
                total = acc[pl.ds(base + HEAD, 8), :][:1]
                rows = span(chip * CHIP + s * KEYS, KEYS)
                vt[h, :HEAD, rows] = (acc[pl.ds(base, HEAD), :] * (1 / total)).astype(BF)
                lse_s[h : h + 1, rows] = top_s[chip, n : n + 1, :] * E + jnp.log2(total)

    def back(chip, at, strip, masked):
        here = span(at, KEYS)
        rows = span(chip * CHIP + strip * KEYS, KEYS)
        qs = [qkv[rows, lanes(h)] for h in TWO]
        dos = [do_s[rows, lanes(h)] for h in TWO]
        scores = [dot(qkv[here, lanes(h, MINE)], qs[h], 1, 1) for h in TWO]
        dps = [dot(qkv[here, lanes(h, 2 * MINE)], dos[h], 1, 1) for h in TWO]
        for h in TWO:
            p = jnp.exp2(scores[h] * E - lse_s[h : h + 1, rows])
            if masked:
                p = causal(p, 0.0)
            ds = (p * (dps[h] - delta_s[h : h + 1, rows])).astype(BF)
            acc[here, lanes(h, MINE)] += dot(p.astype(BF), dos[h])
            acc[here, lanes(h)] += dot(ds, qs[h])
            dq_s[h, :, rows] += dot(kt[h, :, here], ds)

    def back_halves(q, k):
        ats = [code // 2 * CHIP + code % 2 * PIECE for code in (q, k)]
        rows, here = ([span(at + n * KEYS, PIECE) for n in TWO] for at in ats)
        two = lambda ref, at, cols: jnp.concatenate([ref[r, cols] for r in at], 0)
        side = lambda get: jnp.concatenate([get(r) for r in rows], 1)
        qs = [two(qkv, rows, lanes(h)) for h in TWO]
        dos = [two(do_s, rows, lanes(h)) for h in TWO]
        scores = [dot(two(qkv, here, lanes(h, MINE)), qs[h], 1, 1) for h in TWO]
        dps = [dot(two(qkv, here, lanes(h, 2 * MINE)), dos[h], 1, 1) for h in TWO]
        for h in TWO:
            p = jnp.exp2(scores[h] * E - side(lambda r: lse_s[h : h + 1, r]))
            ds = (p * (dps[h] - side(lambda r: delta_s[h : h + 1, r]))).astype(BF)
            for base, t in ((MINE, dot(p.astype(BF), dos[h])), (0, dot(ds, qs[h]))):
                for n in TWO:
                    acc[here[n], lanes(h, base)] += t[n * PIECE : (n + 1) * PIECE]
            t = dot(jnp.concatenate([kt[h, :, r] for r in here], 1), ds)
            for n in TWO:
                dq_s[h, :, rows[n]] += t[:, n * PIECE : (n + 1) * PIECE]

    runs = ["00100110002101211021", "0011011100200120102011201121", "1130113120302031", "10301031213021310030003101300131"]
    digits = [int(c) for c in "".join(runs)]
    ends = [sum(len(r) for r in runs[:n]) // 4 for n in range(len(runs) + 1)]
    bit = lambda field, by: sum((v // by % 2) << n for n, v in enumerate(digits[field::4]))
    masks = [bit(field, by) for field, by in ((0, 2), (0, 1), (1, 1), (2, 2), (2, 1), (3, 1))]

    def between(first, last):
        def body(n, _):
            bits = [lax.rem(lax.shift_right_logical(jnp.int32(m), n), 2) for m in masks]
            a, b = (2 * place.seen(2 * bits[e] + bits[e + 1]) + bits[e + 2] for e in (0, 3))
            back_halves(jnp.maximum(a, b), jnp.minimum(a, b))

        loop(last, body, first)

    def back_self(q):
        loop(2, lambda n, _: back(q, q * CHIP + n * KEYS, n, True))
        back(q, q * CHIP, 1, False)

    def pairs(do, first, last):
        def body(p, _):
            end = p // 5
            a, b = place.seen(p // 2 - 2 * end), place.seen(p - p // 2 + 1 - end)
            do(jnp.maximum(a, b), jnp.minimum(a, b))

        loop(last, body, first)

    def alone(one, first, last):
        loop(last, lambda r, _: one(place.seen(r)), first)

    def gain_row():
        return gain_ref[...].astype(F32).reshape(1, D)

    def normed(h):
        def body(n, _):
            here = span(n * SOME, SOME)
            rows = pl.ds(h * PIECE + n * SOME, SOME)
            wide = x_s[rows, :].astype(F32)
            scale = lax.rsqrt(jnp.mean(wide * wide, -1, keepdims=True) + 1e-6)
            scale_s[rows, :] = jnp.broadcast_to(scale, (SOME, HEAD))
            pool[h, here, :] = (wide * scale * gain_row()).astype(BF)

        fills[h].wait()
        loop(PIECE // SOME, body)

    normed(0)
    pl.semaphore_wait(barrier, len(others))
    a_all.begin(SENDS[:1])
    normed(1)
    a_all.begin(SENDS[1:])
    a_all.keep()
    fetch = [pltpu.make_async_copy(dy_ref.at[pl.ds(h * PIECE, PIECE)], pool.at[2 + h], local.at[1, h]) for h in TWO]
    for c in fetch:
        c.start()
    swaps = [push(w, u, CN, send_w, recv_w, n) for n, (w, u) in enumerate(((wq_in, uq), (wk_in, uk), (wv_in, uv)))]
    for c in swaps:
        c.start()
    top_s[...] = jnp.full(top_s.shape, NEG, F32)
    acc[...] = jnp.zeros(acc.shape, F32)
    for h in TWO:
        vt[h, HEAD:, :] = jnp.ones((16, ROWS), BF)
    for c in fills[2:]:
        c.wait()
    wo[...] = pool[4].T
    for c in fetch:
        c.wait()
    y_all.begin(NEAR_SENDS)
    y_all.keep()

    def forward_pass(g, _):
        for n in (1, 2, 3):

            @pl.when(g == n)
            def _():
                a_all.forward(n)
                if n == 1:
                    y_all.begin(FAR_SENDS)

        a_all.work(g, project)

        @pl.when(g == 0)
        def _():
            y_all.ready()
            y_all.work(0, lift)

        near, far = g // 2 * 3, g // 3 * 3
        pairs(attend_pair, far, near + far)
        alone(attend_self, far, near + far // 3)

    a_all.ready()
    loop(4, forward_pass)
    loop(4, attended)
    acc[...] = jnp.zeros(acc.shape, F32)
    dq_s[...] = jnp.zeros(dq_s.shape, F32)
    loop(4, lambda n, _: prepare(place.chip() * 4 + n))

    def finish(block):
        cos, sin = angles(block)
        rows = span(block * PIECE, PIECE)
        for h in TWO:
            grad[rows, lanes(h)] = turn((dq_s[h, :, rows] * SCALE).T, cos, -sin).astype(BF)
            grad[rows, lanes(h, MINE)] = turn(acc[rows, lanes(h)] * SCALE, cos, -sin).astype(BF)
        grad[rows, 2 * MINE :] = acc[rows, MINE:].astype(BF)

    def block(r, core, half):
        return (place.seen(r) * 2 + core) * 2 + half

    def trade(r, half):
        there = theirs.at[place.seen(r), span(half * PIECE, PIECE), :]
        return push(grad.at[span(block(r, 1 - place.core, half) * PIECE, PIECE), :], there, CN, send_g, recv_g, 2 * r + half)

    def settle(r, half):
        finish(block(r, 1 - place.core, half))
        trade(r, half).start()
        finish(block(r, place.core, half))

    def product(to, start, size, cols):
        there = place.beside(*to)
        mine = grad[pl.ds(pl.multiple_of(there.device() * KEYS + start, PIECE), size), :]
        other = theirs[there.chip(), pl.ds(start, size), :]
        total = None
        for g, ws in ((mine, (wq, wk, wv)), (other, (uq, uk, uv))):
            for n, w in enumerate(ws):
                t = dot(g[:, n * MINE : (n + 1) * MINE], w[cols, :], 1, 1)
                total = t if total is None else total + t
        return total

    routes = [(pool.at[n], to) for n, to in enumerate((YN, XN, XN, YN, XN, YN))]

    def move(slot, j):
        src, to = routes[slot]
        cols = span(j * WIDE, WIDE)
        return push(src.at[:, cols], landing.at[slot, :, cols], to, send_r, recv_r, slot * (D // WIDE) + j)

    def take(slot, j, dst, sem):
        cols = span(j * WIDE, WIDE)
        move(slot, j).wait_recv()
        c = pltpu.make_async_copy(landing.at[slot, :, cols], dst.at[:, cols], sem)
        c.start()
        return c

    def columns(do):
        loop(D // WIDE, lambda j, _: do(j, span(j * WIDE, WIDE)))

    def both(j, cols):
        t = product(ACROSS, 0, KEYS, cols).astype(BF)
        for n in TWO:
            pool[n, :, cols] = t[n * PIECE : (n + 1) * PIECE]
        for n in TWO:
            move(n, j).start()

    def direct(j, cols):
        pool[2, :, cols] = product(XN, PIECE, PIECE, cols).astype(BF)
        move(2, j).start()
        pool[3, :, cols] = product(YN, 0, PIECE, cols).astype(BF)
        move(3, j).start()

    def joined(j):
        cols = span(j * WIDE, WIDE)
        for n in TWO:
            move(n, j).wait_send()
        for c in [take(n, j, pool.at[n], last.at[n]) for n in TWO]:
            c.wait()
        pool[4, :, cols] = (product(XN, 0, PIECE, cols) + pool[0, :, cols].astype(F32)).astype(BF)
        move(4, j).start()
        pool[5, :, cols] = (product(YN, PIECE, PIECE, cols) + pool[1, :, cols].astype(F32)).astype(BF)
        move(5, j).start()

    def backward_pass(n, _):
        for g in (1, 2):

            @pl.when(n == g)
            def _():
                y_all.forward(g)
                y_all.deep(g, lift_all, False)

        @pl.when(n == 3)
        def _():
            y_all.forward(3)

        @pl.when(n == 4)
        def _():
            y_all.deep(3, lift_all, True)

        @pl.when(n == 5)
        def _():
            y_all.sent()
            loop(2, lambda t, _: settle(1 + t, 1 - t))
            for c in swaps:
                c.wait()
            for t in TWO:
                trade(1 + t, 1 - t).wait_recv()
            columns(direct)

        first = last = n * 0
        for at, begin, end in zip((1, 2, 4, 5), ends, ends[1:]):
            here = 1 - jnp.minimum(jnp.abs(n - at), 1)
            first, last = first + here * begin, last + here * end
        between(first, last)
        skip = n % 3 * (2 - n % 3)
        start = (n + 1) // 2
        alone(back_self, start, start + 1 - skip)

    a_all.sent()
    loop(6, backward_pass)

    def remaining(t):
        late = t // 4
        return (1 - late) * (3 - 3 * (t // 2)) + late * (1 + t % 2), t % 2

    loop(2, lambda t, _: settle(*remaining(t)))
    for t in TWO:
        trade(3, t).wait_recv()
    columns(both)
    loop(6, lambda t, _: settle(*remaining(t)), 2)
    loop(6, lambda t, _: trade(*remaining(t)).wait_recv(), 2)

    tiles = [(ga, qkv.at[:, :MINE]), (ga, qkv.at[:, MINE : 2 * MINE]), (gy, qkv.at[:, 2 * MINE :]), (gy, do_s)]
    results = [gq_out, gk_out, gv_out, gwo_out]

    def tile(j, slot):
        made = []
        for n in TWO:
            buf, dst = tiles[2 * n + slot]
            made.append(pltpu.make_async_copy(buf.at[:, span(j * MINE, MINE)], dst, loads.at[2 * n + slot]))
        return made

    def out(j, slot, n):
        to = results[n].at[:, :, span(j * MINE, MINE)] if n == 3 else results[n].at[pl.ds(2 * j, 2)]
        return pltpu.make_async_copy(kt.at[:, :, pl.ds((4 * slot + n) * MINE, MINE)], to, outs.at[4 * slot + n])

    for c in tile(0, 0):
        c.start()

    def stream(n, _):
        for slot in TWO:
            j = 2 * n + slot

            @pl.when(j + 1 < D // MINE)
            def _():
                for c in tile(j + 1, 1 - slot):
                    c.start()

            for c in tile(j, slot):
                c.wait()

            @pl.when(n > 0)
            def _():
                for i in range(4):
                    out(j - 2, slot, i).wait()

            a, dy = tiles[slot][1], tiles[2 + slot][1]
            t = sum(dot(a[k : k + CHIP, :], grad[k : k + CHIP, :], 0, 0) for k in range(0, ROWS, CHIP)).astype(BF)
            for h in TWO:
                for i in range(3):
                    kt[h, :, (4 * slot + i) * MINE : (4 * slot + i + 1) * MINE] = t[lanes(h), i * MINE : (i + 1) * MINE]
                kt[h, :, (4 * slot + 3) * MINE : (4 * slot + 4) * MINE] = dot(vt[h, :HEAD, :], dy[...]).astype(BF)
            for i in range(4):
                out(j, slot, i).start()
        joined(n)

    loop(D // WIDE, stream)

    def mine(j, cols):
        acc[cols, :] = product(OWN, 0, KEYS, cols)

    columns(mine)
    for j in range(D // WIDE):
        for n in (2, 3):
            move(n, j).wait_send()
    again = [pltpu.make_async_copy(dy_ref.at[pl.ds(h * PIECE, PIECE)], pool.at[2 + h], local.at[1, h]) for h in TWO]
    for c in again:
        c.start()

    dgain[...] = jnp.zeros(dgain.shape, F32)
    inner_s[...] = jnp.zeros(inner_s.shape, F32)

    def closing(j, cols):
        for n in TWO:
            move(4 + n, j).wait_send()
        taken = [take(2 + n, j, pool.at[to], last.at[to]) for n, to in ((0, 0), (1, 1), (2, 4), (3, 5))]
        for c in taken:
            c.wait()
        gain = gain_ref[cols].astype(F32).reshape(1, WIDE)
        for half in TWO:

            def body(n, _):
                here = span(n * SOME, SOME)
                rows = span(half * PIECE + n * SOME, SOME)
                mine_rows = span(j * WIDE + half * PIECE + n * SOME, SOME)
                da = acc[mine_rows, :] + pool[1 - half, here, cols].astype(F32) + pool[4 + half, here, cols].astype(F32)
                acc[mine_rows, :] = da
                part = da * (x_s[rows, cols].astype(F32) * scale_s[rows, :1])
                dgain[:, cols] += part.reshape(SOME // 8, 8, WIDE).sum(axis=0)
                part = part * gain
                inner_s[rows, :] += sum(part[:, lanes(k)] for k in range(WIDE // HEAD))

            loop(PIECE // SOME, body)

    columns(closing)
    told[0] = dgain[...].sum(axis=0, keepdims=True)
    tell = [push(told.at[0], told.at[n], (n // 4, n // 2 % 2, n % 2), send_n, recv_n, n) for n in range(1, 8)]
    for c in tell:
        c.start()
    for c in again:
        c.wait()
    for half in TWO:

        def ended(n, _):
            here = span(n * SOME, SOME)
            rows = span(half * PIECE + n * SOME, SOME)
            da = jnp.concatenate([acc[span(j * WIDE + half * PIECE + n * SOME, SOME), :] for j in range(D // WIDE)], 1)
            scale = scale_s[rows, :1]
            inner = inner_s[rows, :].sum(axis=1, keepdims=True) * (1 / D)
            got = (da * gain_row() - x_s[rows, :].astype(F32) * (scale * inner)) * scale
            pool[4 + half, here, :] = (pool[2 + half, here, :].astype(F32) + got).astype(BF)

        loop(PIECE // SOME, ended)
        pltpu.make_async_copy(pool.at[4 + half], dx_out.at[pl.ds(half * PIECE, PIECE)], local.at[0, half]).start()
    for slot in TWO:
        for i in range(4):
            out(D // MINE - 2 + slot, slot, i).wait()
    for r in range(4):
        for half in TWO:
            trade(r, half).wait_send()
    for half in TWO:
        pltpu.make_async_copy(pool.at[4 + half], dx_out.at[pl.ds(half * PIECE, PIECE)], local.at[0, half]).wait()
    for c in tell:
        c.wait()
    total = [told[n] for n in range(8)]
    while len(total) > 1:
        total = [total[n] + total[n + 1] for n in range(0, len(total), 2)]
    gain_out[...] = total[0]


def _hand(n, *refs):
    srcs, dsts, bufs, sems = refs[:n], refs[n : 2 * n], refs[2 * n : 3 * n], refs[3 * n]
    loads = [pltpu.make_async_copy(src, buf, sems.at[0, i]) for i, (src, buf) in enumerate(zip(srcs, bufs))]
    stores = [pltpu.make_async_copy(buf, dst, sems.at[1, i]) for i, (buf, dst) in enumerate(zip(bufs, dsts))]
    for c in loads:
        c.start()
    for load, store in zip(loads, stores):
        load.wait()
        store.start()
    for c in stores:
        c.wait()


def hand(arrays):
    hbm = pl.BlockSpec(memory_space=pltpu.HBM)
    n = len(arrays)
    return pl.pallas_call(
        lambda *refs: _hand(n, *refs),
        in_specs=[hbm] * n,
        out_specs=[hbm] * n,
        out_shape=[jax.ShapeDtypeStruct(t.shape, t.dtype) for t in arrays],
        scratch_shapes=[pltpu.VMEM(t.shape, t.dtype) for t in arrays] + [pltpu.SemaphoreType.DMA((2, n))],
        name="hand",
    )(*arrays)


def solution(mesh):
    hbm, vmem = pl.BlockSpec(memory_space=pltpu.HBM), pl.BlockSpec(memory_space=pltpu.VMEM)
    shape = jax.ShapeDtypeStruct
    dma = lambda *n: pltpu.SemaphoreType.DMA(n)

    def step(x, dy, gain, wq, wk, wv, wo):
        rows, tall = shape((ROWS, D), BF), shape((D // HEAD, HEAD, MINE), BF)
        outs = pl.pallas_call(
            _step,
            in_specs=[hbm, hbm, vmem] + [hbm] * 4 + [vmem] * 4,
            out_specs=[hbm] * 8 + [vmem],
            out_shape=[rows, rows, shape((6, PIECE, D), BF), shape((KEYS, D), BF), tall, tall, tall, shape((2, HEAD, D), BF), shape((1, D), F32)],
            scratch_shapes=[
                pltpu.VMEM((6, PIECE, D), BF),
                pltpu.VMEM((KEYS, D), BF),
                *[pltpu.VMEM((KEYS, HEAD), F32)] * 2,
                pltpu.VMEM((ROWS, 3 * MINE), BF),
                pltpu.VMEM((ROWS, MINE), BF),
                pltpu.VMEM((2, HEAD + 16, ROWS), BF),
                pltpu.VMEM((2, HEAD, ROWS), BF),
                pltpu.VMEM((4, 4, KEYS), F32),
                pltpu.VMEM((2, ROWS), F32),
                pltpu.VMEM((2, ROWS), F32),
                pltpu.VMEM((ROWS, 2 * MINE), F32),
                pltpu.VMEM((2, HEAD, ROWS), F32),
                pltpu.VMEM((ROWS, 3 * MINE), BF),
                pltpu.VMEM((4, KEYS, 3 * MINE), BF),
                *[pltpu.VMEM((D, MINE), BF)] * 7,
                pltpu.VMEM((8, D), F32),
                pltpu.VMEM((8, 1, D), F32),
                *[dma(16)] * 4, dma(2, 2), *[dma(4)] * 3, *[dma(8)] * 2, *[dma(24)] * 2, *[dma(8)] * 3, dma(6), dma(6),
            ],
            compiler_params=pltpu.CompilerParams(collective_id=0, has_side_effects=True, vmem_limit_bytes=67043328),
            cost_estimate=pl.CostEstimate(flops=80 * 10**9, bytes_accessed=2**27, transcendentals=2 * ROWS * ROWS),
            name="step",
        )(x, dy, gain, wq, wk, wv, wo, *tables())
        dx, gq, gk, gv, gwo, dgain = hand(outs[3:])
        return dx, dgain, *[t.reshape(D, MINE) for t in (gq, gk, gv)], gwo.reshape(MINE, D)

    tokens, columns = P(("dp", "tp"), None), P(None, "tp")
    return jax.shard_map(
        step,
        mesh=mesh,
        in_specs=(tokens, tokens, P(None), columns, columns, columns, P("tp", None)),
        out_specs=(tokens, P("dp", None), P("dp", "tp"), P("dp", "tp"), P("dp", "tp"), P(("dp", "tp"), None)),
        check_vma=False,
    )
```

```python
import jax
import jax.numpy as jnp
import numpy as np
from jax import lax
from jax.experimental import pallas as pl
from jax.experimental.pallas import tpu as pltpu
from jax.sharding import PartitionSpec as P

HEAD = 128
THETA = 10000
LOG2E = 1.4426950408889634
NEG, HIDDEN = -1e30, -2e30
ROWS, D, MINE = 4096, 2048, 256
PIECE = 256
KEYS = 512
CHIP = 1024
SOME, MANY = 32, 64
WIDE = 512
SCALE = HEAD**-0.5
E = SCALE * LOG2E
BF, F32 = jnp.bfloat16, jnp.float32
TWO = range(2)
MESH = pl.DeviceIdType.MESH


def tables():
    half = HEAD // 2
    freq = float(THETA) ** (-np.arange(half) / half)
    both = lambda t: np.concatenate([t, t], 1).astype(np.float32)
    near = np.arange(PIECE)[:, None] * freq
    far = np.arange(0, ROWS, PIECE)[:, None] * freq
    return tuple(jnp.asarray(both(f(t))) for t in (near, far) for f in (np.cos, np.sin))


def dot(a, b, ca=1, cb=0):
    return lax.dot_general(a, b, (((ca,), (cb,)), ((), ())), preferred_element_type=F32)


def span(start, size):
    return pl.ds(pl.multiple_of(start, size), size)


def lanes(h, base=0):
    return slice(base + h * HEAD, base + (h + 1) * HEAD)


def turn(t, cos, sin):
    return t * cos + pltpu.roll(t, HEAD // 2, 1) * sin


def causal(s, hidden):
    ok = lax.broadcasted_iota(jnp.int32, s.shape, 1) >= lax.broadcasted_iota(jnp.int32, s.shape, 0)
    return jnp.where(ok, s, hidden)


def loop(last, body, first=0):
    lax.fori_loop(first, last, body, None)


def flipped(at, f):
    return lax.rem(at + f, 2)


class Place:
    def __init__(self, x, y, core):
        self.x, self.y, self.core = x, y, core

    def beside(self, fx, fy, fc):
        return Place(flipped(self.x, fx), flipped(self.y, fy), flipped(self.core, fc))

    def device(self):
        return 2 * self.chip() + self.core

    def chip(self):
        return 2 * self.x + self.y

    def id(self):
        return {"tp": self.device()}

    def seen(self, r):
        return self.beside(lax.rem(r, 2), lax.div(r, 2), 0).chip()

    def piece(self, group, i):
        odd, core = i % 2, i // 2
        beyond = (group + 1) // 2
        far, one = beyond // 2, beyond % 2
        swapped = group // 2 - group // 3
        return self.rows((far + one * (1 - odd), far + one * odd, core), odd + swapped * (1 - 2 * odd))

    def rows(self, to, half):
        return span((2 * self.beside(*to).device() + half) * PIECE, PIECE)


OWN, XN, YN, CN, ACROSS = (0, 0, 0), (1, 0, 0), (0, 1, 0), (0, 0, 1), (1, 1, 0)
FAR_SENDS = [(0, 1, 0, XN), (1, 1, 1, YN), (1, 2, 0, XN), (0, 2, 1, YN)]
NEAR_SENDS = [(0, 0, 2, CN), (1, 0, 3, CN)]
SENDS = FAR_SENDS + NEAR_SENDS
FORWARDS = {1: [(0, 3, 0, YN), (1, 3, 1, XN), (0, 1, 2, CN), (1, 1, 3, CN)], 2: [(0, 2, 2, CN), (1, 2, 3, CN)], 3: [(0, 3, 2, CN), (1, 3, 3, CN)]}


class Gather:
    def __init__(self, place, pool, base, buf, sends, recvs, local, loads):
        self.place, self.pool, self.buf, self.sends, self.recvs, self.local = place, pool, buf, sends, recvs, local
        self.own, self.loads = [pool.at[base + h] for h in TWO], loads

    def copy(self, src, group, i, to):
        there = self.place.beside(*to)
        at = self.buf.at[there.piece(group, i), :]
        slot = 4 * group + i
        return pltpu.make_async_remote_copy(src_ref=at if src is None else src, dst_ref=at, send_sem=self.sends.at[slot],
                                            recv_sem=self.recvs.at[slot], device_id=there.id(), device_id_type=MESH)

    def kept(self):
        return [pltpu.make_async_copy(self.own[h], self.buf.at[self.place.rows(OWN, h), :], self.local.at[h]) for h in TWO]

    def keep(self):
        for c in self.kept():
            c.start()

    def begin(self, sends):
        for h, group, i, to in sends:
            self.copy(self.own[h], group, i, to).start()

    def ready(self):
        for c in self.kept():
            c.wait()

    def arrived(self, group, i):
        at = self.buf.at[self.place.piece(group, i), :]
        slot = 4 * group + i
        pltpu.make_async_remote_copy(src_ref=at, dst_ref=at, send_sem=self.sends.at[slot], recv_sem=self.recvs.at[slot],
                                     device_id=self.place.beside(*XN).id(), device_id_type=MESH).wait_recv()

    def forward(self, group):
        for i in TWO:
            self.arrived(group, i)
        for i, g, n, to in FORWARDS[group]:
            self.copy(self.buf.at[self.place.piece(group, i), :], g, n, to).start()

    def sent(self):
        for h, group, i, to in SENDS:
            self.copy(self.own[h], group, i, to).wait_send()
        for at, todo in FORWARDS.items():
            for i, g, n, to in todo:
                self.copy(self.buf.at[self.place.piece(at, i), :], g, n, to).wait_send()

    def work(self, group, do):
        def load(i):
            slot = lax.rem(i, 2) + 4
            return slot, pltpu.make_async_copy(self.buf.at[self.place.piece(group, i), :], self.pool.at[slot], self.loads.at[slot - 4])

        load(jnp.int32(0))[1].start()

        def body(i, _):
            @pl.when(i < 3)
            def _():
                @pl.when(i >= 1)
                def _():
                    self.arrived(group, i + 1)

                load(i + 1)[1].start()

            slot, c = load(i)
            c.wait()
            do(slot, self.place.piece(group, i).start // PIECE)

        loop(4, body)

    def deep_load(self, group, i):
        slot = lax.rem(i + 4, 6)
        return slot, pltpu.make_async_copy(self.buf.at[self.place.piece(group, i), :], self.pool.at[slot], self.loads.at[i])

    def ahead(self, group):
        for i in TWO:
            self.deep_load(group, jnp.int32(i))[1].start()

    def deep(self, group, do, at_once):
        def others():
            for i in (2, 3):
                self.arrived(group, i)
                self.deep_load(group, jnp.int32(i))[1].start()

        if at_once:
            others()

        def body(t, _):
            if not at_once:
                pl.when(t == 1)(others)
            both = [self.deep_load(group, 2 * t + n) for n in TWO]
            for _, c in both:
                c.wait()
            do(both[0][0], [self.place.piece(group, 2 * t + n).start // PIECE for n in TWO])

        loop(2, body)


def _step(x_ref, dy_ref, gain_ref, wq_in, wk_in, wv_in, wo_in, nc, ns, fc, fs,
          ga, gy, landing, dx_out, gq_out, gk_out, gv_out, gwo_out, gain_out,
          pool, x_s, scale_s, inner_s, qkv, do_s, vt, kt, top_s, lse_s, delta_s, acc, dq_s, grad, theirs, wq, wk, wv, wo, uq, uk, uv, dgain, told,
          send_a, send_y, recv_a, recv_y, local, loads, send_w, recv_w, send_g, recv_g, send_r, recv_r, send_n, recv_n, outs, given, last):
    me = lax.axis_index("tp")
    place = Place(lax.div(me, 4), lax.rem(lax.div(me, 2), 2), lax.rem(me, 2))
    others = [place.beside(n // 4, n // 2 % 2, n % 2) for n in range(1, 8)]
    barrier = pltpu.get_barrier_semaphore()
    for there in others:
        pl.semaphore_signal(barrier, inc=1, device_id=there.id(), device_id_type=MESH)
    fills = [(x_ref.at[pl.ds(h * PIECE, PIECE)], x_s.at[pl.ds(h * PIECE, PIECE)]) for h in TWO]
    fills += [(wo_in, pool.at[4]), (wq_in, wq), (wk_in, wk), (wv_in, wv)]
    fills = [pltpu.make_async_copy(src, dst, given.at[n]) for n, (src, dst) in enumerate(fills)]
    for c in fills[:2]:
        c.start()

    a_all = Gather(place, pool, 0, ga, send_a, recv_a, local.at[0], loads)
    y_all = Gather(place, pool, 2, gy, send_y, recv_y, local.at[1], loads)

    def push(src, dst, to, sends, recvs, slot):
        return pltpu.make_async_remote_copy(src_ref=src, dst_ref=dst, send_sem=sends.at[slot], recv_sem=recvs.at[slot],
                                            device_id=place.beside(*to).id(), device_id_type=MESH)

    def angles(block):
        far_c, far_s = fc[pl.ds(block, 1), :], fs[pl.ds(block, 1), :]
        near_c, near_s = nc[...], ns[...]
        sign = jnp.where(lax.broadcasted_iota(jnp.int32, (1, HEAD), 1) < HEAD // 2, -1.0, 1.0)
        return near_c * far_c - near_s * far_s, (near_s * far_c + near_c * far_s) * sign

    def project(slot, block):
        a = pool[slot]
        cos, sin = angles(block)
        rows = span(block * PIECE, PIECE)
        for at, w in ((0, wq), (MINE, wk)):
            t = dot(a, w[...]).astype(BF).astype(F32)
            for h in TWO:
                got = turn(t[:, lanes(h)], cos, sin).astype(BF)
                qkv[rows, lanes(h, at)] = got
                if at:
                    kt[h, :, rows] = got.T
        v = dot(a, wv[...]).astype(BF)
        qkv[rows, 2 * MINE :] = v
        for h in TWO:
            vt[h, :HEAD, rows] = v[:, lanes(h)].T

    def lift(slot, block):
        rows = span(block * PIECE, PIECE)
        do_s[rows, :] = dot(pool[slot], wo[...]).astype(BF)

    def prepare(block):
        rows = span(block * PIECE, PIECE)
        for h in TWO:
            both = do_s[rows, lanes(h)].astype(F32).T * vt[h, :HEAD, rows].astype(F32)
            delta_s[h : h + 1, rows] = both.sum(axis=0, keepdims=True)

    def lift_all(slot, blocks):
        got = dot(pool[pl.ds(slot, 2)].reshape(2 * PIECE, D), wo[...]).astype(BF)
        for n, block in enumerate(blocks):
            do_s[span(block * PIECE, PIECE), :] = got[n * PIECE : (n + 1) * PIECE]
            prepare(block)

    def attend(chip, at, strips):
        keys = span(at, KEYS)
        pieces = [(h, s, m) for s, m in strips for h in TWO]
        scores = [dot(qkv[keys, lanes(h, MINE)], qkv[span(chip * CHIP + s * KEYS, KEYS), lanes(h)], 1, 1) for h, s, _ in pieces]
        weights, keeps = [], []
        for (h, s, masked), score in zip(pieces, scores):
            if masked:
                score = causal(score, HIDDEN)
            n = 2 * s + h
            old = top_s[chip, n : n + 1, :]
            top = jnp.maximum(old, score.max(axis=0, keepdims=True))
            top_s[chip, n : n + 1, :] = top
            weights.append(jnp.exp2((score - top) * E).astype(BF))
            keeps.append(jnp.exp2((old - top) * E))
        for (h, s, _), p, keep in zip(pieces, weights, keeps):
            here = pl.ds(pl.multiple_of((4 * chip + 2 * s + h) * MINE, MINE), HEAD + 16)
            acc[here, :] = acc[here, :] * keep + dot(vt[h, :, keys], p)

    def attend_pair(q, k):
        loop(2, lambda n, _: attend(q, k * CHIP + n * KEYS, [(0, False), (1, False)]))

    def attend_self(q):
        attend(q, q * CHIP, [(0, True), (1, False)])
        attend(q, q * CHIP + KEYS, [(1, True)])

    def attended(chip, _):
        for s in TWO:
            for h in TWO:
                n = 2 * s + h
                base = pl.multiple_of((4 * chip + n) * MINE, MINE)
                total = acc[pl.ds(base + HEAD, 8), :][:1]
                rows = span(chip * CHIP + s * KEYS, KEYS)
                vt[h, :HEAD, rows] = (acc[pl.ds(base, HEAD), :] * (1 / total)).astype(BF)
                lse_s[h : h + 1, rows] = top_s[chip, n : n + 1, :] * E + jnp.log2(total)

    def back(chip, at, strip, masked):
        here = span(at, KEYS)
        rows = span(chip * CHIP + strip * KEYS, KEYS)
        qs = [qkv[rows, lanes(h)] for h in TWO]
        dos = [do_s[rows, lanes(h)] for h in TWO]
        scores = [dot(qkv[here, lanes(h, MINE)], qs[h], 1, 1) for h in TWO]
        dps = [dot(qkv[here, lanes(h, 2 * MINE)], dos[h], 1, 1) for h in TWO]
        for h in TWO:
            p = jnp.exp2(scores[h] * E - lse_s[h : h + 1, rows])
            if masked:
                p = causal(p, 0.0)
            ds = (p * (dps[h] - delta_s[h : h + 1, rows])).astype(BF)
            acc[here, lanes(h, MINE)] += dot(p.astype(BF), dos[h])
            acc[here, lanes(h)] += dot(ds, qs[h])
            dq_s[h, :, rows] += dot(kt[h, :, here], ds)

    def back_halves(q, k):
        ats = [code // 2 * CHIP + code % 2 * PIECE for code in (q, k)]
        rows, here = ([span(at + n * KEYS, PIECE) for n in TWO] for at in ats)
        two = lambda ref, at, cols: jnp.concatenate([ref[r, cols] for r in at], 0)
        side = lambda get: jnp.concatenate([get(r) for r in rows], 1)
        qs = [two(qkv, rows, lanes(h)) for h in TWO]
        dos = [two(do_s, rows, lanes(h)) for h in TWO]
        scores = [dot(two(qkv, here, lanes(h, MINE)), qs[h], 1, 1) for h in TWO]
        dps = [dot(two(qkv, here, lanes(h, 2 * MINE)), dos[h], 1, 1) for h in TWO]
        for h in TWO:
            p = jnp.exp2(scores[h] * E - side(lambda r: lse_s[h : h + 1, r]))
            ds = (p * (dps[h] - side(lambda r: delta_s[h : h + 1, r]))).astype(BF)
            for base, t in ((MINE, dot(p.astype(BF), dos[h])), (0, dot(ds, qs[h]))):
                for n in TWO:
                    acc[here[n], lanes(h, base)] += t[n * PIECE : (n + 1) * PIECE]
            t = dot(jnp.concatenate([kt[h, :, r] for r in here], 1), ds)
            for n in TWO:
                dq_s[h, :, rows[n]] += t[:, n * PIECE : (n + 1) * PIECE]

    runs = ["00100110002101211021", "0011011100200120102011201121", "1130113120302031", "10301031213021310030003101300131"]
    digits = [int(c) for c in "".join(runs)]
    ends = [sum(len(r) for r in runs[:n]) // 4 for n in range(len(runs) + 1)]
    bit = lambda field, by: sum((v // by % 2) << n for n, v in enumerate(digits[field::4]))
    masks = [bit(field, by) for field, by in ((0, 2), (0, 1), (1, 1), (2, 2), (2, 1), (3, 1))]

    def between(first, last):
        def body(n, _):
            bits = [lax.rem(lax.shift_right_logical(jnp.int32(m), n), 2) for m in masks]
            a, b = (2 * place.seen(2 * bits[e] + bits[e + 1]) + bits[e + 2] for e in (0, 3))
            back_halves(jnp.maximum(a, b), jnp.minimum(a, b))

        loop(last, body, first)

    def back_self(q):
        loop(2, lambda n, _: back(q, q * CHIP + n * KEYS, n, True))
        back(q, q * CHIP, 1, False)

    def pairs(do, first, last):
        def body(p, _):
            end = p // 5
            a, b = place.seen(p // 2 - 2 * end), place.seen(p - p // 2 + 1 - end)
            do(jnp.maximum(a, b), jnp.minimum(a, b))

        loop(last, body, first)

    def alone(one, first, last):
        loop(last, lambda r, _: one(place.seen(r)), first)

    def gain_row():
        return gain_ref[...].astype(F32).reshape(1, D)

    def normed(h):
        def body(n, _):
            here = span(n * MANY, MANY)
            rows = pl.ds(h * PIECE + n * MANY, MANY)
            wide = x_s[rows, :].astype(F32)
            scale = lax.rsqrt(jnp.mean(wide * wide, -1, keepdims=True) + 1e-6)
            scale_s[rows, :] = jnp.broadcast_to(scale, (MANY, HEAD))
            pool[h, here, :] = (wide * scale * gain_row()).astype(BF)

        fills[h].wait()
        loop(PIECE // MANY, body)

    normed(0)
    pl.semaphore_wait(barrier, len(others))
    a_all.begin(SENDS[:1])
    normed(1)
    a_all.begin(SENDS[1:])
    a_all.keep()
    for c in fills[2:]:
        c.start()
    fetch = [pltpu.make_async_copy(dy_ref.at[pl.ds(h * PIECE, PIECE)], pool.at[2 + h], local.at[1, h]) for h in TWO]
    for c in fetch:
        c.start()
    swaps = [push(w, u, CN, send_w, recv_w, n) for n, (w, u) in enumerate(((wq_in, uq), (wk_in, uk), (wv_in, uv)))]
    for c in swaps:
        c.start()
    top_s[...] = jnp.full(top_s.shape, NEG, F32)
    acc[...] = jnp.zeros(acc.shape, F32)
    for h in TWO:
        vt[h, HEAD:, :] = jnp.ones((16, ROWS), BF)
    for c in fills[2:]:
        c.wait()
    wo[...] = pool[4].T
    for c in fetch:
        c.wait()
    y_all.begin(NEAR_SENDS)
    y_all.keep()

    def forward_pass(g, _):
        for n in (1, 2, 3):

            @pl.when(g == n)
            def _():
                a_all.forward(n)
                if n == 1:
                    y_all.begin(FAR_SENDS)

        a_all.work(g, project)

        @pl.when(g == 0)
        def _():
            y_all.ready()
            y_all.work(0, lift)

        near, far = g // 2 * 3, g // 3 * 3
        pairs(attend_pair, far, near + far)
        alone(attend_self, far, near + far // 3)

    a_all.ready()
    loop(4, forward_pass)
    loop(4, attended)
    acc[...] = jnp.zeros(acc.shape, F32)
    dq_s[...] = jnp.zeros(dq_s.shape, F32)
    loop(4, lambda n, _: prepare(place.chip() * 4 + n))

    def finish(block):
        cos, sin = angles(block)
        rows = span(block * PIECE, PIECE)
        for h in TWO:
            grad[rows, lanes(h)] = turn((dq_s[h, :, rows] * SCALE).T, cos, -sin).astype(BF)
            grad[rows, lanes(h, MINE)] = turn(acc[rows, lanes(h)] * SCALE, cos, -sin).astype(BF)
        grad[rows, 2 * MINE :] = acc[rows, MINE:].astype(BF)

    def block(r, core, half):
        return (place.seen(r) * 2 + core) * 2 + half

    def trade(r, half):
        there = theirs.at[place.seen(r), span(half * PIECE, PIECE), :]
        return push(grad.at[span(block(r, 1 - place.core, half) * PIECE, PIECE), :], there, CN, send_g, recv_g, 2 * r + half)

    def settle(r, half):
        finish(block(r, 1 - place.core, half))
        trade(r, half).start()
        finish(block(r, place.core, half))

    def product(to, start, size, cols):
        there = place.beside(*to)
        mine = grad[pl.ds(pl.multiple_of(there.device() * KEYS + start, PIECE), size), :]
        other = theirs[there.chip(), pl.ds(start, size), :]
        total = None
        for g, ws in ((mine, (wq, wk, wv)), (other, (uq, uk, uv))):
            for n, w in enumerate(ws):
                t = dot(g[:, n * MINE : (n + 1) * MINE], w[cols, :], 1, 1)
                total = t if total is None else total + t
        return total

    routes = [(pool.at[n], to) for n, to in enumerate((YN, XN, XN, YN, XN, YN))]

    def move(slot, j):
        src, to = routes[slot]
        cols = span(j * WIDE, WIDE)
        return push(src.at[:, cols], landing.at[slot, :, cols], to, send_r, recv_r, slot * (D // WIDE) + j)

    def take(slot, j, dst, sem):
        cols = span(j * WIDE, WIDE)
        move(slot, j).wait_recv()
        c = pltpu.make_async_copy(landing.at[slot, :, cols], dst.at[:, cols], sem)
        c.start()
        return c

    def columns(do):
        loop(D // WIDE, lambda j, _: do(j, span(j * WIDE, WIDE)))

    def both(j, cols):
        t = product(ACROSS, 0, KEYS, cols).astype(BF)
        for n in TWO:
            pool[n, :, cols] = t[n * PIECE : (n + 1) * PIECE]
        for n in TWO:
            move(n, j).start()

    def direct(j, cols):
        pool[2, :, cols] = product(XN, PIECE, PIECE, cols).astype(BF)
        move(2, j).start()
        pool[3, :, cols] = product(YN, 0, PIECE, cols).astype(BF)
        move(3, j).start()

    def joined(j):
        cols = span(j * WIDE, WIDE)
        for n in TWO:
            move(n, j).wait_send()
        for c in [take(n, j, pool.at[n], last.at[n]) for n in TWO]:
            c.wait()
        pool[4, :, cols] = (product(XN, 0, PIECE, cols) + pool[0, :, cols].astype(F32)).astype(BF)
        move(4, j).start()
        pool[5, :, cols] = (product(YN, PIECE, PIECE, cols) + pool[1, :, cols].astype(F32)).astype(BF)
        move(5, j).start()

    def backward_pass(n, _):
        for g in (1, 2):

            @pl.when(n == g)
            def _():
                y_all.forward(g)
                y_all.ahead(g)
                y_all.deep(g, lift_all, False)

        @pl.when(n == 3)
        def _():
            y_all.forward(3)
            y_all.ahead(3)

        @pl.when(n == 4)
        def _():
            y_all.deep(3, lift_all, True)

        @pl.when(n == 5)
        def _():
            y_all.sent()
            loop(2, lambda t, _: settle(1 + t, 1 - t))
            for c in swaps:
                c.wait()
            for t in TWO:
                trade(1 + t, 1 - t).wait_recv()
            columns(direct)

        first = last = n * 0
        for at, begin, end in zip((1, 2, 4, 5), ends, ends[1:]):
            here = 1 - jnp.minimum(jnp.abs(n - at), 1)
            first, last = first + here * begin, last + here * end
        between(first, last)
        skip = n % 3 * (2 - n % 3)
        start = (n + 1) // 2
        alone(back_self, start, start + 1 - skip)

    a_all.sent()
    loop(6, backward_pass)

    def remaining(t):
        late = t // 4
        return (1 - late) * (3 - 3 * (t // 2)) + late * (1 + t % 2), t % 2

    loop(2, lambda t, _: settle(*remaining(t)))
    for t in TWO:
        trade(3, t).wait_recv()
    columns(both)
    loop(6, lambda t, _: settle(*remaining(t)), 2)
    loop(6, lambda t, _: trade(*remaining(t)).wait_recv(), 2)

    tiles = [(ga, qkv.at[:, :MINE]), (ga, qkv.at[:, MINE : 2 * MINE]), (gy, qkv.at[:, 2 * MINE :]), (gy, do_s)]
    results = [gq_out, gk_out, gv_out, gwo_out]

    def tile(j, slot):
        made = []
        for n in TWO:
            buf, dst = tiles[2 * n + slot]
            made.append(pltpu.make_async_copy(buf.at[:, span(j * MINE, MINE)], dst, loads.at[2 * n + slot]))
        return made

    def out(j, slot, n):
        to = results[n].at[:, :, span(j * MINE, MINE)] if n == 3 else results[n].at[pl.ds(2 * j, 2)]
        return pltpu.make_async_copy(kt.at[:, :, pl.ds((4 * slot + n) * MINE, MINE)], to, outs.at[4 * slot + n])

    for c in tile(0, 0):
        c.start()

    def stream(n, _):
        for slot in TWO:
            j = 2 * n + slot

            @pl.when(j + 1 < D // MINE)
            def _():
                for c in tile(j + 1, 1 - slot):
                    c.start()

            for c in tile(j, slot):
                c.wait()

            @pl.when(n > 0)
            def _():
                for i in range(4):
                    out(j - 2, slot, i).wait()

            a, dy = tiles[slot][1], tiles[2 + slot][1]
            t = sum(dot(a[k : k + CHIP, :], grad[k : k + CHIP, :], 0, 0) for k in range(0, ROWS, CHIP)).astype(BF)
            for h in TWO:
                for i in range(3):
                    kt[h, :, (4 * slot + i) * MINE : (4 * slot + i + 1) * MINE] = t[lanes(h), i * MINE : (i + 1) * MINE]
                kt[h, :, (4 * slot + 3) * MINE : (4 * slot + 4) * MINE] = dot(vt[h, :HEAD, :], dy[...]).astype(BF)
            for i in range(4):
                out(j, slot, i).start()
        joined(n)

    loop(D // WIDE, stream)

    def mine(j, cols):
        taken = [take(2 + n, j, pool.at[n], last.at[n]) for n in TWO]
        t = product(OWN, 0, KEYS, cols)
        for n, c in enumerate(taken):
            c.wait()
            acc[pl.ds(pl.multiple_of(j * WIDE + (1 - n) * PIECE, PIECE), PIECE), :] = t[(1 - n) * PIECE : (2 - n) * PIECE] + pool[n, :, cols].astype(F32)

    for j in range(D // WIDE):
        for n in (2, 3):
            move(n, j).wait_send()
    again = [pltpu.make_async_copy(dy_ref.at[pl.ds(h * PIECE, PIECE)], pool.at[2 + h], local.at[1, h]) for h in TWO]
    for c in again:
        c.start()

    dgain[...] = jnp.zeros(dgain.shape, F32)
    inner_s[...] = jnp.zeros(inner_s.shape, F32)
    columns(mine)

    def closing(j, cols):
        for n in TWO:
            move(4 + n, j).wait_send()
        for c in [take(n, j, pool.at[n], last.at[n]) for n in (4, 5)]:
            c.wait()
        gain = gain_ref[cols].astype(F32).reshape(1, WIDE)
        for half in TWO:

            def body(n, _):
                here = span(n * MANY, MANY)
                rows = span(half * PIECE + n * MANY, MANY)
                mine_rows = span(j * WIDE + half * PIECE + n * MANY, MANY)
                da = acc[mine_rows, :] + pool[4 + half, here, cols].astype(F32)
                acc[mine_rows, :] = da
                part = da * (x_s[rows, cols].astype(F32) * scale_s[rows, :1])
                dgain[:, cols] += part.reshape(MANY // 8, 8, WIDE).sum(axis=0)
                part = part * gain
                inner_s[rows, :] += sum(part[:, lanes(k)] for k in range(WIDE // HEAD))

            loop(PIECE // MANY, body)

    columns(closing)
    told[0] = dgain[...].sum(axis=0, keepdims=True)
    tell = [push(told.at[0], told.at[n], (n // 4, n // 2 % 2, n % 2), send_n, recv_n, n) for n in range(1, 8)]
    for c in tell:
        c.start()
    for c in again:
        c.wait()
    for half in TWO:

        def ended(n, _):
            here = span(n * SOME, SOME)
            rows = span(half * PIECE + n * SOME, SOME)
            da = jnp.concatenate([acc[span(j * WIDE + half * PIECE + n * SOME, SOME), :] for j in range(D // WIDE)], 1)
            scale = scale_s[rows, :1]
            inner = inner_s[rows, :].sum(axis=1, keepdims=True) * (1 / D)
            got = (da * gain_row() - x_s[rows, :].astype(F32) * (scale * inner)) * scale
            pool[4 + half, here, :] = (pool[2 + half, here, :].astype(F32) + got).astype(BF)

        loop(PIECE // SOME, ended)
        pltpu.make_async_copy(pool.at[4 + half], dx_out.at[pl.ds(half * PIECE, PIECE)], local.at[0, half]).start()
    for slot in TWO:
        for i in range(4):
            out(D // MINE - 2 + slot, slot, i).wait()
    for r in range(4):
        for half in TWO:
            trade(r, half).wait_send()
    for half in TWO:
        pltpu.make_async_copy(pool.at[4 + half], dx_out.at[pl.ds(half * PIECE, PIECE)], local.at[0, half]).wait()
    for c in tell:
        c.wait()
    total = [told[n] for n in range(8)]
    while len(total) > 1:
        total = [total[n] + total[n + 1] for n in range(0, len(total), 2)]
    gain_out[...] = total[0]


def _hand(n, *refs):
    srcs, dsts, bufs, sems = refs[:n], refs[n : 2 * n], refs[2 * n : 3 * n], refs[3 * n]
    loads = [pltpu.make_async_copy(src, buf, sems.at[0, i]) for i, (src, buf) in enumerate(zip(srcs, bufs))]
    stores = [pltpu.make_async_copy(buf, dst, sems.at[1, i]) for i, (buf, dst) in enumerate(zip(bufs, dsts))]
    for c in loads:
        c.start()
    for load, store in zip(loads, stores):
        load.wait()
        store.start()
    for c in stores:
        c.wait()


def hand(arrays):
    hbm = pl.BlockSpec(memory_space=pltpu.HBM)
    n = len(arrays)
    return pl.pallas_call(
        lambda *refs: _hand(n, *refs),
        in_specs=[hbm] * n,
        out_specs=[hbm] * n,
        out_shape=[jax.ShapeDtypeStruct(t.shape, t.dtype) for t in arrays],
        scratch_shapes=[pltpu.VMEM(t.shape, t.dtype) for t in arrays] + [pltpu.SemaphoreType.DMA((2, n))],
        name="hand",
    )(*arrays)


def solution(mesh):
    hbm, vmem = pl.BlockSpec(memory_space=pltpu.HBM), pl.BlockSpec(memory_space=pltpu.VMEM)
    shape = jax.ShapeDtypeStruct
    dma = lambda *n: pltpu.SemaphoreType.DMA(n)

    def step(x, dy, gain, wq, wk, wv, wo):
        rows, tall = shape((ROWS, D), BF), shape((D // HEAD, HEAD, MINE), BF)
        outs = pl.pallas_call(
            _step,
            in_specs=[hbm, hbm, vmem] + [hbm] * 4 + [vmem] * 4,
            out_specs=[hbm] * 8 + [vmem],
            out_shape=[rows, rows, shape((6, PIECE, D), BF), shape((KEYS, D), BF), tall, tall, tall, shape((2, HEAD, D), BF), shape((1, D), F32)],
            scratch_shapes=[
                pltpu.VMEM((6, PIECE, D), BF),
                pltpu.VMEM((KEYS, D), BF),
                *[pltpu.VMEM((KEYS, HEAD), F32)] * 2,
                pltpu.VMEM((ROWS, 3 * MINE), BF),
                pltpu.VMEM((ROWS, MINE), BF),
                pltpu.VMEM((2, HEAD + 16, ROWS), BF),
                pltpu.VMEM((2, HEAD, ROWS), BF),
                pltpu.VMEM((4, 4, KEYS), F32),
                pltpu.VMEM((2, ROWS), F32),
                pltpu.VMEM((2, ROWS), F32),
                pltpu.VMEM((ROWS, 2 * MINE), F32),
                pltpu.VMEM((2, HEAD, ROWS), F32),
                pltpu.VMEM((ROWS, 3 * MINE), BF),
                pltpu.VMEM((4, KEYS, 3 * MINE), BF),
                *[pltpu.VMEM((D, MINE), BF)] * 7,
                pltpu.VMEM((8, D), F32),
                pltpu.VMEM((8, 1, D), F32),
                *[dma(16)] * 4, dma(2, 2), *[dma(4)] * 3, *[dma(8)] * 2, *[dma(24)] * 2, *[dma(8)] * 3, dma(6), dma(6),
            ],
            compiler_params=pltpu.CompilerParams(collective_id=0, has_side_effects=True, vmem_limit_bytes=67043328),
            cost_estimate=pl.CostEstimate(flops=80 * 10**9, bytes_accessed=2**27, transcendentals=2 * ROWS * ROWS),
            name="step",
        )(x, dy, gain, wq, wk, wv, wo, *tables())
        dx, gq, gk, gv, gwo, dgain = hand(outs[3:])
        return dx, dgain, *[t.reshape(D, MINE) for t in (gq, gk, gv)], gwo.reshape(MINE, D)

    tokens, columns = P(("dp", "tp"), None), P(None, "tp")
    return jax.shard_map(
        step,
        mesh=mesh,
        in_specs=(tokens, tokens, P(None), columns, columns, columns, P("tp", None)),
        out_specs=(tokens, P("dp", None), P("dp", "tp"), P("dp", "tp"), P("dp", "tp"), P(("dp", "tp"), None)),
        check_vma=False,
    )
```

```python
import jax
import jax.numpy as jnp
import numpy as np
from jax import lax
from jax.experimental import pallas as pl
from jax.experimental.pallas import tpu as pltpu
from jax.sharding import PartitionSpec as P

HEAD = 128
THETA = 10000
LOG2E = 1.4426950408889634
NEG, HIDDEN = -1e30, -2e30
ROWS, D, MINE = 4096, 2048, 256
PIECE = 256
KEYS = 512
CHIP = 1024
MANY = 64
WIDE = 512
SCALE = HEAD**-0.5
E = SCALE * LOG2E
BF, F32 = jnp.bfloat16, jnp.float32
TWO = range(2)
MESH = pl.DeviceIdType.MESH


def tables():
    half = HEAD // 2
    freq = float(THETA) ** (-np.arange(half) / half)
    both = lambda t: np.concatenate([t, t], 1).astype(np.float32)
    near = np.arange(PIECE)[:, None] * freq
    far = np.arange(0, ROWS, PIECE)[:, None] * freq
    return tuple(jnp.asarray(both(f(t))) for t in (near, far) for f in (np.cos, np.sin))


def dot(a, b, ca=1, cb=0):
    return lax.dot_general(a, b, (((ca,), (cb,)), ((), ())), preferred_element_type=F32)


def span(start, size):
    return pl.ds(pl.multiple_of(start, size), size)


def lanes(h, base=0):
    return slice(base + h * HEAD, base + (h + 1) * HEAD)


def turn(t, cos, sin):
    return t * cos + pltpu.roll(t, HEAD // 2, 1) * sin


def causal(s, hidden):
    ok = lax.broadcasted_iota(jnp.int32, s.shape, 1) >= lax.broadcasted_iota(jnp.int32, s.shape, 0)
    return jnp.where(ok, s, hidden)


def loop(last, body, first=0):
    lax.fori_loop(first, last, body, None)


def flipped(at, f):
    return lax.rem(at + f, 2)


class Place:
    def __init__(self, x, y, core):
        self.x, self.y, self.core = x, y, core

    def beside(self, fx, fy, fc):
        return Place(flipped(self.x, fx), flipped(self.y, fy), flipped(self.core, fc))

    def device(self):
        return 2 * self.chip() + self.core

    def chip(self):
        return 2 * self.x + self.y

    def id(self):
        return {"tp": self.device()}

    def seen(self, r):
        return self.beside(lax.rem(r, 2), lax.div(r, 2), 0).chip()

    def piece(self, group, i):
        odd, core = i % 2, i // 2
        beyond = (group + 1) // 2
        far, one = beyond // 2, beyond % 2
        swapped = group // 2 - group // 3
        return self.rows((far + one * (1 - odd), far + one * odd, core), odd + swapped * (1 - 2 * odd))

    def rows(self, to, half):
        return span((2 * self.beside(*to).device() + half) * PIECE, PIECE)


OWN, XN, YN, CN, ACROSS = (0, 0, 0), (1, 0, 0), (0, 1, 0), (0, 0, 1), (1, 1, 0)
FAR_SENDS = [(0, 1, 0, XN), (1, 1, 1, YN), (1, 2, 0, XN), (0, 2, 1, YN)]
NEAR_SENDS = [(0, 0, 2, CN), (1, 0, 3, CN)]
SENDS = FAR_SENDS + NEAR_SENDS
FORWARDS = {1: [(0, 3, 0, YN), (1, 3, 1, XN), (0, 1, 2, CN), (1, 1, 3, CN)], 2: [(0, 2, 2, CN), (1, 2, 3, CN)], 3: [(0, 3, 2, CN), (1, 3, 3, CN)]}


class Gather:
    def __init__(self, place, pool, base, buf, sends, recvs, local, loads):
        self.place, self.pool, self.buf, self.sends, self.recvs, self.local = place, pool, buf, sends, recvs, local
        self.own, self.loads = [pool.at[base + h] for h in TWO], loads

    def copy(self, src, group, i, to):
        there = self.place.beside(*to)
        at = self.buf.at[there.piece(group, i), :]
        slot = 4 * group + i
        return pltpu.make_async_remote_copy(src_ref=at if src is None else src, dst_ref=at, send_sem=self.sends.at[slot],
                                            recv_sem=self.recvs.at[slot], device_id=there.id(), device_id_type=MESH)

    def kept(self):
        return [pltpu.make_async_copy(self.own[h], self.buf.at[self.place.rows(OWN, h), :], self.local.at[h]) for h in TWO]

    def keep(self):
        for c in self.kept():
            c.start()

    def begin(self, sends):
        for h, group, i, to in sends:
            self.copy(self.own[h], group, i, to).start()

    def ready(self):
        for c in self.kept():
            c.wait()

    def arrived(self, group, i):
        at = self.buf.at[self.place.piece(group, i), :]
        slot = 4 * group + i
        pltpu.make_async_remote_copy(src_ref=at, dst_ref=at, send_sem=self.sends.at[slot], recv_sem=self.recvs.at[slot],
                                     device_id=self.place.beside(*XN).id(), device_id_type=MESH).wait_recv()

    def forward(self, group):
        for i in TWO:
            self.arrived(group, i)
        for i, g, n, to in FORWARDS[group]:
            self.copy(self.buf.at[self.place.piece(group, i), :], g, n, to).start()

    def sent(self):
        for h, group, i, to in SENDS:
            self.copy(self.own[h], group, i, to).wait_send()
        for at, todo in FORWARDS.items():
            for i, g, n, to in todo:
                self.copy(self.buf.at[self.place.piece(at, i), :], g, n, to).wait_send()

    def work(self, group, do):
        def load(i):
            slot = lax.rem(i, 2) + 4
            return slot, pltpu.make_async_copy(self.buf.at[self.place.piece(group, i), :], self.pool.at[slot], self.loads.at[slot - 4])

        load(jnp.int32(0))[1].start()

        def body(i, _):
            @pl.when(i < 3)
            def _():
                @pl.when(i >= 1)
                def _():
                    self.arrived(group, i + 1)

                load(i + 1)[1].start()

            slot, c = load(i)
            c.wait()
            do(slot, self.place.piece(group, i).start // PIECE)

        loop(4, body)

    def deep_load(self, group, i):
        slot = lax.rem(i + 4, 6)
        return slot, pltpu.make_async_copy(self.buf.at[self.place.piece(group, i), :], self.pool.at[slot], self.loads.at[i])

    def ahead(self, group):
        for i in TWO:
            self.deep_load(group, jnp.int32(i))[1].start()

    def deep(self, group, do, at_once):
        def others():
            for i in (2, 3):
                self.arrived(group, i)
                self.deep_load(group, jnp.int32(i))[1].start()

        if at_once:
            others()

        def body(t, _):
            if not at_once:
                pl.when(t == 1)(others)
            both = [self.deep_load(group, 2 * t + n) for n in TWO]
            for _, c in both:
                c.wait()
            do(both[0][0], [self.place.piece(group, 2 * t + n).start // PIECE for n in TWO])

        loop(2, body)


def _step(x_ref, dy_ref, gain_ref, wq_in, wk_in, wv_in, wo_in, nc, ns, fc, fs,
          ga, gy, landing, dx_out, gq_out, gk_out, gv_out, gwo_out, gain_out,
          pool, x_s, scale_s, inner_s, qkv, do_s, vt, kt, top_s, lse_s, delta_s, acc, dq_s, grad, theirs, wq, wk, wv, wo, uq, uk, uv, dgain, told,
          send_a, send_y, recv_a, recv_y, local, loads, send_w, recv_w, send_g, recv_g, send_r, recv_r, send_n, recv_n, outs, given, last):
    me = lax.axis_index("tp")
    place = Place(lax.div(me, 4), lax.rem(lax.div(me, 2), 2), lax.rem(me, 2))
    others = [place.beside(n // 4, n // 2 % 2, n % 2) for n in range(1, 8)]
    barrier = pltpu.get_barrier_semaphore()
    for there in others:
        pl.semaphore_signal(barrier, inc=1, device_id=there.id(), device_id_type=MESH)
    fills = [(x_ref.at[pl.ds(h * PIECE, PIECE)], x_s.at[pl.ds(h * PIECE, PIECE)]) for h in TWO]
    fills += [(wo_in, pool.at[4]), (wq_in, wq), (wk_in, wk), (wv_in, wv)]
    fills = [pltpu.make_async_copy(src, dst, given.at[n]) for n, (src, dst) in enumerate(fills)]
    for c in fills[:2]:
        c.start()

    a_all = Gather(place, pool, 0, ga, send_a, recv_a, local.at[0], loads)
    y_all = Gather(place, pool, 2, gy, send_y, recv_y, local.at[1], loads)

    def push(src, dst, to, sends, recvs, slot):
        return pltpu.make_async_remote_copy(src_ref=src, dst_ref=dst, send_sem=sends.at[slot], recv_sem=recvs.at[slot],
                                            device_id=place.beside(*to).id(), device_id_type=MESH)

    def angles(block):
        far_c, far_s = fc[pl.ds(block, 1), :], fs[pl.ds(block, 1), :]
        near_c, near_s = nc[...], ns[...]
        sign = jnp.where(lax.broadcasted_iota(jnp.int32, (1, HEAD), 1) < HEAD // 2, -1.0, 1.0)
        return near_c * far_c - near_s * far_s, (near_s * far_c + near_c * far_s) * sign

    def project(slot, block):
        a = pool[slot]
        cos, sin = angles(block)
        rows = span(block * PIECE, PIECE)
        for at, w in ((0, wq), (MINE, wk)):
            t = dot(a, w[...]).astype(BF).astype(F32)
            for h in TWO:
                got = turn(t[:, lanes(h)], cos, sin).astype(BF)
                qkv[rows, lanes(h, at)] = got
                if at:
                    kt[h, :, rows] = got.T
        v = dot(a, wv[...]).astype(BF)
        qkv[rows, 2 * MINE :] = v
        for h in TWO:
            vt[h, :HEAD, rows] = v[:, lanes(h)].T

    def lift(slot, block):
        rows = span(block * PIECE, PIECE)
        do_s[rows, :] = dot(pool[slot], wo[...]).astype(BF)

    def prepare(block):
        rows = span(block * PIECE, PIECE)
        for h in TWO:
            both = do_s[rows, lanes(h)].astype(F32).T * vt[h, :HEAD, rows].astype(F32)
            delta_s[h : h + 1, rows] = both.sum(axis=0, keepdims=True)

    def lift_all(slot, blocks):
        got = dot(pool[pl.ds(slot, 2)].reshape(2 * PIECE, D), wo[...]).astype(BF)
        for n, block in enumerate(blocks):
            do_s[span(block * PIECE, PIECE), :] = got[n * PIECE : (n + 1) * PIECE]
            prepare(block)

    def attend(chip, at, strips):
        keys = span(at, KEYS)
        pieces = [(h, s, m) for s, m in strips for h in TWO]
        scores = [dot(qkv[keys, lanes(h, MINE)], qkv[span(chip * CHIP + s * KEYS, KEYS), lanes(h)], 1, 1) for h, s, _ in pieces]
        weights, keeps = [], []
        for (h, s, masked), score in zip(pieces, scores):
            if masked:
                score = causal(score, HIDDEN)
            n = 2 * s + h
            old = top_s[chip, n : n + 1, :]
            top = jnp.maximum(old, score.max(axis=0, keepdims=True))
            top_s[chip, n : n + 1, :] = top
            weights.append(jnp.exp2((score - top) * E).astype(BF))
            keeps.append(jnp.exp2((old - top) * E))
        for (h, s, _), p, keep in zip(pieces, weights, keeps):
            here = pl.ds(pl.multiple_of((4 * chip + 2 * s + h) * MINE, MINE), HEAD + 16)
            acc[here, :] = acc[here, :] * keep + dot(vt[h, :, keys], p)

    def attend_pair(q, k):
        loop(2, lambda n, _: attend(q, k * CHIP + n * KEYS, [(0, False), (1, False)]))

    def attend_self(q):
        attend(q, q * CHIP, [(0, True), (1, False)])
        attend(q, q * CHIP + KEYS, [(1, True)])

    def attended(chip, _):
        for s in TWO:
            for h in TWO:
                n = 2 * s + h
                base = pl.multiple_of((4 * chip + n) * MINE, MINE)
                total = acc[pl.ds(base + HEAD, 8), :][:1]
                rows = span(chip * CHIP + s * KEYS, KEYS)
                vt[h, :HEAD, rows] = (acc[pl.ds(base, HEAD), :] * (1 / total)).astype(BF)
                lse_s[h : h + 1, rows] = top_s[chip, n : n + 1, :] * E + jnp.log2(total)

    def back(chip, at, strip, masked):
        here = span(at, KEYS)
        rows = span(chip * CHIP + strip * KEYS, KEYS)
        qs = [qkv[rows, lanes(h)] for h in TWO]
        dos = [do_s[rows, lanes(h)] for h in TWO]
        scores = [dot(qkv[here, lanes(h, MINE)], qs[h], 1, 1) for h in TWO]
        dps = [dot(qkv[here, lanes(h, 2 * MINE)], dos[h], 1, 1) for h in TWO]
        for h in TWO:
            p = jnp.exp2(scores[h] * E - lse_s[h : h + 1, rows])
            if masked:
                p = causal(p, 0.0)
            ds = (p * (dps[h] - delta_s[h : h + 1, rows])).astype(BF)
            acc[here, lanes(h, MINE)] += dot(p.astype(BF), dos[h])
            acc[here, lanes(h)] += dot(ds, qs[h])
            dq_s[h, :, rows] += dot(kt[h, :, here], ds)

    def back_halves(q, k):
        ats = [code // 2 * CHIP + code % 2 * PIECE for code in (q, k)]
        rows, here = ([span(at + n * KEYS, PIECE) for n in TWO] for at in ats)
        two = lambda ref, at, cols: jnp.concatenate([ref[r, cols] for r in at], 0)
        side = lambda get: jnp.concatenate([get(r) for r in rows], 1)
        qs = [two(qkv, rows, lanes(h)) for h in TWO]
        dos = [two(do_s, rows, lanes(h)) for h in TWO]
        scores = [dot(two(qkv, here, lanes(h, MINE)), qs[h], 1, 1) for h in TWO]
        dps = [dot(two(qkv, here, lanes(h, 2 * MINE)), dos[h], 1, 1) for h in TWO]
        for h in TWO:
            p = jnp.exp2(scores[h] * E - side(lambda r: lse_s[h : h + 1, r]))
            ds = (p * (dps[h] - side(lambda r: delta_s[h : h + 1, r]))).astype(BF)
            for base, t in ((MINE, dot(p.astype(BF), dos[h])), (0, dot(ds, qs[h]))):
                for n in TWO:
                    acc[here[n], lanes(h, base)] += t[n * PIECE : (n + 1) * PIECE]
            t = dot(jnp.concatenate([kt[h, :, r] for r in here], 1), ds)
            for n in TWO:
                dq_s[h, :, rows[n]] += t[:, n * PIECE : (n + 1) * PIECE]

    runs = ["00100110002101211021", "0011011100200120102011201121", "1130113120302031", "10301031213021310030003101300131"]
    digits = [int(c) for c in "".join(runs)]
    ends = [sum(len(r) for r in runs[:n]) // 4 for n in range(len(runs) + 1)]
    bit = lambda field, by: sum((v // by % 2) << n for n, v in enumerate(digits[field::4]))
    masks = [bit(field, by) for field, by in ((0, 2), (0, 1), (1, 1), (2, 2), (2, 1), (3, 1))]

    def between(first, last):
        def body(n, _):
            bits = [lax.rem(lax.shift_right_logical(jnp.int32(m), n), 2) for m in masks]
            a, b = (2 * place.seen(2 * bits[e] + bits[e + 1]) + bits[e + 2] for e in (0, 3))
            back_halves(jnp.maximum(a, b), jnp.minimum(a, b))

        loop(last, body, first)

    def back_self(q):
        loop(2, lambda n, _: back(q, q * CHIP + n * KEYS, n, True))
        back(q, q * CHIP, 1, False)

    def pairs(do, first, last):
        def body(p, _):
            end = p // 5
            a, b = place.seen(p // 2 - 2 * end), place.seen(p - p // 2 + 1 - end)
            do(jnp.maximum(a, b), jnp.minimum(a, b))

        loop(last, body, first)

    def alone(one, first, last):
        loop(last, lambda r, _: one(place.seen(r)), first)

    def gain_row():
        return gain_ref[...].astype(F32).reshape(1, D)

    def normed(h):
        def body(n, _):
            here = span(n * MANY, MANY)
            rows = pl.ds(h * PIECE + n * MANY, MANY)
            wide = x_s[rows, :].astype(F32)
            scale = lax.rsqrt(jnp.mean(wide * wide, -1, keepdims=True) + 1e-6)
            scale_s[rows, :] = jnp.broadcast_to(scale, (MANY, HEAD))
            pool[h, here, :] = (wide * scale * gain_row()).astype(BF)

        fills[h].wait()
        loop(PIECE // MANY, body)

    normed(0)
    pl.semaphore_wait(barrier, len(others))
    a_all.begin(SENDS[:1])
    normed(1)
    a_all.begin(SENDS[1:])
    a_all.keep()
    for c in fills[2:]:
        c.start()
    fetch = [pltpu.make_async_copy(dy_ref.at[pl.ds(h * PIECE, PIECE)], pool.at[2 + h], local.at[1, h]) for h in TWO]
    for c in fetch:
        c.start()
    swaps = [push(w, u, CN, send_w, recv_w, n) for n, (w, u) in enumerate(((wq_in, uq), (wk_in, uk), (wv_in, uv)))]
    for c in swaps:
        c.start()
    top_s[...] = jnp.full(top_s.shape, NEG, F32)
    acc[...] = jnp.zeros(acc.shape, F32)
    for h in TWO:
        vt[h, HEAD:, :] = jnp.ones((16, ROWS), BF)
    for c in fills[2:]:
        c.wait()
    wo[...] = pool[4].T
    for c in fetch:
        c.wait()
    y_all.begin(NEAR_SENDS)
    y_all.keep()

    def forward_pass(g, _):
        for n in (1, 2, 3):

            @pl.when(g == n)
            def _():
                a_all.forward(n)
                if n == 1:
                    y_all.begin(FAR_SENDS)

        a_all.work(g, project)

        @pl.when(g == 0)
        def _():
            y_all.ready()
            y_all.work(0, lift)

        near, far = g // 2 * 3, g // 3 * 3
        pairs(attend_pair, far, near + far)
        alone(attend_self, far, near + far // 3)

    a_all.ready()
    loop(4, forward_pass)
    loop(4, attended)
    acc[...] = jnp.zeros(acc.shape, F32)
    dq_s[...] = jnp.zeros(dq_s.shape, F32)
    loop(4, lambda n, _: prepare(place.chip() * 4 + n))

    def finish(block):
        cos, sin = angles(block)
        rows = span(block * PIECE, PIECE)
        for h in TWO:
            grad[rows, lanes(h)] = turn((dq_s[h, :, rows] * SCALE).T, cos, -sin).astype(BF)
            grad[rows, lanes(h, MINE)] = turn(acc[rows, lanes(h)] * SCALE, cos, -sin).astype(BF)
        grad[rows, 2 * MINE :] = acc[rows, MINE:].astype(BF)

    def block(r, core, half):
        return (place.seen(r) * 2 + core) * 2 + half

    def trade(r, half):
        there = theirs.at[place.seen(r), span(half * PIECE, PIECE), :]
        return push(grad.at[span(block(r, 1 - place.core, half) * PIECE, PIECE), :], there, CN, send_g, recv_g, 2 * r + half)

    def offer(r, half):
        finish(block(r, 1 - place.core, half))
        trade(r, half).start()

    def hold(r, half):
        finish(block(r, place.core, half))

    def settle(r, half):
        offer(r, half)
        hold(r, half)

    def product(to, start, size, cols):
        there = place.beside(*to)
        mine = grad[pl.ds(pl.multiple_of(there.device() * KEYS + start, PIECE), size), :]
        other = theirs[there.chip(), pl.ds(start, size), :]
        total = None
        for g, ws in ((mine, (wq, wk, wv)), (other, (uq, uk, uv))):
            for n, w in enumerate(ws):
                t = dot(g[:, n * MINE : (n + 1) * MINE], w[cols, :], 1, 1)
                total = t if total is None else total + t
        return total

    routes = [(pool.at[n], to) for n, to in enumerate((YN, XN, XN, YN, XN, YN))]

    def move(slot, j):
        src, to = routes[slot]
        cols = span(j * WIDE, WIDE)
        return push(src.at[:, cols], landing.at[slot, :, cols], to, send_r, recv_r, slot * (D // WIDE) + j)

    def take(slot, j, dst, sem):
        cols = span(j * WIDE, WIDE)
        move(slot, j).wait_recv()
        c = pltpu.make_async_copy(landing.at[slot, :, cols], dst.at[:, cols], sem)
        c.start()
        return c

    def columns(do):
        loop(D // WIDE, lambda j, _: do(j, span(j * WIDE, WIDE)))

    def both(j, cols):
        t = product(ACROSS, 0, KEYS, cols).astype(BF)
        for n in TWO:
            pool[n, :, cols] = t[n * PIECE : (n + 1) * PIECE]
        for n in TWO:
            move(n, j).start()

    def direct(j, cols):
        pool[2, :, cols] = product(XN, PIECE, PIECE, cols).astype(BF)
        move(2, j).start()
        pool[3, :, cols] = product(YN, 0, PIECE, cols).astype(BF)
        move(3, j).start()

    def joined(j):
        cols = span(j * WIDE, WIDE)
        for n in TWO:
            move(n, j).wait_send()
        for c in [take(n, j, pool.at[n], last.at[n]) for n in TWO]:
            c.wait()
        pool[4, :, cols] = (product(XN, 0, PIECE, cols) + pool[0, :, cols].astype(F32)).astype(BF)
        move(4, j).start()
        pool[5, :, cols] = (product(YN, PIECE, PIECE, cols) + pool[1, :, cols].astype(F32)).astype(BF)
        move(5, j).start()

    def backward_pass(n, _):
        for g in (1, 2):

            @pl.when(n == g)
            def _():
                y_all.forward(g)
                y_all.ahead(g)
                y_all.deep(g, lift_all, False)

        @pl.when(n == 3)
        def _():
            y_all.forward(3)
            y_all.ahead(3)

        @pl.when(n == 4)
        def _():
            y_all.deep(3, lift_all, True)

        @pl.when(n == 5)
        def _():
            y_all.sent()
            loop(2, lambda t, _: offer(1 + t, 1 - t))
            loop(2, lambda t, _: hold(1 + t, 1 - t))
            for c in swaps:
                c.wait()
            for t in TWO:
                trade(1 + t, 1 - t).wait_recv()
            columns(direct)

        first = last = n * 0
        for at, begin, end in zip((1, 2, 4, 5), ends, ends[1:]):
            here = 1 - jnp.minimum(jnp.abs(n - at), 1)
            first, last = first + here * begin, last + here * end
        between(first, last)
        skip = n % 3 * (2 - n % 3)
        start = (n + 1) // 2
        alone(back_self, start, start + 1 - skip)

    a_all.sent()
    loop(6, backward_pass)

    def remaining(t):
        late = t // 4
        return (1 - late) * (3 - 3 * (t // 2)) + late * (1 + t % 2), t % 2

    loop(2, lambda t, _: offer(*remaining(t)))
    loop(2, lambda t, _: hold(*remaining(t)))
    for t in TWO:
        trade(3, t).wait_recv()
    columns(both)
    loop(6, lambda t, _: settle(*remaining(t)), 2)
    loop(6, lambda t, _: trade(*remaining(t)).wait_recv(), 2)

    tiles = [(ga, qkv.at[:, :MINE]), (ga, qkv.at[:, MINE : 2 * MINE]), (gy, qkv.at[:, 2 * MINE :]), (gy, do_s)]
    results = [gq_out, gk_out, gv_out, gwo_out]

    def tile(j, slot):
        made = []
        for n in TWO:
            buf, dst = tiles[2 * n + slot]
            made.append(pltpu.make_async_copy(buf.at[:, span(j * MINE, MINE)], dst, loads.at[2 * n + slot]))
        return made

    def out(j, slot, n):
        to = results[n].at[:, :, span(j * MINE, MINE)] if n == 3 else results[n].at[pl.ds(2 * j, 2)]
        return pltpu.make_async_copy(kt.at[:, :, pl.ds((4 * slot + n) * MINE, MINE)], to, outs.at[4 * slot + n])

    for c in tile(0, 0):
        c.start()

    def stream(n, _):
        for slot in TWO:
            j = 2 * n + slot

            @pl.when(j + 1 < D // MINE)
            def _():
                for c in tile(j + 1, 1 - slot):
                    c.start()

            for c in tile(j, slot):
                c.wait()

            @pl.when(n > 0)
            def _():
                for i in range(4):
                    out(j - 2, slot, i).wait()

            a, dy = tiles[slot][1], tiles[2 + slot][1]
            t = sum(dot(a[k : k + CHIP, :], grad[k : k + CHIP, :], 0, 0) for k in range(0, ROWS, CHIP)).astype(BF)
            for h in TWO:
                for i in range(3):
                    kt[h, :, (4 * slot + i) * MINE : (4 * slot + i + 1) * MINE] = t[lanes(h), i * MINE : (i + 1) * MINE]
                kt[h, :, (4 * slot + 3) * MINE : (4 * slot + 4) * MINE] = dot(vt[h, :HEAD, :], dy[...]).astype(BF)
            for i in range(4):
                out(j, slot, i).start()
        joined(n)

    loop(D // WIDE, stream)

    def mine(j, cols):
        taken = [take(2 + n, j, pool.at[n], last.at[n]) for n in TWO]
        t = product(OWN, 0, KEYS, cols)
        for n, c in enumerate(taken):
            c.wait()
            acc[pl.ds(pl.multiple_of(j * WIDE + (1 - n) * PIECE, PIECE), PIECE), :] = t[(1 - n) * PIECE : (2 - n) * PIECE] + pool[n, :, cols].astype(F32)

    for j in range(D // WIDE):
        for n in (2, 3):
            move(n, j).wait_send()
    again = [pltpu.make_async_copy(dy_ref.at[pl.ds(h * PIECE, PIECE)], pool.at[2 + h], local.at[1, h]) for h in TWO]
    for c in again:
        c.start()

    dgain[...] = jnp.zeros(dgain.shape, F32)
    inner_s[...] = jnp.zeros(inner_s.shape, F32)
    columns(mine)

    def closing(j, cols):
        for n in TWO:
            move(4 + n, j).wait_send()
        for c in [take(n, j, pool.at[n], last.at[n]) for n in (4, 5)]:
            c.wait()
        gain = gain_ref[cols].astype(F32).reshape(1, WIDE)
        for half in TWO:

            def body(n, _):
                here = span(n * MANY, MANY)
                rows = span(half * PIECE + n * MANY, MANY)
                mine_rows = span(j * WIDE + half * PIECE + n * MANY, MANY)
                da = acc[mine_rows, :] + pool[4 + half, here, cols].astype(F32)
                acc[mine_rows, :] = da
                part = da * (x_s[rows, cols].astype(F32) * scale_s[rows, :1])
                dgain[:, cols] += part.reshape(MANY // 8, 8, WIDE).sum(axis=0)
                part = part * gain
                inner_s[rows, :] += sum(part[:, lanes(k)] for k in range(WIDE // HEAD))

            loop(PIECE // MANY, body)

    columns(closing)
    told[0] = dgain[...].sum(axis=0, keepdims=True)
    tell = [push(told.at[0], told.at[n], (n // 4, n // 2 % 2, n % 2), send_n, recv_n, n) for n in range(1, 8)]
    for c in tell:
        c.start()
    for c in again:
        c.wait()
    for half in TWO:

        def ended(n, _):
            here = span(n * MANY, MANY)
            rows = span(half * PIECE + n * MANY, MANY)
            da = jnp.concatenate([acc[span(j * WIDE + half * PIECE + n * MANY, MANY), :] for j in range(D // WIDE)], 1)
            scale = scale_s[rows, :1]
            inner = inner_s[rows, :].sum(axis=1, keepdims=True) * (1 / D)
            got = (da * gain_row() - x_s[rows, :].astype(F32) * (scale * inner)) * scale
            pool[4 + half, here, :] = (pool[2 + half, here, :].astype(F32) + got).astype(BF)

        loop(PIECE // MANY, ended)
        pltpu.make_async_copy(pool.at[4 + half], dx_out.at[pl.ds(half * PIECE, PIECE)], local.at[0, half]).start()
    for slot in TWO:
        for i in range(4):
            out(D // MINE - 2 + slot, slot, i).wait()
    for r in range(4):
        for half in TWO:
            trade(r, half).wait_send()
    for half in TWO:
        pltpu.make_async_copy(pool.at[4 + half], dx_out.at[pl.ds(half * PIECE, PIECE)], local.at[0, half]).wait()
    for c in tell:
        c.wait()
    total = [told[n] for n in range(8)]
    while len(total) > 1:
        total = [total[n] + total[n + 1] for n in range(0, len(total), 2)]
    gain_out[...] = total[0]


def _hand(n, *refs):
    srcs, dsts, bufs, sems = refs[:n], refs[n : 2 * n], refs[2 * n : 3 * n], refs[3 * n]
    loads = [pltpu.make_async_copy(src, buf, sems.at[0, i]) for i, (src, buf) in enumerate(zip(srcs, bufs))]
    stores = [pltpu.make_async_copy(buf, dst, sems.at[1, i]) for i, (buf, dst) in enumerate(zip(bufs, dsts))]
    for c in loads:
        c.start()
    for load, store in zip(loads, stores):
        load.wait()
        store.start()
    for c in stores:
        c.wait()


def hand(arrays):
    hbm = pl.BlockSpec(memory_space=pltpu.HBM)
    n = len(arrays)
    return pl.pallas_call(
        lambda *refs: _hand(n, *refs),
        in_specs=[hbm] * n,
        out_specs=[hbm] * n,
        out_shape=[jax.ShapeDtypeStruct(t.shape, t.dtype) for t in arrays],
        scratch_shapes=[pltpu.VMEM(t.shape, t.dtype) for t in arrays] + [pltpu.SemaphoreType.DMA((2, n))],
        name="hand",
    )(*arrays)


def solution(mesh):
    hbm, vmem = pl.BlockSpec(memory_space=pltpu.HBM), pl.BlockSpec(memory_space=pltpu.VMEM)
    shape = jax.ShapeDtypeStruct
    dma = lambda *n: pltpu.SemaphoreType.DMA(n)

    def step(x, dy, gain, wq, wk, wv, wo):
        rows, tall = shape((ROWS, D), BF), shape((D // HEAD, HEAD, MINE), BF)
        outs = pl.pallas_call(
            _step,
            in_specs=[hbm, hbm, vmem] + [hbm] * 4 + [vmem] * 4,
            out_specs=[hbm] * 8 + [vmem],
            out_shape=[rows, rows, shape((6, PIECE, D), BF), shape((KEYS, D), BF), tall, tall, tall, shape((2, HEAD, D), BF), shape((1, D), F32)],
            scratch_shapes=[
                pltpu.VMEM((6, PIECE, D), BF),
                pltpu.VMEM((KEYS, D), BF),
                *[pltpu.VMEM((KEYS, HEAD), F32)] * 2,
                pltpu.VMEM((ROWS, 3 * MINE), BF),
                pltpu.VMEM((ROWS, MINE), BF),
                pltpu.VMEM((2, HEAD + 16, ROWS), BF),
                pltpu.VMEM((2, HEAD, ROWS), BF),
                pltpu.VMEM((4, 4, KEYS), F32),
                pltpu.VMEM((2, ROWS), F32),
                pltpu.VMEM((2, ROWS), F32),
                pltpu.VMEM((ROWS, 2 * MINE), F32),
                pltpu.VMEM((2, HEAD, ROWS), F32),
                pltpu.VMEM((ROWS, 3 * MINE), BF),
                pltpu.VMEM((4, KEYS, 3 * MINE), BF),
                *[pltpu.VMEM((D, MINE), BF)] * 7,
                pltpu.VMEM((8, D), F32),
                pltpu.VMEM((8, 1, D), F32),
                *[dma(16)] * 4, dma(2, 2), *[dma(4)] * 3, *[dma(8)] * 2, *[dma(24)] * 2, *[dma(8)] * 3, dma(6), dma(6),
            ],
            compiler_params=pltpu.CompilerParams(collective_id=0, has_side_effects=True, vmem_limit_bytes=67043328),
            cost_estimate=pl.CostEstimate(flops=ROWS**3, bytes_accessed=ROWS * ROWS, transcendentals=ROWS * ROWS),
            name="step",
        )(x, dy, gain, wq, wk, wv, wo, *tables())
        dx, gq, gk, gv, gwo, dgain = hand(outs[3:])
        return dx, dgain, *[t.reshape(D, MINE) for t in (gq, gk, gv)], gwo.reshape(MINE, D)

    tokens, columns = P(("dp", "tp"), None), P(None, "tp")
    return jax.shard_map(
        step,
        mesh=mesh,
        in_specs=(tokens, tokens, P(None), columns, columns, columns, P("tp", None)),
        out_specs=(tokens, P("dp", None), P("dp", "tp"), P("dp", "tp"), P("dp", "tp"), P(("dp", "tp"), None)),
        check_vma=False,
    )
```
